128 devices in a mesh: dp: 16 (over z, y), fsdp: 8 (over x, core).
Axes of the slice: x: 4, y: 4, z: 4, core: 2. Of those that a mesh axis runs over, the one named last changes fastest.
Arguments:
- h_saved: bfloat16 [3, 128, 128, 2048], P(None, ('dp', 'fsdp'))
- grad_out: bfloat16 [128, 128, 2048], P(('dp', 'fsdp'))
- w_gate: bfloat16 [3, 2048, 5632], P(None, 'fsdp')
- w_up: bfloat16 [3, 2048, 5632], P(None, 'fsdp')
- w_down: bfloat16 [3, 5632, 2048], P(None, 'fsdp')
Outputs:
- output 1: float32 [3, 2048, 5632], P(None, 'fsdp')
- output 2: float32 [3, 2048, 5632], P(None, 'fsdp')
- output 3: float32 [3, 5632, 2048], P(None, 'fsdp')
- output 4: bfloat16 [128, 128, 2048], P(('dp', 'fsdp'))
All inputs are finite; a program needn't handle non-finite values.
Results may differ from the reference program's by a relative error of at most 0.00604773.
Values are sent between devices in bfloat16 or wider.
A program may use at most 1 GiB of HBM per device.

```python
import jax
import jax.numpy as jnp
from jax import lax

LAYERS = 3
BATCH_DEV = 1
SEQ = 128
D = 2048
FF = 5632
SHARDS = 128

BATCH = SHARDS * BATCH_DEV
TOK_SHARD = BATCH_DEV * SEQ
EPS = 1e-5


def setup_inputs(seed: int = 0) -> dict:
    keys = jax.random.split(jax.random.key(seed), 5)
    h_saved = jax.random.normal(keys[0], (LAYERS, BATCH, SEQ, D), jnp.float32).astype(jnp.bfloat16)
    grad_out = jax.random.normal(keys[1], (BATCH, SEQ, D), jnp.float32).astype(jnp.bfloat16)
    w_gate = (jax.random.normal(keys[2], (LAYERS, D, FF), jnp.float32) * D ** -0.5).astype(jnp.bfloat16)
    w_up = (jax.random.normal(keys[3], (LAYERS, D, FF), jnp.float32) * D ** -0.5).astype(jnp.bfloat16)
    w_down = (jax.random.normal(keys[4], (LAYERS, FF, D), jnp.float32) * FF ** -0.5).astype(jnp.bfloat16)
    return {"h_saved": h_saved, "grad_out": grad_out, "w_gate": w_gate, "w_up": w_up, "w_down": w_down}


def layer_backward(h_in, g_acc, gate_w, up_w, down_w):
    x_full = h_in.astype(jnp.float32)
    inv_rms = lax.rsqrt(jnp.mean(x_full * x_full, axis=-1, keepdims=True) + EPS)
    norm_f = x_full * inv_rms
    norm_b = norm_f.astype(jnp.bfloat16)
    pre_gate = jnp.dot(norm_b, gate_w, preferred_element_type=jnp.float32)
    pre_up = jnp.dot(norm_b, up_w, preferred_element_type=jnp.float32)
    sig_gate = jax.nn.sigmoid(pre_gate)
    silu_gate = pre_gate * sig_gate
    act_b = (silu_gate * pre_up).astype(jnp.bfloat16)
    g_bf = g_acc.astype(jnp.bfloat16)
    d_act = jnp.dot(g_bf, down_w.T, preferred_element_type=jnp.float32)
    grad_down = jnp.dot(act_b.T, g_bf, preferred_element_type=jnp.float32)
    d_gate_b = (d_act * pre_up * sig_gate * (1.0 + pre_gate * (1.0 - sig_gate))).astype(jnp.bfloat16)
    d_up_b = (d_act * silu_gate).astype(jnp.bfloat16)
    grad_gate = jnp.dot(norm_b.T, d_gate_b, preferred_element_type=jnp.float32)
    grad_up = jnp.dot(norm_b.T, d_up_b, preferred_element_type=jnp.float32)
    d_norm = jnp.dot(d_gate_b, gate_w.T, preferred_element_type=jnp.float32) + jnp.dot(d_up_b, up_w.T, preferred_element_type=jnp.float32)
    d_x = inv_rms * (d_norm - norm_f * jnp.mean(d_norm * norm_f, axis=-1, keepdims=True))
    return g_acc + d_x, grad_gate, grad_up, grad_down


def reference(h_saved, grad_out, w_gate, w_up, w_down):
    h_blocks = h_saved.reshape(LAYERS, SHARDS, TOK_SHARD, D)
    g_init = grad_out.reshape(SHARDS, TOK_SHARD, D).astype(jnp.float32)

    def layer_step(g_all, layer_in):
        h_layer, gate_w, up_w, down_w = layer_in
        zero_in = jnp.zeros((D, FF), jnp.float32)
        zero_out = jnp.zeros((FF, D), jnp.float32)

        def shard_step(sums, shard_in):
            h_in, g_acc = shard_in
            g_next, grad_gate, grad_up, grad_down = layer_backward(h_in, g_acc, gate_w, up_w, down_w)
            return (sums[0] + grad_gate, sums[1] + grad_up, sums[2] + grad_down), g_next

        sums, g_new = lax.scan(shard_step, (zero_in, zero_in, zero_out), (h_layer, g_all))
        return g_new, sums

    g_final, grads = lax.scan(layer_step, g_init, (h_blocks, w_gate, w_up, w_down), reverse=True)
    d_h0 = g_final.reshape(BATCH, SEQ, D).astype(jnp.bfloat16)
    return grads[0], grads[1], grads[2], d_h0
```

```python
import functools

import jax
import jax.numpy as jnp
from jax import lax
from jax.experimental import pallas as pl
from jax.experimental.pallas import tpu as pltpu
from jax.sharding import PartitionSpec as P


EPS = 1e-5
CHIPS = 4
MESH = pl.DeviceIdType.MESH
VMEM = pltpu.VMEM
ANY = pl.ANY
DMA = pltpu.SemaphoreType.DMA


class Place:
    def __init__(self):
        self.dp = lax.axis_index("dp")
        f = lax.axis_index("fsdp")
        self.x = f // 2
        self.c = f % 2

    def chip(self, step):
        return (self.x + step) % CHIPS

    def ring(self, step):
        return (self.dp, 2 * self.chip(step) + self.c)

    def partner(self):
        return (self.dp, 2 * self.x + (1 - self.c))


def meet(peers):
    barrier = pltpu.get_barrier_semaphore()
    for peer in peers:
        pl.semaphore_signal(barrier, inc=1, device_id=peer, device_id_type=MESH)
    pl.semaphore_wait(barrier, len(peers))


def send(src, dst, send_sem, recv_sem, device):
    copy = pltpu.make_async_remote_copy(
        src_ref=src, dst_ref=dst, send_sem=send_sem, recv_sem=recv_sem, device_id=device, device_id_type=MESH
    )
    copy.start()
    return copy


def arrived(ref, recv_sem, device, send_sem):
    pltpu.make_async_remote_copy(
        src_ref=ref, dst_ref=ref, send_sem=send_sem, recv_sem=recv_sem, device_id=device, device_id_type=MESH
    ).wait_recv()


def params(collective_id, vmem=None):
    return pltpu.CompilerParams(collective_id=collective_id, has_side_effects=True, vmem_limit_bytes=vmem)


def cost(us):
    return pl.CostEstimate(flops=int(us * 4.0e6), bytes_accessed=0, transcendentals=0)


def weight_rows_kernel(layers, rows, cols, gate, up, *refs):
    outs, (buf, load_sem, out_sem, send_sem, recv_sem) = refs[: len(layers)], refs[len(layers):]
    here = Place()
    mine = pl.ds(pl.multiple_of(here.dp * rows, rows), rows)
    loads = []
    for k, layer in enumerate(layers):
        for j in range(CHIPS):
            at = pl.ds(pl.multiple_of(here.chip(j) * cols, cols), cols)
            for m, w in enumerate((gate, up)):
                load = pltpu.make_async_copy(w.at[layer, mine, at], buf.at[k, j, :, pl.ds(m * cols, cols)], load_sem.at[k, j, m])
                load.start()
                loads.append(load)
    meet([here.ring(j) for j in range(1, CHIPS)])
    sends, stores = [], []
    for k in range(len(layers)):
        for j in (1, 3, 2, 0):
            for m in range(2):
                loads[(k * CHIPS + j) * 2 + m].wait()
            if j:
                sends.append(send(buf.at[k, j], outs[k].at[here.x], send_sem.at[k, j], recv_sem.at[k, j], here.ring(j)))
            else:
                store = pltpu.make_async_copy(buf.at[k, 0], outs[k].at[here.x], out_sem.at[k])
                store.start()
                stores.append(store)
    for copy in sends:
        copy.wait_send()
    for k in range(len(layers)):
        for j in range(1, CHIPS):
            arrived(outs[k].at[here.chip(-j)], recv_sem.at[k, j], here.ring(-j), send_sem.at[k, j])
    for store in stores:
        store.wait()


def weight_rows(gate, up, layers, dp, collective_id):
    _, shard, ff = gate.shape
    rows, cols = shard // dp, ff // CHIPS
    out = jax.ShapeDtypeStruct((CHIPS, rows, 2 * cols), gate.dtype)
    n = len(layers)
    return pl.pallas_call(
        functools.partial(weight_rows_kernel, layers, rows, cols),
        out_shape=(out,) * n,
        in_specs=[pl.BlockSpec(memory_space=ANY)] * 2,
        out_specs=(pl.BlockSpec(memory_space=ANY),) * n,
        scratch_shapes=[
            VMEM((n, CHIPS, rows, 2 * cols), gate.dtype),
            DMA((n, CHIPS, 2)),
            DMA((n,)),
            DMA((n, CHIPS)),
            DMA((n, CHIPS)),
        ],
        compiler_params=params(collective_id),
        cost_estimate=cost(6 * n),
        name="weight_rows",
    )(gate, up)


def weight_pair_kernel(own, *refs):
    full, buf, load_sem, out_sem, send_sem, recv_sem = refs[-6:]
    here = Place()
    loads = [pltpu.make_async_copy(own.at[k], buf.at[k], load_sem.at[k]) for k in range(CHIPS)]
    for load in loads:
        load.start()
    meet([here.partner()])
    copies, stores = [], []
    for k in range(CHIPS):
        loads[k].wait()
        copies.append(send(buf.at[k], full.at[k, here.c], send_sem.at[k], recv_sem.at[k], here.partner()))
        store = pltpu.make_async_copy(buf.at[k], full.at[k, here.c], out_sem.at[k])
        store.start()
        stores.append(store)
    for k in range(CHIPS):
        copies[k].wait_send()
        stores[k].wait()
        arrived(full.at[k, 1 - here.c], recv_sem.at[k], here.partner(), send_sem.at[k])


def weight_pair(own, order, collective_id):
    k, rows, cols = own.shape
    return pl.pallas_call(
        weight_pair_kernel,
        out_shape=jax.ShapeDtypeStruct((k, 2, rows, cols), own.dtype),
        in_specs=[pl.BlockSpec(memory_space=ANY)] * (1 + len(order)),
        out_specs=pl.BlockSpec(memory_space=ANY),
        scratch_shapes=[VMEM(own.shape, own.dtype), DMA((k,)), DMA((k,)), DMA((k,)), DMA((k,))],
        compiler_params=params(collective_id),
        cost_estimate=cost(12),
        name="weight_pair",
    )(own, *order)


class RingGather:
    COPIES = 8

    def __init__(self, here, own, slots, pair_slots, send_sem, recv_sem):
        self.here, self.own, self.slots, self.pair = here, own, slots, pair_slots
        self.send_sem, self.recv_sem = send_sem, recv_sem
        self.half = slots.shape[1] // 2
        self.copies = []

    def _send(self, k, src, dst, device):
        self.copies.append(send(src, dst, self.send_sem.at[k], self.recv_sem.at[k], device))

    def _arrived(self, k, ref, device):
        arrived(ref, self.recv_sem.at[k], device, self.send_sem.at[k])

    def start(self):
        x = self.here.x
        self._send(0, self.own, self.slots.at[x], self.here.ring(1))
        self._send(1, self.own, self.slots.at[x], self.here.ring(-1))
        self._send(2, self.own, self.pair.at[x], self.here.partner())

    def relay(self):
        here, half = self.here, self.half
        left, right = here.chip(-1), here.chip(1)
        low, high = pl.ds(0, half), pl.ds(half, half)
        self._arrived(0, self.slots.at[left], here.ring(-1))
        self._send(3, self.slots.at[left, low], self.slots.at[left, low], here.ring(1))
        self._send(5, self.slots.at[left], self.pair.at[left], here.partner())
        self._arrived(1, self.slots.at[right], here.ring(1))
        self._send(4, self.slots.at[right, high], self.slots.at[right, high], here.ring(-1))
        self._send(6, self.slots.at[right], self.pair.at[right], here.partner())

    def finish(self):
        here, half = self.here, self.half
        far = here.chip(2)
        self._arrived(3, self.slots.at[far, pl.ds(0, half)], here.ring(-1))
        self._arrived(4, self.slots.at[far, pl.ds(half, half)], here.ring(1))
        self._send(7, self.slots.at[far], self.pair.at[far], here.partner())
        for k, chip in ((2, here.x), (5, here.chip(-1)), (6, here.chip(1)), (7, far)):
            self._arrived(k, self.pair.at[chip], here.partner())
        for copy in self.copies:
            copy.wait_send()


def own_columns(here, tokens, pair_tokens, out):
    width = out.shape[-1] // CHIPS
    for group, src in enumerate((tokens, pair_tokens)):
        for s in range(CHIPS):
            for k in range(CHIPS):
                at = pl.ds(pl.multiple_of(2 * width * k + width * here.c, width), width)
                out[group, s, :, width * k : width * (k + 1)] = src[s, :, at]


def first_tokens_kernel(n_own, g_own, down, n_all, n_cols, g_all, *refs):
    layers = down.shape[0]
    downs = refs[:layers]
    n_pair, d_buf, d_load, d_out, d_send, d_recv, n_send, n_recv, g_send, g_recv = refs[layers:]
    here = Place()
    loads = [pltpu.make_async_copy(down.at[l], d_buf.at[l], d_load.at[l]) for l in range(layers)]
    for load in loads:
        load.start()
    n_all[here.x] = n_own[...]
    g_all[0, here.x] = g_own[...]
    meet([here.ring(1), here.ring(-1), here.partner()])
    gather_g = RingGather(here, g_own, g_all.at[0], g_all.at[1], g_send, g_recv)
    gather_n = RingGather(here, n_own, n_all, n_pair, n_send, n_recv)
    gather_g.start()
    gather_n.start()
    copies = []
    for l in reversed(range(layers)):
        loads[l].wait()
        copies.append(send(d_buf.at[l], downs[l].at[here.c], d_send.at[l], d_recv.at[l], here.partner()))
        store = pltpu.make_async_copy(d_buf.at[l], downs[l].at[here.c], d_out.at[l])
        store.start()
        loads[l] = store
    gather_g.relay()
    gather_n.relay()
    gather_g.finish()
    gather_n.finish()
    own_columns(here, n_all, n_pair, n_cols)
    for copy in copies:
        copy.wait_send()
    for l in range(layers):
        loads[l].wait()
        arrived(downs[l].at[1 - here.c], d_recv.at[l], here.partner(), d_send.at[l])


def token_shapes(tokens, width):
    return (
        jax.ShapeDtypeStruct((CHIPS, tokens, width), jnp.bfloat16),
        jax.ShapeDtypeStruct((2, CHIPS, tokens, width // 2), jnp.bfloat16),
        jax.ShapeDtypeStruct((2, CHIPS, tokens, width), jnp.bfloat16),
    )


def first_tokens(n_own, g_own, down, collective_id):
    tokens, width = n_own.shape
    layers, rows, _ = down.shape
    full = jax.ShapeDtypeStruct((2, rows, width), down.dtype)
    vmem = pl.BlockSpec(memory_space=VMEM)
    anywhere = pl.BlockSpec(memory_space=ANY)
    c = RingGather.COPIES
    return pl.pallas_call(
        first_tokens_kernel,
        out_shape=token_shapes(tokens, width) + (full,) * layers,
        in_specs=[vmem, vmem, anywhere],
        out_specs=(vmem,) * 3 + (anywhere,) * layers,
        scratch_shapes=[VMEM((CHIPS, tokens, width), jnp.bfloat16), VMEM(down.shape, down.dtype)]
        + [DMA((layers,))] * 4
        + [DMA((c,))] * 4,
        compiler_params=params(collective_id),
        cost_estimate=cost(40),
        name="first_tokens",
    )(n_own, g_own, down)


def pair_rows_kernel(du, dv, act, duv_all, act_all, send_sem, recv_sem, local_sem):
    here = Place()
    ff = du.shape[1]
    low, high = pl.ds(0, ff), pl.ds(ff, ff)
    local = [
        pltpu.make_async_copy(du, duv_all.at[0, :, low], local_sem.at[0]),
        pltpu.make_async_copy(dv, duv_all.at[0, :, high], local_sem.at[1]),
        pltpu.make_async_copy(act, act_all.at[0], local_sem.at[2]),
    ]
    for copy in local:
        copy.start()
    meet([here.partner()])
    copies = [
        send(du, duv_all.at[1, :, low], send_sem.at[0], recv_sem.at[0], here.partner()),
        send(dv, duv_all.at[1, :, high], send_sem.at[1], recv_sem.at[1], here.partner()),
        send(act, act_all.at[1], send_sem.at[2], recv_sem.at[2], here.partner()),
    ]
    for copy in local:
        copy.wait()
    for copy in copies:
        copy.wait()


def pair_rows(du, dv, act, collective_id):
    tokens, ff = du.shape
    vmem = pl.BlockSpec(memory_space=VMEM)
    return pl.pallas_call(
        pair_rows_kernel,
        out_shape=(
            jax.ShapeDtypeStruct((2, tokens, 2 * ff), du.dtype),
            jax.ShapeDtypeStruct((2, tokens, ff), du.dtype),
        ),
        in_specs=[vmem] * 3,
        out_specs=(vmem,) * 2,
        scratch_shapes=[DMA((3,))] * 3,
        compiler_params=params(collective_id),
        cost_estimate=cost(8),
        name="pair_rows",
    )(du, dv, act)


def ring_sum(here, dn, from_left, from_right, in_left, in_right, sum_right, sum_left, send_sem, recv_sem):
    half = dn.shape[1] // 2
    low, high = pl.ds(0, half), pl.ds(half, half)
    right, left, far = here.chip(1), here.chip(-1), here.chip(2)
    to_right, to_left = here.ring(1), here.ring(-1)
    copies = [
        send(dn.at[far, low], from_left, send_sem.at[0], recv_sem.at[0], to_right),
        send(dn.at[far, high], from_right, send_sem.at[1], recv_sem.at[1], to_left),
        send(dn.at[right, high], in_left.at[high], send_sem.at[2], recv_sem.at[2], to_right),
        send(dn.at[left, low], in_right.at[low], send_sem.at[3], recv_sem.at[3], to_left),
    ]
    arrived(from_left, recv_sem.at[0], to_left, send_sem.at[0])
    sum_right[...] = dn[right, low] + from_left[...]
    copies.append(send(sum_right, in_left.at[low], send_sem.at[4], recv_sem.at[4], to_right))
    arrived(from_right, recv_sem.at[1], to_right, send_sem.at[1])
    sum_left[...] = dn[left, high] + from_right[...]
    copies.append(send(sum_left, in_right.at[high], send_sem.at[5], recv_sem.at[5], to_left))
    return copies


def ring_total(here, dn, in_left, in_right, send_sem, recv_sem):
    half = dn.shape[1] // 2
    low, high = pl.ds(0, half), pl.ds(half, half)
    to_right, to_left = here.ring(1), here.ring(-1)
    arrived(in_left.at[high], recv_sem.at[2], to_left, send_sem.at[2])
    arrived(in_right.at[low], recv_sem.at[3], to_right, send_sem.at[3])
    arrived(in_left.at[low], recv_sem.at[4], to_left, send_sem.at[4])
    arrived(in_right.at[high], recv_sem.at[5], to_right, send_sem.at[5])


def g_step(here, dn, in_left, in_right, g, h):
    d_norm = dn[here.x] + in_left[...] + in_right[...]
    x_full = h[...].astype(jnp.float32)
    inv_rms = lax.rsqrt(jnp.mean(x_full * x_full, axis=-1, keepdims=True) + EPS)
    norm_f = x_full * inv_rms
    return g[...] + inv_rms * (d_norm - norm_f * jnp.mean(d_norm * norm_f, axis=-1, keepdims=True))


def next_tokens_kernel(n_order, dn, g, h, n_own, *refs):
    g_out, n_all, n_cols, g_all, n_pair, g_own = refs[n_order : n_order + 6]
    refs = refs[n_order + 6 :]
    ring = refs[:6]
    s_send, s_recv, n_send, n_recv, g_send, g_recv = refs[6:]
    here = Place()
    n_all[here.x] = n_own[...]
    meet([here.ring(1), here.ring(-1), here.partner()])
    copies = ring_sum(here, dn, *ring, s_send, s_recv)
    gather_n = RingGather(here, n_own, n_all, n_pair, n_send, n_recv)
    gather_n.start()
    ring_total(here, dn, ring[2], ring[3], s_send, s_recv)
    g_new = g_step(here, dn, ring[2], ring[3], g, h)
    g_out[...] = g_new
    g_own[...] = g_new.astype(jnp.bfloat16)
    g_all[0, here.x] = g_own[...]
    gather_g = RingGather(here, g_own, g_all.at[0], g_all.at[1], g_send, g_recv)
    gather_g.start()
    gather_n.relay()
    gather_g.relay()
    gather_n.finish()
    own_columns(here, n_all, n_pair, n_cols)
    gather_g.finish()
    for copy in copies:
        copy.wait_send()


def last_tokens_kernel(n_order, dn, g, h, *refs):
    g_out, *refs = refs[n_order:]
    ring = refs[:6]
    s_send, s_recv = refs[6:]
    here = Place()
    meet([here.ring(1), here.ring(-1)])
    copies = ring_sum(here, dn, *ring, s_send, s_recv)
    ring_total(here, dn, ring[2], ring[3], s_send, s_recv)
    g_out[...] = g_step(here, dn, ring[2], ring[3], g, h).astype(g_out.dtype)
    for copy in copies:
        copy.wait_send()


def ring_scratch(tokens, width):
    half, whole = VMEM((tokens // 2, width), jnp.float32), VMEM((tokens, width), jnp.float32)
    return [half, half, whole, whole, half, half]


def next_tokens(dn, g, h, n_own, order, collective_id):
    tokens, width = g.shape
    vmem = pl.BlockSpec(memory_space=VMEM)
    c = RingGather.COPIES
    return pl.pallas_call(
        functools.partial(next_tokens_kernel, len(order)),
        out_shape=(jax.ShapeDtypeStruct(g.shape, g.dtype),) + token_shapes(tokens, width),
        in_specs=[vmem] * 4 + [pl.BlockSpec(memory_space=ANY)] * len(order),
        out_specs=(vmem,) * 4,
        scratch_shapes=[VMEM((CHIPS, tokens, width), jnp.bfloat16), VMEM((tokens, width), jnp.bfloat16)]
        + ring_scratch(tokens, width)
        + [DMA((6,))] * 2
        + [DMA((c,))] * 4,
        compiler_params=params(collective_id),
        cost_estimate=cost(75),
        name="next_tokens",
    )(dn, g, h, n_own, *order)


def last_tokens(dn, g, h, order, collective_id):
    vmem = pl.BlockSpec(memory_space=VMEM)
    return pl.pallas_call(
        functools.partial(last_tokens_kernel, len(order)),
        out_shape=jax.ShapeDtypeStruct(g.shape, jnp.bfloat16),
        in_specs=[vmem] * 3 + [pl.BlockSpec(memory_space=ANY)] * len(order),
        out_specs=vmem,
        scratch_shapes=ring_scratch(*g.shape) + [DMA((6,))] * 2,
        compiler_params=params(collective_id),
        cost_estimate=cost(45),
        name="last_tokens",
    )(dn, g, h, *order)


def grad_rows_kernel(piece, *refs):
    out, send_sem, recv_sem, local_sem = refs[-4:]
    here = Place()
    cols = out.shape[2] // CHIPS

    def landing(m, chip):
        return out.at[m, :, pl.ds(pl.multiple_of(chip * cols, cols), cols)]

    def part(m, chip):
        return piece.at[chip, :, pl.ds(m * cols, cols)]

    local = []
    for m in range(2):
        copy = pltpu.make_async_copy(part(m, here.x), landing(m, here.x), local_sem.at[m])
        copy.start()
        local.append(copy)
    meet([here.ring(j) for j in range(1, CHIPS)])
    copies = []
    for j in (2, 1, 3):
        for m in range(2):
            copies.append(
                send(part(m, here.chip(j)), landing(m, here.x), send_sem.at[j, m], recv_sem.at[j, m], here.ring(j))
            )
    for j in (1, 3, 2):
        for m in range(2):
            arrived(landing(m, here.chip(-j)), recv_sem.at[j, m], here.ring(-j), send_sem.at[j, m])
    for copy in copies:
        copy.wait_send()
    for copy in local:
        copy.wait()


def grad_rows(piece, order, collective_id):
    chips, rows, cols = piece.shape
    vmem = pl.BlockSpec(memory_space=VMEM)
    return pl.pallas_call(
        grad_rows_kernel,
        out_shape=jax.ShapeDtypeStruct((2, rows, chips * cols // 2), piece.dtype),
        in_specs=[vmem] + [pl.BlockSpec(memory_space=ANY)] * len(order),
        out_specs=vmem,
        scratch_shapes=[DMA((chips, 2)), DMA((chips, 2)), DMA((2,))],
        compiler_params=params(collective_id),
        cost_estimate=cost(12),
        name="grad_rows",
    )(piece, *order)


PARTS = 4


def place_kernel(layer, count, *refs):
    grad, outs, (buf, load_sem, store_sem) = refs[0], refs[-3 - count : -3], refs[-3:]
    rows = buf.shape[1] // PARTS
    loads = []
    for m in range(count):
        for k in range(PARTS):
            at = pl.ds(k * rows, rows)
            load = pltpu.make_async_copy(grad.at[m, at], buf.at[m, at], load_sem.at[m, k])
            load.start()
            loads.append(load)
    stores = []
    for m in range(count):
        for k in range(PARTS):
            at = pl.ds(k * rows, rows)
            loads[m * PARTS + k].wait()
            store = pltpu.make_async_copy(buf.at[m, at], outs[m].at[layer, at], store_sem.at[m, k])
            store.start()
            stores.append(store)
    for store in stores:
        store.wait()


def place(grad, layer, layers, stacks):
    count, rows, cols = grad.shape
    anywhere = pl.BlockSpec(memory_space=ANY)
    return pl.pallas_call(
        functools.partial(place_kernel, layer, count),
        out_shape=(jax.ShapeDtypeStruct((layers, rows, cols), grad.dtype),) * count,
        in_specs=[anywhere] * (1 + len(stacks)),
        out_specs=(anywhere,) * count,
        input_output_aliases={1 + m: m for m in range(len(stacks))},
        scratch_shapes=[VMEM(grad.shape, grad.dtype), DMA((count, PARTS)), DMA((count, PARTS))],
        cost_estimate=cost(4 * count),
        name="place",
    )(grad, *stacks)


def gather_dp(value, axis):
    return lax.all_gather(value, "dp", axis=axis, tiled=True)


def scatter_dp(value):
    return lax.psum_scatter(value, "dp", scatter_dimension=1, tiled=True)


def gather_grads(rows, piece_down):
    return gather_dp(rows, 1), gather_dp(piece_down[None], 2)


def solution(mesh):
    dp = mesh.shape["dp"]
    tok_spec = P(("dp", "fsdp"))
    stack_spec = P(None, ("dp", "fsdp"))
    weight_spec = P(None, "fsdp")

    def local_backward(h_saved, grad_out, gate_sh, up_sh, down_sh):
        layers = h_saved.shape[0]
        b_loc, seq, width = grad_out.shape
        tokens = b_loc * seq
        core = lax.axis_index("fsdp") % 2
        h = h_saved.reshape(layers, tokens, width)
        x_full = h.astype(jnp.float32)
        inv_rms = lax.rsqrt(jnp.mean(x_full * x_full, axis=-1, keepdims=True) + EPS)
        n = (x_full * inv_rms).astype(jnp.bfloat16)
        g_bf = grad_out.reshape(tokens, width)
        g = g_bf.astype(jnp.float32)
        last = layers - 1

        own = {}
        ids = iter(range(1, 100))
        (rows,) = weight_rows(gate_sh, up_sh, (last,), dp, next(ids))
        own[last] = gather_dp(rows, 1)
        others = tuple(reversed(range(last)))
        for layer, rows in zip(others, weight_rows(gate_sh, up_sh, others, dp, next(ids))):
            own[layer] = gather_dp(rows, 1)

        n_all, n_cols, g_all, *down = first_tokens(n[last], g_bf, down_sh, next(ids))
        gathered, held, rows_done = {}, {}, ()
        for layer in reversed(range(layers)):
            down_w = down[layer].reshape(-1, width)
            d_act = jnp.einsum("td,fd->tf", g_all[0].reshape(-1, width), down_w, preferred_element_type=jnp.float32)
            w = weight_pair(own[layer], rows_done, next(ids)).reshape(width, -1)
            uv = jnp.einsum("td,df->tf", n_all.reshape(-1, width), w, preferred_element_type=jnp.float32)
            ff = uv.shape[1] // 2
            u, v = uv[:, :ff], uv[:, ff:]
            sig = jax.nn.sigmoid(u)
            silu = u * sig
            act = (silu * v).astype(jnp.bfloat16)
            du = (d_act * v * sig * (1.0 + u * (1.0 - sig))).astype(jnp.bfloat16)
            dv = (d_act * silu).astype(jnp.bfloat16)
            duv_all, act_all = pair_rows(du, dv, act, next(ids))
            grad = jnp.einsum(
                "tk,tf->kf",
                n_cols.reshape(-1, width // 2),
                duv_all.reshape(-1, 2 * ff),
                preferred_element_type=jnp.float32,
            )
            grad = grad.reshape(CHIPS, -1, 2 * ff)
            piece = scatter_dp(grad)
            act_half = lax.dynamic_slice_in_dim(act_all.reshape(-1, ff), core * (ff // 2), ff // 2, axis=1)
            grad_down = jnp.einsum(
                "tf,td->fd", act_half, g_all.reshape(-1, width), preferred_element_type=jnp.float32
            )
            piece_down = scatter_dp(grad_down)
            dn = jnp.einsum("tf,df->td", duv_all[0], w, preferred_element_type=jnp.float32)
            dn = dn.reshape(CHIPS, tokens, width)
            held[layer] = piece, piece_down
            order = (grad, grad_down)
            if layer:
                g, n_all, n_cols, g_all = next_tokens(dn, g, h[layer], n[layer - 1], order, next(ids))
            else:
                d_h0 = last_tokens(dn, g, h[0], order, next(ids))
            if layer == last:
                rows = grad_rows(piece, (g,), next(ids))
                rows_done = (rows, piece_down)
                gathered[layer] = gather_grads(rows, piece_down)
        for layer in reversed(range(last)):
            piece, piece_down = held[layer]
            rows = grad_rows(piece, (d_h0,), next(ids))
            gathered[layer] = gather_grads(rows, piece_down)

        pair, single = (), ()
        for layer in reversed(range(layers)):
            gate_up, down_grad = gathered[layer]
            pair = place(gate_up, layer, layers, pair)
            single = place(down_grad, layer, layers, single)
        return (*pair, *single, d_h0.reshape(b_loc, seq, width))

    return jax.shard_map(
        local_backward,
        mesh=mesh,
        in_specs=(stack_spec, tok_spec, weight_spec, weight_spec, weight_spec),
        out_specs=(weight_spec, weight_spec, weight_spec, tok_spec),
        check_vma=False,
    )
```

```python
import functools

import jax
import jax.numpy as jnp
from jax import lax
from jax.experimental import pallas as pl
from jax.experimental.pallas import tpu as pltpu
from jax.sharding import PartitionSpec as P


EPS = 1e-5
CHIPS = 4
RING = 4
MESH = pl.DeviceIdType.MESH
VMEM = pltpu.VMEM
ANY = pl.ANY
DMA = pltpu.SemaphoreType.DMA


class Place:
    def __init__(self):
        self.dp = lax.axis_index("dp")
        self.f = lax.axis_index("fsdp")
        self.x, self.c = self.f // 2, self.f % 2
        self.z, self.y = self.dp // RING, self.dp % RING

    def chip(self, step):
        return (self.x + step) % CHIPS

    def ring(self, step):
        return (self.dp, 2 * self.chip(step) + self.c)

    def partner(self):
        return (self.dp, 2 * self.x + (1 - self.c))

    def at_y(self, step):
        return (self.y + step) % RING

    def at_z(self, step):
        return (self.z + step) % RING

    def ring_y(self, step):
        return (self.z * RING + self.at_y(step), self.f)

    def ring_z(self, step):
        return (self.at_z(step) * RING + self.y, self.f)


def meet(peers):
    barrier = pltpu.get_barrier_semaphore()
    for peer in peers:
        pl.semaphore_signal(barrier, inc=1, device_id=peer, device_id_type=MESH)
    pl.semaphore_wait(barrier, len(peers))


def send(src, dst, send_sem, recv_sem, device):
    copy = pltpu.make_async_remote_copy(
        src_ref=src, dst_ref=dst, send_sem=send_sem, recv_sem=recv_sem, device_id=device, device_id_type=MESH
    )
    copy.start()
    return copy


def arrived(ref, recv_sem, device, send_sem):
    pltpu.make_async_remote_copy(
        src_ref=ref, dst_ref=ref, send_sem=send_sem, recv_sem=recv_sem, device_id=device, device_id_type=MESH
    ).wait_recv()


def params(collective_id, vmem=None):
    return pltpu.CompilerParams(collective_id=collective_id, has_side_effects=True, vmem_limit_bytes=vmem)


def cost(us):
    return pl.CostEstimate(flops=int(us * 4.0e6), bytes_accessed=0, transcendentals=0)


def weight_rows_kernel(layers, rows, cols, gate, up, *refs):
    first, others, buf, load_sem, out_sem, send_sem, recv_sem = refs
    outs = [first] + [others.at[k] for k in range(len(layers) - 1)]
    here = Place()
    mine = pl.ds(pl.multiple_of(here.dp * rows, rows), rows)
    loads = []
    for k, layer in enumerate(layers):
        for j in range(CHIPS):
            at = pl.ds(pl.multiple_of(here.chip(j) * cols, cols), cols)
            for m, w in enumerate((gate, up)):
                load = pltpu.make_async_copy(w.at[layer, mine, at], buf.at[k, j, :, pl.ds(m * cols, cols)], load_sem.at[k, j, m])
                load.start()
                loads.append(load)
    meet([here.ring(j) for j in range(1, CHIPS)])
    sends, stores = [], []
    for k in range(len(layers)):
        for j in (1, 3, 2, 0):
            for m in range(2):
                loads[(k * CHIPS + j) * 2 + m].wait()
            if j:
                sends.append(send(buf.at[k, j], outs[k].at[here.x], send_sem.at[k, j], recv_sem.at[k, j], here.ring(j)))
            else:
                store = pltpu.make_async_copy(buf.at[k, 0], outs[k].at[here.x], out_sem.at[k])
                store.start()
                stores.append(store)
    for copy in sends:
        copy.wait_send()
    for k in range(len(layers)):
        for j in range(1, CHIPS):
            arrived(outs[k].at[here.chip(-j)], recv_sem.at[k, j], here.ring(-j), send_sem.at[k, j])
    for store in stores:
        store.wait()


def weight_rows(gate, up, layers, dp, collective_id):
    _, shard, ff = gate.shape
    rows, cols = shard // dp, ff // CHIPS
    n = len(layers)
    block = (CHIPS, rows, 2 * cols)
    return pl.pallas_call(
        functools.partial(weight_rows_kernel, layers, rows, cols),
        out_shape=(jax.ShapeDtypeStruct(block, gate.dtype), jax.ShapeDtypeStruct((n - 1, *block), gate.dtype)),
        in_specs=[pl.BlockSpec(memory_space=ANY)] * 2,
        out_specs=(pl.BlockSpec(memory_space=ANY),) * 2,
        scratch_shapes=[
            VMEM((n, *block), gate.dtype),
            DMA((n, CHIPS, 2)),
            DMA((n,)),
            DMA((n, CHIPS)),
            DMA((n, CHIPS)),
        ],
        compiler_params=params(collective_id),
        cost_estimate=cost(12),
        name="weight_rows",
    )(gate, up)


class Ring:
    def __init__(self, device, at, block, own, send_sem, recv_sem):
        self.device, self.at, self.block, self.own = device, at, block, own
        self.send_sem, self.recv_sem = send_sem, recv_sem
        self.copies = []

    def _send(self, k, src, dst, step):
        self.copies.append(send(src, dst, self.send_sem(k), self.recv_sem(k), self.device(step)))

    def _arrived(self, k, ref, step):
        arrived(ref, self.recv_sem(k), self.device(step), self.send_sem(k))

    def start(self):
        here = self.block(self.at(0), None)
        self._send(0, self.own, here, 1)
        self._send(1, self.own, here, -1)

    def relay_right(self):
        self._arrived(0, self.block(self.at(-1), None), -1)
        half = self.block(self.at(-1), 0)
        self._send(2, half, half, 1)

    def relay_left(self):
        self._arrived(1, self.block(self.at(1), None), 1)
        half = self.block(self.at(1), 1)
        self._send(3, half, half, -1)

    def finish(self):
        self._arrived(2, self.block(self.at(2), 0), -1)
        self._arrived(3, self.block(self.at(2), 1), 1)

    def drain(self):
        for copy in self.copies:
            copy.wait_send()


class Tokens:
    COPIES = 8

    def __init__(self, here, own, out, send_sem, recv_sem):
        half = out.shape[2] // 2

        def block(chip, part):
            return out.at[0, chip] if part is None else out.at[0, chip, pl.ds(part * half, half)]

        self.here, self.own, self.out = here, own, out
        self.send_sem, self.recv_sem = send_sem, recv_sem
        self.ring = Ring(here.ring, here.chip, block, own, lambda k: send_sem.at[k], lambda k: recv_sem.at[k])
        self.pairs = []

    def _pair(self, k, src, chip):
        dst = self.out.at[1, chip]
        copy = send(src, dst, self.send_sem.at[4 + k], self.recv_sem.at[4 + k], self.here.partner())
        self.pairs.append((k, chip, copy))

    def start(self):
        self.ring.start()
        self._pair(0, self.own, self.here.x)

    def relay(self):
        left, right = self.here.chip(-1), self.here.chip(1)
        self.ring.relay_right()
        self._pair(1, self.out.at[0, left], left)
        self.ring.relay_left()
        self._pair(2, self.out.at[0, right], right)

    def finish(self):
        far = self.here.chip(2)
        self.ring.finish()
        self._pair(3, self.out.at[0, far], far)
        for k, chip, copy in self.pairs:
            arrived(self.out.at[1, chip], self.recv_sem.at[4 + k], self.here.partner(), self.send_sem.at[4 + k])
            copy.wait_send()
        self.ring.drain()


class Members:
    def __init__(self, here, slots, send_sem, recv_sem):
        self.here, self.slots, self.send_sem, self.recv_sem = here, slots, send_sem, recv_sem
        a1, b1 = self._ring(0, 0, True, here.z), self._ring(1, 2, False, here.y)
        a2 = {step: self._ring(2 + k, 0, False, here.at_y(step)) for k, step in enumerate((0, -1, 1, 2))}
        b2 = {step: self._ring(6 + k, 2, True, here.at_z(step)) for k, step in enumerate((0, -1, 1, 2))}
        self.pairs = ((a1, a2), (b1, b2))

    def _ring(self, group, first, along_y, fixed):
        def block(at, part):
            k = pl.ds(first, 2) if part is None else pl.ds(first + part, 1)
            return self.slots.at[fixed, at, k] if along_y else self.slots.at[at, fixed, k]

        here = self.here
        device, at = (here.ring_y, here.at_y) if along_y else (here.ring_z, here.at_z)
        sems = (lambda k: self.send_sem.at[group, k]), (lambda k: self.recv_sem.at[group, k])
        return Ring(device, at, block, block(at(0), None), *sems)

    def start(self):
        for first, second in self.pairs:
            first.start()
        for first, second in self.pairs:
            second[0].start()

    def relay_first(self):
        for first, second in self.pairs:
            first.relay_right()
            second[-1].start()
        for first, second in self.pairs:
            first.relay_left()
            second[1].start()
        for _, second in self.pairs:
            second[0].relay_right()
            second[0].relay_left()

    def finish(self):
        for first, second in self.pairs:
            first.finish()
            second[2].start()
        for step in (-1, 1, 2):
            for _, second in self.pairs:
                second[step].relay_right()
                second[step].relay_left()
        for step in (0, -1, 1, 2):
            for _, second in self.pairs:
                second[step].finish()

    def drain(self):
        for first, second in self.pairs:
            for r in (first, *second.values()):
                r.drain()


def first_gather_kernel(rows, n_own, g_own, down, w_out, n_all, g_all, *refs):
    layers = down.shape[0]
    downs = refs[:layers]
    w_v, d_v, w_load, own_sem, d_load, d_send, d_recv, w_send, w_recv, n_send, n_recv, g_send, g_recv = refs[layers:]
    here = Place()
    load_w = pltpu.make_async_copy(rows, w_v.at[here.z, here.y], w_load.at[0])
    load_w.start()
    owns = [
        pltpu.make_async_copy(n_own, n_all.at[0, here.x], own_sem.at[0]),
        pltpu.make_async_copy(g_own, g_all.at[0, here.x], own_sem.at[1]),
    ]
    for copy in owns:
        copy.start()
    loads = [pltpu.make_async_copy(down.at[l], d_v.at[l], d_load.at[l]) for l in range(layers)]
    for load in loads:
        load.start()
    meet(
        [here.ring(1), here.ring(-1), here.partner()]
        + [here.ring_y(1), here.ring_y(-1), here.ring_z(1), here.ring_z(-1)]
    )

    members = Members(here, w_v, w_send, w_recv)
    tok_g = Tokens(here, g_own, g_all, g_send, g_recv)
    tok_n = Tokens(here, n_own, n_all, n_send, n_recv)

    tok_n.start()
    tok_g.start()
    load_w.wait()
    members.start()
    copies = []
    for l in reversed(range(layers)):
        loads[l].wait()
        copies.append(send(d_v.at[l], downs[l].at[here.c], d_send.at[l], d_recv.at[l], here.partner()))
        loads[l] = pltpu.make_async_copy(d_v.at[l], downs[l].at[here.c], d_load.at[l])
        loads[l].start()
    members.relay_first()
    tok_n.relay()
    tok_g.relay()
    members.finish()
    store_w = pltpu.make_async_copy(w_v, w_out, w_load.at[0])
    store_w.start()
    tok_n.finish()
    tok_g.finish()
    members.drain()
    for copy in copies:
        copy.wait_send()
    for l in range(layers):
        loads[l].wait()
        arrived(downs[l].at[1 - here.c], d_recv.at[l], here.partner(), d_send.at[l])
    for copy in owns:
        copy.wait()
    store_w.wait()


def first_gather(rows, n_own, g_own, down, collective_id):
    tokens, width = n_own.shape
    layers, d_rows, _ = down.shape
    vmem, anywhere = pl.BlockSpec(memory_space=VMEM), pl.BlockSpec(memory_space=ANY)
    bf = jnp.bfloat16
    token = jax.ShapeDtypeStruct((2, CHIPS, tokens, width), bf)
    weight = (RING, RING, *rows.shape)
    return pl.pallas_call(
        first_gather_kernel,
        out_shape=(jax.ShapeDtypeStruct(weight, bf), token, token)
        + (jax.ShapeDtypeStruct((2, d_rows, width), bf),) * layers,
        in_specs=[anywhere, vmem, vmem, anywhere],
        out_specs=(anywhere,) * (3 + layers),
        scratch_shapes=[VMEM(weight, bf), VMEM(down.shape, bf), DMA((1,)), DMA((2,))]
        + [DMA((layers,))] * 3
        + [DMA((10, 4))] * 2
        + [DMA((Tokens.COPIES,))] * 4,
        compiler_params=params(collective_id),
        cost_estimate=cost(45),
        name="first_gather",
    )(rows, n_own, g_own, down)


def transpose_into(dst, first, src, rows):
    tokens = src.shape[0]
    for k in range(src.shape[1] // rows):
        dst[k * rows : (k + 1) * rows, first : first + tokens] = src[:, k * rows : (k + 1) * rows].T


def layer_kernel(index, has_next, w, n_all, g_all, down, *refs):
    refs = list(refs)
    n_own = refs.pop(0) if has_next else None
    grad, dn = refs[:2]
    n_next = refs[2] if has_next else None
    refs = refs[3:] if has_next else refs[2:]
    w_v, d_v, g_v, n_v, n_t, da_v, uv_v, duv_v, act_v, act_t, dn_v, gu_v, down_v, pack_v = refs[:14]
    w_load, load, w_send, w_recv, x_send, x_recv, out_sem, n_send, n_recv = refs[14:]
    here = Place()
    c = here.c
    f32 = jnp.float32
    _, _, members, rows, width = w_v.shape
    shard, ff, deep = members * rows, width // 2, pack_v.shape[2]
    d_model = g_v.shape[-1]
    tokens = g_v.shape[1] * g_v.shape[2]

    w_loads = [pltpu.make_async_copy(w.at[:, index, k], w_v.at[0, k], w_load.at[k]) for k in range(CHIPS)]
    g_load = pltpu.make_async_copy(g_all, g_v, load.at[0])
    d_loads = [
        pltpu.make_async_copy(down.at[m], d_v.at[pl.ds(m * ff // 2, ff // 2)], load.at[1 + m]) for m in range(2)
    ]
    n_loads = []
    for m, (group, core) in enumerate(((0, c), (0, 1 - c), (1, c))):
        for k in range(CHIPS):
            at = pl.ds(pl.multiple_of(2 * shard * k + shard * core, shard), shard)
            n_loads.append(
                pltpu.make_async_copy(
                    n_all.at[group, :, :, at], n_v.at[m, :, :, pl.ds(shard * k, shard)], load.at[3 + CHIPS * m + k]
                )
            )
    for copy in (*w_loads, g_load, *d_loads, *n_loads):
        copy.start()
    if has_next:
        own = pltpu.make_async_copy(n_own, n_next.at[0, here.x], out_sem.at[6])
        own.start()
        meet([here.partner(), here.ring(1), here.ring(-1)])
        ahead = Tokens(here, n_own, n_next, n_send, n_recv)
        ahead.start()
    else:
        meet([here.partner()])
    w_copies = []
    for k in range(CHIPS):
        w_loads[k].wait()
        w_copies.append(send(w_v.at[0, k], w_v.at[1, k], w_send.at[k], w_recv.at[k], here.partner()))

    g_load.wait()
    for copy in d_loads:
        copy.wait()
    g_here = g_v[0].reshape(tokens, d_model)
    for first in range(0, ff, 768):
        last = min(first + 768, ff)
        da_v[:, first:last] = lax.dot_general(
            g_here, d_v[first:last, :], (((1,), (1,)), ((), ())), preferred_element_type=f32
        )
    for copy in n_loads:
        copy.wait()
    for m, first in ((0, 0), (2, tokens)):
        transpose_into(n_t, first, n_v[m].reshape(tokens, CHIPS * shard), min(128, shard))

    def uv_pass(part):
        lhs = n_v.at[part]
        step = 256 if width % 256 == 0 else width

        @pl.loop(0, width // step)
        def _(k):
            at = pl.ds(pl.multiple_of(k * step, step), step)
            rhs = w_v[part, :, :, :, at].reshape(CHIPS * shard, step)
            block = jnp.dot(lhs[...].reshape(tokens, CHIPS * shard), rhs, preferred_element_type=f32)
            uv_v[:, at] = block if part == 0 else uv_v[:, at] + block

    uv_pass(0)
    for k in range(CHIPS):
        arrived(w_v.at[1, k], w_recv.at[k], here.partner(), w_send.at[k])
    uv_pass(1)
    if has_next:
        ahead.relay()

    tile = min(32, tokens)

    @pl.loop(0, tokens // tile)
    def _(k):
        at = pl.ds(pl.multiple_of(k * tile, tile), tile)
        u, v, d_act = uv_v[at, :ff], uv_v[at, ff:], da_v[at, :]
        sig = jax.nn.sigmoid(u)
        silu = u * sig
        act_v[0, at] = (silu * v).astype(jnp.bfloat16)
        duv_v[0, at, :ff] = (d_act * v * sig * (1.0 + u * (1.0 - sig))).astype(jnp.bfloat16)
        duv_v[0, at, ff:] = (d_act * silu).astype(jnp.bfloat16)

    def dn_pass(part):
        core = c if part == 0 else 1 - c

        @pl.loop(0, CHIPS)
        def _(k):
            at = pl.ds(pl.multiple_of(2 * shard * k + shard * core, shard), shard)
            block = lax.dot_general(
                duv_v[0], w_v[part, k].reshape(shard, width), (((1,), (1,)), ((), ())), preferred_element_type=f32
            )
            dn_v[:, :, at] = block.reshape(dn_v.shape[0], dn_v.shape[1], shard)

    dn_pass(0)
    x_copies = [
        send(duv_v.at[0], duv_v.at[1], x_send.at[0], x_recv.at[0], here.partner()),
        send(act_v.at[0], act_v.at[1], x_send.at[1], x_recv.at[1], here.partner()),
    ]
    dn_pass(1)
    dn_out = pltpu.make_async_copy(dn_v, dn, out_sem.at[4])
    dn_out.start()

    def gu_out(m, k):
        return pltpu.make_async_copy(
            gu_v.at[k % 2],
            grad.at[:, pl.ds(pl.multiple_of(rows * k, rows), rows), pl.ds(m * ff, ff)],
            out_sem.at[k % 2],
        )

    arrived(duv_v.at[1], x_recv.at[0], here.partner(), x_send.at[0])
    for m in range(2):

        @pl.loop(0, CHIPS)
        def _(k):
            if m == 0:

                @pl.when(k >= 2)
                def _():
                    gu_out(m, k).wait()
            else:
                gu_out(m, k).wait()

            at = pl.ds(pl.multiple_of(k * shard, shard), shard)
            rhs = duv_v[:, :, m * ff : (m + 1) * ff].reshape(2 * tokens, ff)
            gu_v[k % 2] = jnp.dot(n_t[at, :], rhs, preferred_element_type=f32).reshape(members, rows, ff)
            gu_out(m, k).start()

    arrived(act_v.at[1], x_recv.at[1], here.partner(), x_send.at[1])
    half = ff // 2
    odd = half % 128
    act_at = pl.ds(pl.multiple_of(c * (half - odd), 128), half + odd)
    for m in range(2):
        transpose_into(act_t, m * tokens, act_v[m, :, act_at], 128)
    group = pack_v.shape[1]
    col = d_model // members

    def down_out(k):
        return pltpu.make_async_copy(
            pack_v.at[k % 2], grad.at[pl.ds(k * group, group), pl.ds(CHIPS * rows, deep)], out_sem.at[2 + k % 2]
        )

    @pl.loop(0, members // group)
    def _(k):
        at = pl.ds(pl.multiple_of(k * group * col, group * col), group * col)
        rhs = g_v[:, :, :, at].reshape(2 * tokens, group * col)
        down_v[...] = jnp.dot(act_t[...], rhs, preferred_element_type=f32)

        @pl.when(k >= 2)
        def _():
            down_out(k).wait()

        for d in range(group):
            for j in range(half // deep):
                at_rows = pl.ds(pl.multiple_of(c * odd + j * deep, 8), deep)
                pack_v[k % 2, d, :, j * col : (j + 1) * col] = down_v[at_rows, d * col : (d + 1) * col]
        down_out(k).start()

    for copy in (*w_copies, *x_copies):
        copy.wait_send()
    if has_next:
        ahead.finish()
        own.wait()
    dn_out.wait()
    for k in range(2):
        gu_out(1, k).wait()
        down_out(k).wait()


def layer_grads(w, index, n_all, g_all, down, n_own, collective_id):
    members, _, _, rows, width = w.shape
    _, _, seq, d_model = n_all.shape
    tokens, shard, ff = CHIPS * seq, members * rows, width // 2
    deep = d_model // members // CHIPS
    half = ff // 2 + (ff // 2) % 128
    group = max(members // 4, 1)
    bf, f32 = jnp.bfloat16, jnp.float32
    vmem, anywhere = pl.BlockSpec(memory_space=VMEM), pl.BlockSpec(memory_space=ANY)
    has_next = n_own is not None
    out = [
        jax.ShapeDtypeStruct((members, CHIPS * rows + deep, width), f32),
        jax.ShapeDtypeStruct((CHIPS, seq, d_model), f32),
    ]
    if has_next:
        out.append(jax.ShapeDtypeStruct(n_all.shape, bf))
    extra = Tokens.COPIES if has_next else 1
    return pl.pallas_call(
        functools.partial(layer_kernel, index, has_next),
        out_shape=tuple(out),
        in_specs=[anywhere] * 4 + [vmem] * has_next,
        out_specs=(anywhere,) * len(out),
        scratch_shapes=[
            VMEM((2, CHIPS, members, rows, width), bf),
            VMEM((ff, d_model), bf),
            VMEM((2, CHIPS, seq, d_model), bf),
            VMEM((3, CHIPS, seq, CHIPS * shard), bf),
            VMEM((CHIPS * shard, 2 * tokens), bf),
            VMEM((tokens, ff), f32),
            VMEM((tokens, width), f32),
            VMEM((2, tokens, width), bf),
            VMEM((2, tokens, ff), bf),
            VMEM((half, 2 * tokens), bf),
            VMEM((CHIPS, seq, d_model), f32),
            VMEM((2, members, rows, ff), f32),
            VMEM((half, group * d_model // members), f32),
            VMEM((2, group, deep, width), f32),
            DMA((CHIPS,)),
            DMA((3 + 3 * CHIPS,)),
            DMA((CHIPS,)),
            DMA((CHIPS,)),
            DMA((2,)),
            DMA((2,)),
            DMA((7,)),
            DMA((extra,)),
            DMA((extra,)),
        ],
        compiler_params=params(collective_id, 60 * 1024 * 1024),
        cost_estimate=cost(45),
        name="layer_grads",
    )(w, n_all, g_all, down, *((n_own,) if has_next else ()))


def ring_sum(here, dn, from_left, from_right, in_left, in_right, sum_right, sum_left, send_sem, recv_sem):
    half = dn.shape[1] // 2
    low, high = pl.ds(0, half), pl.ds(half, half)
    right, left, far = here.chip(1), here.chip(-1), here.chip(2)
    to_right, to_left = here.ring(1), here.ring(-1)
    copies = [
        send(dn.at[far, low], from_left, send_sem.at[0], recv_sem.at[0], to_right),
        send(dn.at[far, high], from_right, send_sem.at[1], recv_sem.at[1], to_left),
        send(dn.at[right, high], in_left.at[high], send_sem.at[2], recv_sem.at[2], to_right),
        send(dn.at[left, low], in_right.at[low], send_sem.at[3], recv_sem.at[3], to_left),
    ]
    arrived(from_left, recv_sem.at[0], to_left, send_sem.at[0])
    sum_right[...] = dn[right, low] + from_left[...]
    copies.append(send(sum_right, in_left.at[low], send_sem.at[4], recv_sem.at[4], to_right))
    arrived(from_right, recv_sem.at[1], to_right, send_sem.at[1])
    sum_left[...] = dn[left, high] + from_right[...]
    copies.append(send(sum_left, in_right.at[high], send_sem.at[5], recv_sem.at[5], to_left))
    return copies


def ring_total(here, dn, in_left, in_right, send_sem, recv_sem):
    half = dn.shape[1] // 2
    low, high = pl.ds(0, half), pl.ds(half, half)
    to_right, to_left = here.ring(1), here.ring(-1)
    arrived(in_left.at[high], recv_sem.at[2], to_left, send_sem.at[2])
    arrived(in_right.at[low], recv_sem.at[3], to_right, send_sem.at[3])
    arrived(in_left.at[low], recv_sem.at[4], to_left, send_sem.at[4])
    arrived(in_right.at[high], recv_sem.at[5], to_right, send_sem.at[5])


def g_step(here, dn, in_left, in_right, g, h):
    d_norm = dn[here.x] + in_left[...] + in_right[...]
    x_full = h[...].astype(jnp.float32)
    inv_rms = lax.rsqrt(jnp.mean(x_full * x_full, axis=-1, keepdims=True) + EPS)
    norm_f = x_full * inv_rms
    return g[...] + inv_rms * (d_norm - norm_f * jnp.mean(d_norm * norm_f, axis=-1, keepdims=True))


def next_tokens_kernel(n_order, dn, g, h, *refs):
    g_out, g_all, g_own = refs[n_order : n_order + 3]
    refs = refs[n_order + 3 :]
    ring = refs[:6]
    s_send, s_recv, g_send, g_recv = refs[6:]
    here = Place()
    meet([here.ring(1), here.ring(-1), here.partner()])
    copies = ring_sum(here, dn, *ring, s_send, s_recv)
    ring_total(here, dn, ring[2], ring[3], s_send, s_recv)
    g_new = g_step(here, dn, ring[2], ring[3], g, h)
    g_own[...] = g_new.astype(jnp.bfloat16)
    g_out[...] = g_new
    g_all[0, here.x] = g_own[...]
    gather = Tokens(here, g_own, g_all, g_send, g_recv)
    gather.start()
    gather.relay()
    gather.finish()
    for copy in copies:
        copy.wait_send()


def last_tokens_kernel(n_order, dn, g, h, *refs):
    g_out, *refs = refs[n_order:]
    ring = refs[:6]
    s_send, s_recv = refs[6:]
    here = Place()
    meet([here.ring(1), here.ring(-1)])
    copies = ring_sum(here, dn, *ring, s_send, s_recv)
    ring_total(here, dn, ring[2], ring[3], s_send, s_recv)
    g_out[...] = g_step(here, dn, ring[2], ring[3], g, h).astype(g_out.dtype)
    for copy in copies:
        copy.wait_send()


def ring_scratch(tokens, width):
    half, whole = VMEM((tokens // 2, width), jnp.float32), VMEM((tokens, width), jnp.float32)
    return [half, half, whole, whole, half, half]


def next_tokens(dn, g, h, order, collective_id):
    tokens, width = g.shape
    vmem = pl.BlockSpec(memory_space=VMEM)
    c = Tokens.COPIES
    return pl.pallas_call(
        functools.partial(next_tokens_kernel, len(order)),
        out_shape=(
            jax.ShapeDtypeStruct(g.shape, g.dtype),
            jax.ShapeDtypeStruct((2, CHIPS, tokens, width), jnp.bfloat16),
        ),
        in_specs=[vmem] * 3 + [pl.BlockSpec(memory_space=ANY)] * len(order),
        out_specs=(vmem,) * 2,
        scratch_shapes=[VMEM((tokens, width), jnp.bfloat16)]
        + ring_scratch(tokens, width)
        + [DMA((6,))] * 2
        + [DMA((c,))] * 2,
        compiler_params=params(collective_id),
        cost_estimate=cost(60),
        name="next_tokens",
    )(dn, g, h, *order)


def last_tokens(dn, g, h, order, collective_id):
    vmem = pl.BlockSpec(memory_space=VMEM)
    return pl.pallas_call(
        functools.partial(last_tokens_kernel, len(order)),
        out_shape=jax.ShapeDtypeStruct(g.shape, jnp.bfloat16),
        in_specs=[vmem] * 3 + [pl.BlockSpec(memory_space=ANY)] * len(order),
        out_specs=vmem,
        scratch_shapes=ring_scratch(*g.shape) + [DMA((6,))] * 2,
        compiler_params=params(collective_id),
        cost_estimate=cost(45),
        name="last_tokens",
    )(dn, g, h, *order)


def grad_rows_kernel(piece, *refs):
    out, send_sem, recv_sem, local_sem = refs[-4:]
    here = Place()
    rows, cols = out.shape[0] // 3, out.shape[1] // CHIPS
    half = 2 * cols

    def landing(m, chip):
        return out.at[pl.ds(m * rows, rows), pl.ds(pl.multiple_of(chip * cols, cols), cols)]

    def part(m, chip):
        return piece.at[pl.ds(pl.multiple_of(chip * rows, rows), rows), pl.ds(m * cols, cols)]

    def down(m):
        return pltpu.make_async_copy(
            piece.at[pl.ds((CHIPS + m) * rows, rows)],
            out.at[pl.ds(2 * rows, rows), pl.ds(m * half, half)],
            local_sem.at[2 + m],
        )

    local = [down(m) for m in range(2)]
    for m in range(2):
        local.append(pltpu.make_async_copy(part(m, here.x), landing(m, here.x), local_sem.at[m]))
    for copy in local:
        copy.start()
    meet([here.ring(j) for j in range(1, CHIPS)])
    copies = []
    for j in (2, 1, 3):
        for m in range(2):
            copies.append(
                send(part(m, here.chip(j)), landing(m, here.x), send_sem.at[j, m], recv_sem.at[j, m], here.ring(j))
            )
    for j in (1, 3, 2):
        for m in range(2):
            arrived(landing(m, here.chip(-j)), recv_sem.at[j, m], here.ring(-j), send_sem.at[j, m])
    for copy in copies:
        copy.wait_send()
    for copy in local:
        copy.wait()


def grad_rows(piece, order, collective_id):
    rows, cols = piece.shape
    vmem = pl.BlockSpec(memory_space=VMEM)
    return pl.pallas_call(
        grad_rows_kernel,
        out_shape=jax.ShapeDtypeStruct((rows // 2, 2 * cols), piece.dtype),
        in_specs=[vmem] + [pl.BlockSpec(memory_space=ANY)] * len(order),
        out_specs=vmem,
        scratch_shapes=[DMA((CHIPS, 2)), DMA((CHIPS, 2)), DMA((4,))],
        compiler_params=params(collective_id),
        cost_estimate=cost(12),
        name="grad_rows",
    )(piece, *order)


PARTS = 4


def place_kernel(index, layer, grad_all, *refs):
    grad = grad_all.at[:, index]
    gate, up, down, buf, pack, load_sem, store_sem = refs[-7:]
    members, rows, ff = grad.shape[0], grad.shape[1] // 3, grad.shape[2]
    part = max(members // PARTS, 1)
    parts = members // part
    loads = []
    for m in (2, 0, 1):
        for k in range(parts):
            at = pl.ds(k * part, part)
            load = pltpu.make_async_copy(grad.at[at, pl.ds(m * rows, rows)], buf.at[m, at], load_sem.at[m, k])
            load.start()
            loads.append(load)
    for k in range(parts):
        loads[k].wait()
    half = ff // 2
    stores = []
    for m, out in enumerate((gate, up)):
        for k in range(parts):
            loads[(1 + m) * parts + k].wait()
            store = pltpu.make_async_copy(
                buf.at[m, pl.ds(k * part, part)],
                out.at[layer, pl.ds(k * part, part)],
                store_sem.at[m, k],
            )
            store.start()
            stores.append(store)

    col = down.shape[2] // members

    @pl.loop(0, half // col)
    def _(j):
        for h in range(2):
            at = pl.ds(pl.multiple_of((2 * j + h) * rows, rows), rows)
            cols = pl.ds(pl.multiple_of(h * half + j * col, col), col)
            for d in range(members):
                pack[at, d * col : (d + 1) * col] = buf[2, d, :, cols]

    store = pltpu.make_async_copy(pack, down.at[layer], store_sem.at[2, 0])
    store.start()
    stores.append(store)
    for store in stores:
        store.wait()


def place(grad, index, layer, stacks, shapes):
    members, _, rows, ff = grad.shape
    anywhere = pl.BlockSpec(memory_space=ANY)
    return pl.pallas_call(
        functools.partial(place_kernel, index, layer),
        out_shape=shapes,
        in_specs=[anywhere] * (1 + len(stacks)),
        out_specs=(anywhere,) * 3,
        input_output_aliases={1 + m: m for m in range(len(stacks))},
        scratch_shapes=[
            VMEM((3, members, rows // 3, ff), grad.dtype),
            VMEM(shapes[2].shape[1:], grad.dtype),
            DMA((3, PARTS)),
            DMA((3, PARTS)),
        ],
        compiler_params=pltpu.CompilerParams(vmem_limit_bytes=58 * 1024 * 1024),
        cost_estimate=cost(13),
        name="place",
    )(grad, *stacks)


def gather_dp(value):
    return lax.all_gather(value[None], "dp", axis=0, tiled=True)


def scatter_dp(value):
    members, *piece = value.shape
    value = value.reshape(members * piece[0], *piece[1:])
    return lax.psum_scatter(value, "dp", scatter_dimension=0, tiled=True)


def solution(mesh):
    dp = mesh.shape["dp"]
    tok_spec = P(("dp", "fsdp"))
    stack_spec = P(None, ("dp", "fsdp"))
    weight_spec = P(None, "fsdp")

    def local_backward(h_saved, grad_out, gate_sh, up_sh, down_sh):
        layers = h_saved.shape[0]
        b_loc, seq, width = grad_out.shape
        tokens = b_loc * seq
        h = h_saved.reshape(layers, tokens, width)
        x_full = h.astype(jnp.float32)
        inv_rms = lax.rsqrt(jnp.mean(x_full * x_full, axis=-1, keepdims=True) + EPS)
        n = (x_full * inv_rms).astype(jnp.bfloat16)
        g_bf = grad_out.reshape(tokens, width)
        g = g_bf.astype(jnp.float32)
        last = layers - 1
        ids = iter(range(1, 100))

        order = tuple(reversed(range(layers)))
        rows, other_rows = weight_rows(gate_sh, up_sh, order, dp, next(ids))
        others = gather_dp(other_rows)
        w, n_all, g_all, *down = first_gather(rows, n[last], g_bf, down_sh, next(ids))
        weights = {layer: (others, k - 1) for k, layer in enumerate(order)}
        weights[last] = w.reshape(dp, 1, *w.shape[2:]), 0
        pieces = {}
        for layer in order:
            n_own = n[layer - 1] if layer else None
            grad, dn, *n_next = layer_grads(*weights[layer], n_all, g_all, down[layer], n_own, next(ids))
            pieces[layer] = scatter_dp(grad)
            if layer:
                n_all = n_next[0]
                g, g_all = next_tokens(dn, g, h[layer], (), next(ids))
            else:
                d_h0 = last_tokens(dn, g, h[0], (), next(ids))
        shard_rows = [grad_rows(pieces[layer], (d_h0,), next(ids)) for layer in order]
        first = gather_dp(jnp.stack(shard_rows[:-1]))
        gathered = [(first, k) for k in range(last)] + [(gather_dp(shard_rows[-1][None]), 0)]

        rows = (layers, dp, gate_sh.shape[1] // dp, gate_sh.shape[2])
        shapes = tuple(jax.ShapeDtypeStruct(shape, jnp.float32) for shape in (rows, rows, down_sh.shape))
        stacks = ()
        for layer, (grad, k) in zip(order, gathered):
            stacks = place(grad, k, layer, stacks, shapes)
        gate, up, down_grad = stacks
        return gate.reshape(gate_sh.shape), up.reshape(up_sh.shape), down_grad, d_h0.reshape(b_loc, seq, width)

    return jax.shard_map(
        local_backward,
        mesh=mesh,
        in_specs=(stack_spec, tok_spec, weight_spec, weight_spec, weight_spec),
        out_specs=(weight_spec, weight_spec, weight_spec, tok_spec),
        check_vma=False,
    )
```

```python
import functools

import jax
import jax.numpy as jnp
from jax import lax
from jax.experimental import pallas as pl
from jax.experimental.pallas import tpu as pltpu
from jax.sharding import PartitionSpec as P


EPS = 1e-5
CHIPS = 4
RING = 4
MESH = pl.DeviceIdType.MESH
VMEM = pltpu.VMEM
ANY = pl.ANY
DMA = pltpu.SemaphoreType.DMA


class Place:
    def __init__(self):
        self.dp = lax.axis_index("dp")
        self.f = lax.axis_index("fsdp")
        self.x, self.c = self.f // 2, self.f % 2
        self.z, self.y = self.dp // RING, self.dp % RING

    def chip(self, step):
        return (self.x + step) % CHIPS

    def ring(self, step):
        return (self.dp, 2 * self.chip(step) + self.c)

    def partner(self):
        return (self.dp, 2 * self.x + (1 - self.c))

    def at_y(self, step):
        return (self.y + step) % RING

    def at_z(self, step):
        return (self.z + step) % RING

    def ring_y(self, step):
        return (self.z * RING + self.at_y(step), self.f)

    def ring_z(self, step):
        return (self.at_z(step) * RING + self.y, self.f)


def meet(peers):
    barrier = pltpu.get_barrier_semaphore()
    for peer in peers:
        pl.semaphore_signal(barrier, inc=1, device_id=peer, device_id_type=MESH)
    pl.semaphore_wait(barrier, len(peers))


def send(src, dst, send_sem, recv_sem, device):
    copy = pltpu.make_async_remote_copy(
        src_ref=src, dst_ref=dst, send_sem=send_sem, recv_sem=recv_sem, device_id=device, device_id_type=MESH
    )
    copy.start()
    return copy


def arrived(ref, recv_sem, device, send_sem):
    pltpu.make_async_remote_copy(
        src_ref=ref, dst_ref=ref, send_sem=send_sem, recv_sem=recv_sem, device_id=device, device_id_type=MESH
    ).wait_recv()


def params(collective_id, vmem=None):
    return pltpu.CompilerParams(collective_id=collective_id, has_side_effects=True, vmem_limit_bytes=vmem)


def cost(us):
    return pl.CostEstimate(flops=int(us * 4.0e6), bytes_accessed=0, transcendentals=0)


class Ring:
    def __init__(self, device, at, block, own, send_sem, recv_sem):
        self.device, self.at, self.block, self.own = device, at, block, own
        self.send_sem, self.recv_sem = send_sem, recv_sem
        self.copies = []

    def _send(self, k, src, dst, step):
        self.copies.append(send(src, dst, self.send_sem(k), self.recv_sem(k), self.device(step)))

    def _arrived(self, k, ref, step):
        arrived(ref, self.recv_sem(k), self.device(step), self.send_sem(k))

    def start(self):
        here = self.block(self.at(0), None)
        self._send(0, self.own, here, 1)
        self._send(1, self.own, here, -1)

    def relay_right(self):
        self._arrived(0, self.block(self.at(-1), None), -1)
        half = self.block(self.at(-1), 0)
        self._send(2, half, half, 1)

    def relay_left(self):
        self._arrived(1, self.block(self.at(1), None), 1)
        half = self.block(self.at(1), 1)
        self._send(3, half, half, -1)

    def finish(self):
        self._arrived(2, self.block(self.at(2), 0), -1)
        self._arrived(3, self.block(self.at(2), 1), 1)

    def drain(self):
        for copy in self.copies:
            copy.wait_send()


class Tokens:
    COPIES = 8

    def __init__(self, here, own, out, send_sem, recv_sem):
        half = out.shape[2] // 2

        def block(chip, part):
            return out.at[0, chip] if part is None else out.at[0, chip, pl.ds(part * half, half)]

        self.here, self.own, self.out = here, own, out
        self.send_sem, self.recv_sem = send_sem, recv_sem
        self.ring = Ring(here.ring, here.chip, block, own, lambda k: send_sem.at[k], lambda k: recv_sem.at[k])
        self.pairs = []

    def _pair(self, k, src, chip):
        dst = self.out.at[1, chip]
        copy = send(src, dst, self.send_sem.at[4 + k], self.recv_sem.at[4 + k], self.here.partner())
        self.pairs.append((k, chip, copy))

    def start(self):
        self.ring.start()
        self._pair(0, self.own, self.here.x)

    def relay(self):
        left, right = self.here.chip(-1), self.here.chip(1)
        self.ring.relay_right()
        self._pair(1, self.out.at[0, left], left)
        self.ring.relay_left()
        self._pair(2, self.out.at[0, right], right)

    def far(self):
        far = self.here.chip(2)
        self.ring.finish()
        self._pair(3, self.out.at[0, far], far)

    def finish(self):
        for k, chip, copy in self.pairs:
            arrived(self.out.at[1, chip], self.recv_sem.at[4 + k], self.here.partner(), self.send_sem.at[4 + k])
            copy.wait_send()
        self.ring.drain()


class Members:
    GROUPS = 10
    PAIRS = 8

    def __init__(self, here, slots, send_sem, recv_sem, pair=None, pair_send=None, pair_recv=None):
        self.here, self.slots, self.send_sem, self.recv_sem = here, slots, send_sem, recv_sem
        self.pair, self.pair_send, self.pair_recv = pair, pair_send, pair_recv
        a1, b1 = self._ring(0, 0, True, here.z), self._ring(1, 2, False, here.y)
        a2 = {step: self._ring(2 + k, 0, False, here.at_y(step)) for k, step in enumerate((0, -1, 1, 2))}
        b2 = {step: self._ring(6 + k, 2, True, here.at_z(step)) for k, step in enumerate((0, -1, 1, 2))}
        self.rings = ((a1, a2), (b1, b2))
        self.forwards = []

    def _ring(self, group, first, along_y, fixed):
        def block(at, part):
            k = pl.ds(first, 2) if part is None else pl.ds(first + part, 1)
            return self.slots.at[fixed, at, k] if along_y else self.slots.at[at, fixed, k]

        here = self.here
        device, at = (here.ring_y, here.at_y) if along_y else (here.ring_z, here.at_z)
        sems = (lambda k: self.send_sem.at[group, k]), (lambda k: self.recv_sem.at[group, k])
        return Ring(device, at, block, block(at(0), None), *sems)

    def start(self):
        for first, second in self.rings:
            first.start()
        for first, second in self.rings:
            second[0].start()

    def relay_first(self):
        for first, second in self.rings:
            first.relay_right()
            second[-1].start()
        for first, second in self.rings:
            first.relay_left()
            second[1].start()
        for _, second in self.rings:
            second[0].relay_right()
            second[0].relay_left()

    def far(self):
        for first, second in self.rings:
            first.finish()
            second[2].start()
        self.relay(-1)

    def relay(self, step):
        for _, second in self.rings:
            second[step].relay_right()
            second[step].relay_left()

    def done(self, *steps):
        for step in steps:
            for m, (_, second) in enumerate(self.rings):
                second[step].finish()
                if self.pair is not None:
                    self._forward(m, step)

    def _group(self, ref, m, step):
        here = self.here
        return ref.at[:, here.at_y(step), pl.ds(0, 2)] if m == 0 else ref.at[here.at_z(step), :, pl.ds(2, 2)]

    def _forward(self, m, step):
        k = 4 * m + (step + 1)
        dst = self._group(self.pair, m, step)
        send_sem, recv_sem = self.pair_send.at[k], self.pair_recv.at[k]
        copy = send(self._group(self.slots, m, step), dst, send_sem, recv_sem, self.here.partner())
        self.forwards.append((copy, dst, k))

    def drain(self):
        for copy, dst, k in self.forwards:
            arrived(dst, self.pair_recv.at[k], self.here.partner(), self.pair_send.at[k])
            copy.wait_send()
        for first, second in self.rings:
            for r in (first, *second.values()):
                r.drain()


def first_gather_kernel(order, gate, up, n_own, g_own, down, w_out, n_all, g_all, rows_out, *refs):
    layers = down.shape[0]
    downs = refs[:layers]
    rows_v, w_v, d_v, r_load, r_out, r_send, r_recv, own_sem, d_load, d_send, d_recv, *refs = refs[layers:]
    w_send, w_recv, p_send, p_recv, n_send, n_recv, g_send, g_recv = refs
    here = Place()
    rows, cols = rows_v.shape[2], rows_v.shape[3] // 2
    mine = pl.ds(pl.multiple_of(here.dp * rows, rows), rows)
    loads = []
    for i, layer in enumerate(order):
        for j in range(CHIPS):
            at = pl.ds(pl.multiple_of(here.chip(j) * cols, cols), cols)
            for m, w in enumerate((gate, up)):
                dst = rows_v.at[i, j, :, pl.ds(m * cols, cols)]
                loads.append(pltpu.make_async_copy(w.at[layer, mine, at], dst, r_load.at[i, j, m]))
                loads[-1].start()
    owns = [
        pltpu.make_async_copy(n_own, n_all.at[0, here.x], own_sem.at[0]),
        pltpu.make_async_copy(g_own, g_all.at[0, here.x], own_sem.at[1]),
    ]
    for copy in owns:
        copy.start()
    d_loads = [pltpu.make_async_copy(down.at[l], d_v.at[l], d_load.at[l]) for l in range(layers)]
    for load in d_loads:
        load.start()
    meet(
        [here.ring(1), here.ring(-1), here.ring(2), here.partner()]
        + [here.ring_y(1), here.ring_y(-1), here.ring_z(1), here.ring_z(-1)]
    )

    def landing(i):
        return w_v.at[here.z, here.y] if i == 0 else rows_out.at[i - 1]

    row_sends, row_stores = [], []

    def exchange(i):
        for j in (2, 1, 3, 0):
            for m in range(2):
                loads[(i * CHIPS + j) * 2 + m].wait()
            if j:
                dst, device = landing(i).at[here.x], here.ring(j)
                row_sends.append(send(rows_v.at[i, j], dst, r_send.at[i, j], r_recv.at[i, j], device))
            else:
                row_stores.append(pltpu.make_async_copy(rows_v.at[i, 0], landing(i).at[here.x], r_out.at[i]))
                row_stores[-1].start()

    def exchanged(i):
        row_stores[i].wait()
        for j in (1, 3, 2):
            arrived(landing(i).at[here.chip(-j)], r_recv.at[i, j], here.ring(-j), r_send.at[i, j])

    exchange(0)
    tok_n = Tokens(here, n_own, n_all, n_send, n_recv)
    tok_g = Tokens(here, g_own, g_all, g_send, g_recv)
    members = Members(here, w_v, w_send, w_recv, w_out.at[1], p_send, p_recv)
    tok_n.start()
    exchanged(0)
    members.start()
    tok_g.start()
    copies = []
    for l in reversed(range(layers)):
        d_loads[l].wait()
        copies.append(send(d_v.at[l], downs[l].at[here.c], d_send.at[l], d_recv.at[l], here.partner()))
        d_loads[l] = pltpu.make_async_copy(d_v.at[l], downs[l].at[here.c], d_load.at[l])
        d_loads[l].start()
    members.relay_first()
    tok_n.relay()
    members.far()
    members.relay(1)
    tok_g.relay()
    for i in range(1, len(order)):
        exchange(i)
    members.done(0)
    members.relay(2)
    members.done(-1, 1, 2)
    store_w = pltpu.make_async_copy(w_v, w_out.at[0], own_sem.at[2])
    store_w.start()
    tok_n.far()
    tok_g.far()
    tok_n.finish()
    tok_g.finish()
    for i in range(1, len(order)):
        exchanged(i)
    for copy in (*copies, *row_sends):
        copy.wait_send()
    members.drain()
    for l in range(layers):
        d_loads[l].wait()
        arrived(downs[l].at[1 - here.c], d_recv.at[l], here.partner(), d_send.at[l])
    for copy in (*owns, store_w):
        copy.wait()


def first_gather(gate, up, n_own, g_own, down, order, dp, collective_id):
    tokens, width = n_own.shape
    layers, d_rows, _ = down.shape
    _, shard, ff = gate.shape
    vmem, anywhere = pl.BlockSpec(memory_space=VMEM), pl.BlockSpec(memory_space=ANY)
    bf = jnp.bfloat16
    token = jax.ShapeDtypeStruct((2, CHIPS, tokens, width), bf)
    block = (CHIPS, shard // dp, 2 * ff // CHIPS)
    slots = (RING, RING, *block)
    return pl.pallas_call(
        functools.partial(first_gather_kernel, order),
        out_shape=(
            jax.ShapeDtypeStruct((2, *slots), bf),
            token,
            token,
            jax.ShapeDtypeStruct((layers - 1, *block), bf),
        )
        + (jax.ShapeDtypeStruct((2, d_rows, width), bf),) * layers,
        in_specs=[anywhere, anywhere, vmem, vmem, anywhere],
        out_specs=(anywhere,) * (4 + layers),
        scratch_shapes=[VMEM((layers, *block), bf), VMEM(slots, bf), VMEM(down.shape, bf)]
        + [DMA((layers, CHIPS, 2)), DMA((layers,)), DMA((layers, CHIPS)), DMA((layers, CHIPS)), DMA((3,))]
        + [DMA((layers,))] * 3
        + [DMA((Members.GROUPS, 4))] * 2
        + [DMA((Members.PAIRS,))] * 2
        + [DMA((Tokens.COPIES,))] * 4,
        compiler_params=params(collective_id),
        cost_estimate=cost(45),
        name="first_gather",
    )(gate, up, n_own, g_own, down)


def transpose_into(dst, first, src, rows):
    tokens = src.shape[0]
    for k in range(src.shape[1] // rows):
        dst[k * rows : (k + 1) * rows, first : first + tokens] = src[:, k * rows : (k + 1) * rows].T


def layer_kernel(index, has_g, has_next, w, n_all, g_in, down, *refs):
    refs = list(refs)
    n_own, rows_next = (refs.pop(0), refs.pop(0)) if has_next else (None, None)
    grad, dn = refs[:2]
    n_next, w_next = refs[2:4] if has_next else (None, None)
    refs = refs[4:] if has_next else refs[2:]
    w_v, d_v, g_v, n_v, n_t, da_v, uv_v, duv_v, act_v, act_t, dn_v, gu_v, down_v, pack_v, rows_v = refs[:15]
    w_load, load, x_send, x_recv, out_sem, g_send, g_recv, n_send, n_recv = refs[15:24]
    m_send, m_recv, p_send, p_recv = refs[24:]
    here = Place()
    c = here.c
    f32 = jnp.float32
    _, _, members, rows, width = w_v.shape
    shard, ff, deep = members * rows, width // 2, pack_v.shape[2]
    d_model = g_v.shape[-1]
    tokens = g_v.shape[1] * g_v.shape[2]

    if has_next:
        rows_load = pltpu.make_async_copy(rows_next.at[index], rows_v, out_sem.at[7])
        rows_load.start()
    w_loads = [
        pltpu.make_async_copy(w.at[m, :, k], w_v.at[m, k], w_load.at[m, k]) for m in range(2) for k in range(CHIPS)
    ]
    g_load = pltpu.make_async_copy(g_in, g_v if has_g else g_v.at[0, here.x], load.at[0])
    d_loads = [
        pltpu.make_async_copy(down.at[m], d_v.at[pl.ds(m * ff // 2, ff // 2)], load.at[1 + m]) for m in range(2)
    ]
    n_loads = []
    for m, (group, core) in enumerate(((0, c), (0, 1 - c), (1, c))):
        for k in range(CHIPS):
            at = pl.ds(pl.multiple_of(2 * shard * k + shard * core, shard), shard)
            n_loads.append(
                pltpu.make_async_copy(
                    n_all.at[group, :, :, at], n_v.at[m, :, :, pl.ds(shard * k, shard)], load.at[3 + CHIPS * m + k]
                )
            )
    early, late = (w_loads, (g_load, *d_loads)) if has_g else ((g_load, *w_loads), d_loads)
    for copy in (*early, *n_loads, *late):
        copy.start()
    peers = [here.partner(), here.ring(1), here.ring(-1)]
    if has_next:
        own = pltpu.make_async_copy(n_own, n_next.at[0, here.x], out_sem.at[6])
        own.start()
        rows_load.wait()
        rows_store = pltpu.make_async_copy(rows_v, w_next.at[0, here.z, here.y], out_sem.at[7])
        rows_store.start()
        ahead = Tokens(here, n_own, n_next, n_send, n_recv)
        ahead_w = Members(here, w_next.at[0], m_send, m_recv, w_next.at[1], p_send, p_recv)
        peers += [here.ring_y(1), here.ring_y(-1), here.ring_z(1), here.ring_z(-1)]
    meet(peers)
    if not has_g:
        tok_g = Tokens(here, g_in, g_v, g_send, g_recv)
        tok_g.start()
    if has_next:
        rows_store.wait()
        ahead_w.start()
    for copy in n_loads:
        copy.wait()
    for m, first in ((0, 0), (2, tokens)):
        transpose_into(n_t, first, n_v[m].reshape(tokens, CHIPS * shard), min(128, shard))

    def uv_pass(part):
        lhs = n_v.at[part]
        step = 256 if width % 256 == 0 else width

        @pl.loop(0, width // step)
        def _(k):
            at = pl.ds(pl.multiple_of(k * step, step), step)
            rhs = w_v[part, :, :, :, at].reshape(CHIPS * shard, step)
            block = jnp.dot(lhs[...].reshape(tokens, CHIPS * shard), rhs, preferred_element_type=f32)
            uv_v[:, at] = block if part == 0 else uv_v[:, at] + block

    for copy in w_loads:
        copy.wait()
    uv_pass(0)
    if has_next:
        ahead_w.relay_first()
    uv_pass(1)
    tile = min(32, tokens)

    def act_rows(k, u, v, sig):
        act_v[0, k] = (u * sig * v).astype(jnp.bfloat16)

    def act_out():
        return send(act_v.at[0], act_v.at[1], x_send.at[1], x_recv.at[1], here.partner())

    if not has_g:
        tok_g.relay()
    if has_next:
        ahead.start()
    if not has_g:

        @pl.loop(0, tokens // tile)
        def _(k):
            at = pl.ds(pl.multiple_of(k * tile, tile), tile)
            u = uv_v[at, :ff]
            act_rows(at, u, uv_v[at, ff:], jax.nn.sigmoid(u))

        tok_g.far()
    g_load.wait()
    for copy in d_loads:
        copy.wait()
    g_here = g_v[0].reshape(tokens, d_model)
    for first in range(0, ff, 768):
        last = min(first + 768, ff)
        da_v[:, first:last] = lax.dot_general(
            g_here, d_v[first:last, :], (((1,), (1,)), ((), ())), preferred_element_type=f32
        )
    if has_next:
        ahead_w.far()

    @pl.loop(0, tokens // tile)
    def _(k):
        at = pl.ds(pl.multiple_of(k * tile, tile), tile)
        u, v, d_act = uv_v[at, :ff], uv_v[at, ff:], da_v[at, :]
        sig = jax.nn.sigmoid(u)
        if has_g:
            act_rows(at, u, v, sig)
        duv_v[0, at, :ff] = (d_act * v * sig * (1.0 + u * (1.0 - sig))).astype(jnp.bfloat16)
        duv_v[0, at, ff:] = (d_act * (u * sig)).astype(jnp.bfloat16)

    if has_next:
        ahead_w.relay(1)
        ahead.relay()

    def dn_pass(part):
        core = c if part == 0 else 1 - c

        @pl.loop(0, CHIPS)
        def _(k):
            at = pl.ds(pl.multiple_of(2 * shard * k + shard * core, shard), shard)
            block = lax.dot_general(
                duv_v[0], w_v[part, k].reshape(shard, width), (((1,), (1,)), ((), ())), preferred_element_type=f32
            )
            dn_v[:, :, at] = block.reshape(dn_v.shape[0], dn_v.shape[1], shard)

    dn_pass(0)
    x_copies = [
        send(duv_v.at[0], duv_v.at[1], x_send.at[0], x_recv.at[0], here.partner()),
        act_out(),
    ]
    if has_next:
        ahead_w.done(0)
        ahead_w.relay(2)
    dn_pass(1)
    dn_out = pltpu.make_async_copy(dn_v, dn, out_sem.at[4])
    dn_out.start()
    if has_next:
        ahead.far()

    def gu_out(m, k):
        return pltpu.make_async_copy(
            gu_v.at[k % 2],
            grad.at[:, pl.ds(pl.multiple_of(rows * k, rows), rows), pl.ds(m * ff, ff)],
            out_sem.at[k % 2],
        )

    arrived(duv_v.at[1], x_recv.at[0], here.partner(), x_send.at[0])
    for m in range(2):

        @pl.loop(0, CHIPS)
        def _(k):
            if m == 0:

                @pl.when(k >= 2)
                def _():
                    gu_out(m, k).wait()
            else:
                gu_out(m, k).wait()

            at = pl.ds(pl.multiple_of(k * shard, shard), shard)
            rhs = duv_v[:, :, m * ff : (m + 1) * ff].reshape(2 * tokens, ff)
            gu_v[k % 2] = jnp.dot(n_t[at, :], rhs, preferred_element_type=f32).reshape(members, rows, ff)
            gu_out(m, k).start()

    arrived(act_v.at[1], x_recv.at[1], here.partner(), x_send.at[1])
    if has_next:
        ahead_w.done(-1, 1, 2)
    if not has_g:
        tok_g.finish()
    half = ff // 2
    odd = half % 128
    act_at = pl.ds(pl.multiple_of(c * (half - odd), 128), half + odd)
    for m in range(2):
        transpose_into(act_t, m * tokens, act_v[m, :, act_at], 128)
    group = pack_v.shape[1]
    col = d_model // members

    def down_out(k):
        return pltpu.make_async_copy(
            pack_v.at[k % 2], grad.at[pl.ds(k * group, group), pl.ds(CHIPS * rows, deep)], out_sem.at[2 + k % 2]
        )

    @pl.loop(0, members // group)
    def _(k):
        at = pl.ds(pl.multiple_of(k * group * col, group * col), group * col)
        rhs = g_v[:, :, :, at].reshape(2 * tokens, group * col)
        down_v[...] = jnp.dot(act_t[...], rhs, preferred_element_type=f32)

        @pl.when(k >= 2)
        def _():
            down_out(k).wait()

        for d in range(group):
            for j in range(half // deep):
                at_rows = pl.ds(pl.multiple_of(c * odd + j * deep, 8), deep)
                pack_v[k % 2, d, :, j * col : (j + 1) * col] = down_v[at_rows, d * col : (d + 1) * col]
        down_out(k).start()

    for copy in x_copies:
        copy.wait_send()
    if has_next:
        ahead.finish()
        ahead_w.drain()
        own.wait()
    dn_out.wait()
    for k in range(2):
        gu_out(1, k).wait()
        down_out(k).wait()


def layer_grads(w, n_all, g, down, ahead, index, collective_id):
    _, members, _, rows, width = w.shape
    _, _, seq, d_model = n_all.shape
    tokens, shard, ff = CHIPS * seq, members * rows, width // 2
    deep = d_model // members // CHIPS
    half = ff // 2 + (ff // 2) % 128
    group = max(members // 4, 1)
    bf, f32 = jnp.bfloat16, jnp.float32
    vmem, anywhere = pl.BlockSpec(memory_space=VMEM), pl.BlockSpec(memory_space=ANY)
    has_next, has_g = bool(ahead), len(g.shape) == 4
    out = [
        jax.ShapeDtypeStruct((members, CHIPS * rows + deep, width), f32),
        jax.ShapeDtypeStruct((CHIPS, seq, d_model), f32),
    ]
    if has_next:
        out.append(jax.ShapeDtypeStruct(n_all.shape, bf))
        out.append(jax.ShapeDtypeStruct((2, members // RING, RING, *w.shape[2:]), bf))
    return pl.pallas_call(
        functools.partial(layer_kernel, index, has_g, has_next),
        out_shape=tuple(out),
        in_specs=[anywhere] * 2 + [anywhere if has_g else vmem, anywhere] + [vmem, anywhere] * has_next,
        out_specs=(anywhere,) * len(out),
        scratch_shapes=[
            VMEM((2, CHIPS, members, rows, width), bf),
            VMEM((ff, d_model), bf),
            VMEM((2, CHIPS, seq, d_model), bf),
            VMEM((3, CHIPS, seq, CHIPS * shard), bf),
            VMEM((CHIPS * shard, 2 * tokens), bf),
            VMEM((tokens, ff), f32),
            VMEM((tokens, width), f32),
            VMEM((2, tokens, width), bf),
            VMEM((2, tokens, ff), bf),
            VMEM((half, 2 * tokens), bf),
            VMEM((CHIPS, seq, d_model), f32),
            VMEM((2, members, rows, ff), f32),
            VMEM((half, group * d_model // members), f32),
            VMEM((2, group, deep, width), f32),
            VMEM((CHIPS, rows, width), bf),
            DMA((2, CHIPS)),
            DMA((3 + 3 * CHIPS,)),
            DMA((2,)),
            DMA((2,)),
            DMA((8,)),
        ]
        + [DMA((Tokens.COPIES,))] * 4
        + [DMA((Members.GROUPS, 4))] * 2
        + [DMA((Members.PAIRS,))] * 2,
        compiler_params=params(collective_id, 60 * 1024 * 1024),
        cost_estimate=cost(50),
        name="layer_grads",
    )(w, n_all, g, down, *ahead)


class RingSum:
    def __init__(self, device, block, buffers, send_sem, recv_sem):
        self.device, self.block = device, block
        self.from_left, self.from_right, self.in_left, self.in_right = buffers
        self.send_sem, self.recv_sem = send_sem, recv_sem
        self.copies = []

    def _half(self, ref, part):
        half = ref.shape[-2] // 2
        return ref.at[*[slice(None)] * (len(ref.shape) - 2), pl.ds(part * half, half)]

    def _send(self, k, src, dst, step):
        self.copies.append(send(src, dst, self.send_sem.at[k], self.recv_sem.at[k], self.device(step)))

    def _arrived(self, k, ref, step):
        arrived(ref, self.recv_sem.at[k], self.device(step), self.send_sem.at[k])

    def start(self):
        self._send(0, self.block(2, 0), self.from_left, 1)
        self._send(1, self.block(2, 1), self.from_right, -1)
        self._send(2, self.block(1, 1), self._half(self.in_left, 1), 1)
        self._send(3, self.block(-1, 0), self._half(self.in_right, 0), -1)

    def pass_right(self):
        self._arrived(0, self.from_left, -1)
        block = self.block(1, 0)
        block[...] = block[...] + self.from_left[...]
        self._send(4, block, self._half(self.in_left, 0), 1)

    def pass_left(self):
        self._arrived(1, self.from_right, 1)
        block = self.block(-1, 1)
        block[...] = block[...] + self.from_right[...]
        self._send(5, block, self._half(self.in_right, 1), -1)

    def total(self):
        self._arrived(2, self._half(self.in_left, 1), -1)
        self._arrived(3, self._half(self.in_right, 0), 1)
        self._arrived(4, self._half(self.in_left, 0), -1)
        self._arrived(5, self._half(self.in_right, 1), 1)
        return self.block(0, None)[...] + self.in_left[...] + self.in_right[...]

    def drain(self):
        for copy in self.copies:
            copy.wait_send()


def sum_scratch(lead, rows, width):
    half, whole = VMEM((*lead, rows // 2, width), jnp.float32), VMEM((*lead, rows, width), jnp.float32)
    return [half, half, whole, whole]


def dn_ring(here, dn_v, buffers, send_sem, recv_sem):
    half = dn_v.shape[1] // 2

    def block(step, part):
        at = here.chip(step)
        return dn_v.at[at] if part is None else dn_v.at[at, pl.ds(part * half, half)]

    return RingSum(here.ring, block, buffers, send_sem, recv_sem)


def dn_loads(here, dn, dn_v, load_sem):
    loads = []
    for k, step in enumerate((2, 1, -1, 0)):
        loads.append(pltpu.make_async_copy(dn.at[here.chip(step)], dn_v.at[here.chip(step)], load_sem.at[k]))
        loads[k].start()
    return loads


def g_step(d_norm, g, h):
    x_full = h[...].astype(jnp.float32)
    inv_rms = lax.rsqrt(jnp.mean(x_full * x_full, axis=-1, keepdims=True) + EPS)
    norm_f = x_full * inv_rms
    return g[...] + inv_rms * (d_norm - norm_f * jnp.mean(d_norm * norm_f, axis=-1, keepdims=True))


def next_g_kernel(dn, g, h, g_out, g_bf, dn_v, *refs):
    load_sem, send_sem, recv_sem = refs[4:]
    here = Place()
    loads = dn_loads(here, dn, dn_v, load_sem)
    meet([here.ring(1), here.ring(-1)])
    ring = dn_ring(here, dn_v, refs[:4], send_sem, recv_sem)
    for load in loads:
        load.wait()
    ring.start()
    ring.pass_right()
    ring.pass_left()
    g_new = g_step(ring.total(), g, h)
    g_out[...] = g_new
    g_bf[...] = g_new.astype(jnp.bfloat16)
    ring.drain()


def next_g(dn, g, h, collective_id):
    vmem = pl.BlockSpec(memory_space=VMEM)
    return pl.pallas_call(
        next_g_kernel,
        out_shape=(jax.ShapeDtypeStruct(g.shape, g.dtype), jax.ShapeDtypeStruct(g.shape, jnp.bfloat16)),
        in_specs=[pl.BlockSpec(memory_space=ANY), vmem, vmem],
        out_specs=(vmem,) * 2,
        scratch_shapes=[VMEM(dn.shape, dn.dtype)] + sum_scratch((), *g.shape) + [DMA((4,)), DMA((6,)), DMA((6,))],
        compiler_params=params(collective_id),
        cost_estimate=cost(42),
        name="next_g",
    )(dn, g, h)


class MemberSum:
    def __init__(self, here, grad_v, buffers, send_sem, recv_sem):
        rows = grad_v.shape[2] // 2
        self.rows = rows

        def span(first, part):
            return pl.ds(first, rows) if part is None else pl.ds(first + part * rows // 2, rows // 2)

        def block_a1(step, part):
            return grad_v.at[:, here.at_y(step), span(0, part)]

        def block_b1(step, part):
            return grad_v.at[here.at_z(step), :, span(rows, part)]

        def block_a2(step, part):
            return grad_v.at[here.at_z(step), here.y, span(0, part)]

        def block_b2(step, part):
            return grad_v.at[here.z, here.at_y(step), span(rows, part)]

        devices = (here.ring_y, here.ring_z, here.ring_z, here.ring_y)
        blocks = (block_a1, block_b1, block_a2, block_b2)
        self.a1, self.b1, self.a2, self.b2 = (
            RingSum(*each) for each in zip(devices, blocks, buffers, send_sem, recv_sem)
        )

    def start(self):
        self.a1.start()
        self.b1.start()

    def pass_first(self):
        for ring in (self.a1, self.b1):
            ring.pass_right()
        for ring in (self.a1, self.b1):
            ring.pass_left()

    def second(self):
        for first, second in ((self.a1, self.a2), (self.b1, self.b2)):
            first.block(0, None)[...] = first.total()
            second.start()

    def finish(self, piece):
        for ring in (self.a2, self.b2):
            ring.pass_right()
            ring.pass_left()
        piece[: self.rows] = self.a2.total()
        piece[self.rows :] = self.b2.total()

    def drain(self):
        for ring in (self.a1, self.b1, self.a2, self.b2):
            ring.drain()


def last_sum_kernel(n_order, dn, g, h, grad, *refs):
    g_out, piece, dn_v, grad_v = refs[n_order : n_order + 4]
    refs = refs[n_order + 4 :]
    buffers = [refs[4 * k : 4 * k + 4] for k in range(5)]
    load_sem, grad_sem, send_sem, recv_sem = refs[20:]
    here = Place()
    rows = grad.shape[2] // 2
    loads = dn_loads(here, dn, dn_v, load_sem)
    grad_loads = []
    for k, step in enumerate((2, 1, -1, 0)):
        for m in range(2):
            at = (slice(None), here.at_y(step)) if m == 0 else (here.at_z(step), slice(None))
            part = pl.ds(m * rows, rows)
            load = pltpu.make_async_copy(grad.at[*at, part], grad_v.at[*at, part], grad_sem.at[m, k])
            load.start()
            grad_loads.append(load)

    meet(
        [here.ring(1), here.ring(-1), here.ring_y(1), here.ring_y(-1), here.ring_z(1), here.ring_z(-1)]
    )
    x = dn_ring(here, dn_v, buffers[0], send_sem.at[0], recv_sem.at[0])
    members = MemberSum(here, grad_v, buffers[1:], [send_sem.at[k] for k in range(1, 5)], [recv_sem.at[k] for k in range(1, 5)])
    for load in grad_loads:
        load.wait()
    members.start()
    for load in loads:
        load.wait()
    x.start()
    x.pass_right()
    x.pass_left()
    members.pass_first()
    g_out[...] = g_step(x.total(), g, h).astype(g_out.dtype)
    members.second()
    members.finish(piece)
    x.drain()
    members.drain()


def last_sum(dn, g, h, grad, order, collective_id):
    vmem, anywhere = pl.BlockSpec(memory_space=VMEM), pl.BlockSpec(memory_space=ANY)
    _, _, rows, width = grad.shape
    return pl.pallas_call(
        functools.partial(last_sum_kernel, len(order)),
        out_shape=(jax.ShapeDtypeStruct(g.shape, jnp.bfloat16), jax.ShapeDtypeStruct((rows, width), grad.dtype)),
        in_specs=[anywhere, vmem, vmem, anywhere] + [anywhere] * len(order),
        out_specs=(vmem,) * 2,
        scratch_shapes=[VMEM(dn.shape, dn.dtype), VMEM(grad.shape, grad.dtype)]
        + sum_scratch((), *g.shape)
        + sum_scratch((RING,), rows // 2, width) * 2
        + sum_scratch((), rows // 2, width) * 2
        + [DMA((4,)), DMA((2, 4)), DMA((5, 6)), DMA((5, 6))],
        compiler_params=params(collective_id, 60 * 1024 * 1024),
        cost_estimate=cost(100),
        name="last_sum",
    )(dn, g, h, grad, *order)


def gather_rows_kernel(n_order, rows, *refs):
    out, send_sem, recv_sem, own_sem = refs[n_order:]
    here = Place()
    own = pltpu.make_async_copy(rows, out.at[here.z, here.y], own_sem.at[0])
    own.start()
    meet([here.ring_y(1), here.ring_y(-1), here.ring_z(1), here.ring_z(-1)])
    own.wait()
    members = Members(here, out, send_sem, recv_sem)
    members.start()
    members.relay_first()
    members.far()
    members.relay(1)
    members.relay(2)
    members.done(0, -1, 1, 2)
    members.drain()


def gather_rows(rows, order, collective_id):
    anywhere = pl.BlockSpec(memory_space=ANY)
    return pl.pallas_call(
        functools.partial(gather_rows_kernel, len(order)),
        out_shape=jax.ShapeDtypeStruct((RING, RING, *rows.shape), rows.dtype),
        in_specs=[pl.BlockSpec(memory_space=VMEM)] + [anywhere] * len(order),
        out_specs=anywhere,
        scratch_shapes=[DMA((Members.GROUPS, 4)), DMA((Members.GROUPS, 4)), DMA((1,))],
        compiler_params=params(collective_id),
        cost_estimate=cost(100),
        name="gather_rows",
    )(rows, *order)


def grad_rows_kernel(count, *refs):
    pieces, outs, (send_sem, recv_sem, local_sem) = refs[:count], refs[-3 - count : -3], refs[-3:]
    here = Place()
    cols = pieces[0].shape[1] // 2
    rows = pieces[0].shape[0] // 6

    def landing(i, m, chip):
        at = pl.ds(pl.multiple_of((2 * m + chip // 2) * rows, rows), rows)
        return outs[i].at[at, pl.ds(pl.multiple_of(chip % 2 * cols, cols), cols)]

    def part(i, m, chip):
        return pieces[i].at[pl.ds(pl.multiple_of(chip * rows, rows), rows), pl.ds(m * cols, cols)]

    down = pl.ds(4 * rows, 2 * rows)
    local = []
    for i in range(count):
        local.append(pltpu.make_async_copy(pieces[i].at[down], outs[i].at[down], local_sem.at[i, 2]))
        for m in range(2):
            local.append(pltpu.make_async_copy(part(i, m, here.x), landing(i, m, here.x), local_sem.at[i, m]))
    for copy in local:
        copy.start()
    meet([here.ring(j) for j in range(1, CHIPS)])
    copies = []
    for i in range(count):
        for j in (2, 1, 3):
            for m in range(2):
                src, dst = part(i, m, here.chip(j)), landing(i, m, here.x)
                copies.append(send(src, dst, send_sem.at[i, j, m], recv_sem.at[i, j, m], here.ring(j)))
    for i in range(count):
        for j in (1, 3, 2):
            for m in range(2):
                sems = recv_sem.at[i, j, m], here.ring(-j), send_sem.at[i, j, m]
                arrived(landing(i, m, here.chip(-j)), *sems)
    for copy in copies:
        copy.wait_send()
    for copy in local:
        copy.wait()


def grad_rows(pieces, order, collective_id):
    vmem = pl.BlockSpec(memory_space=VMEM)
    n = len(pieces)
    return pl.pallas_call(
        functools.partial(grad_rows_kernel, n),
        out_shape=tuple(jax.ShapeDtypeStruct(piece.shape, piece.dtype) for piece in pieces),
        in_specs=[vmem] * n + [pl.BlockSpec(memory_space=ANY)] * len(order),
        out_specs=(vmem,) * n,
        scratch_shapes=[DMA((n, CHIPS, 2)), DMA((n, CHIPS, 2)), DMA((n, 3))],
        compiler_params=params(collective_id),
        cost_estimate=cost(12),
        name="grad_rows",
    )(*pieces, *order)


PARTS = 4


def place_kernel(layer, grad, *refs):
    gate, up, down, buf, d_buf, pack, load_sem, d_sem, store_sem = refs[-9:]
    members, rows, half = grad.shape[0], grad.shape[1] // 6, grad.shape[2]
    part = max(members // PARTS, 1)
    parts = members // part
    d_load = pltpu.make_async_copy(grad.at[:, pl.ds(4 * rows, 2 * rows)], d_buf, d_sem.at[0])
    d_load.start()
    loads = []
    for m in range(2):
        for k in range(parts):
            at = pl.ds(k * part, part)
            for h in range(2):
                src = grad.at[at, pl.ds((2 * m + h) * rows, rows)]
                load = pltpu.make_async_copy(src, buf.at[m, at, :, pl.ds(h * half, half)], load_sem.at[m, k, h])
                load.start()
                loads.append(load)
    d_load.wait()
    stores = []
    for m, out in enumerate((gate, up)):
        for k in range(parts):
            at = pl.ds(k * part, part)
            for h in range(2):
                loads[(m * parts + k) * 2 + h].wait()
            store = pltpu.make_async_copy(buf.at[m, at], out.at[layer, at], store_sem.at[m, k])
            store.start()
            stores.append(store)
    col, deep = down.shape[2] // members, 2 * rows

    @pl.loop(0, half // col)
    def _(j):
        at = pl.ds(pl.multiple_of(j * deep, deep), deep)
        cols = pl.ds(pl.multiple_of(j * col, col), col)
        for d in range(members):
            pack[at, d * col : (d + 1) * col] = d_buf[d, :, cols]

    store = pltpu.make_async_copy(pack, down.at[layer], d_sem.at[1])
    store.start()
    stores.append(store)
    for store in stores:
        store.wait()


def place(grad, layer, stacks, order, shapes):
    members, rows, half = grad.shape
    anywhere = pl.BlockSpec(memory_space=ANY)
    return pl.pallas_call(
        functools.partial(place_kernel, layer),
        out_shape=shapes,
        in_specs=[anywhere] * (1 + len(stacks) + len(order)),
        out_specs=(anywhere,) * 3,
        input_output_aliases={1 + m: m for m in range(len(stacks))},
        scratch_shapes=[
            VMEM((2, members, rows // 6, 2 * half), grad.dtype),
            VMEM((members, rows // 3, half), grad.dtype),
            VMEM(shapes[2].shape[1:], grad.dtype),
            DMA((2, PARTS, 2)),
            DMA((2,)),
            DMA((2, PARTS)),
        ],
        compiler_params=pltpu.CompilerParams(vmem_limit_bytes=58 * 1024 * 1024),
        cost_estimate=cost(13),
        name="place",
    )(grad, *stacks, *order)


def gather_dp(value):
    return lax.all_gather(value[None], "dp", axis=0, tiled=True)


def scatter_dp(value):
    members, *piece = value.shape
    value = value.reshape(members * piece[0], *piece[1:])
    return lax.psum_scatter(value, "dp", scatter_dimension=0, tiled=True)


def solution(mesh):
    dp = mesh.shape["dp"]
    tok_spec = P(("dp", "fsdp"))
    stack_spec = P(None, ("dp", "fsdp"))
    weight_spec = P(None, "fsdp")

    def local_backward(h_saved, grad_out, gate_sh, up_sh, down_sh):
        layers = h_saved.shape[0]
        b_loc, seq, width = grad_out.shape
        tokens = b_loc * seq
        h = h_saved.reshape(layers, tokens, width)
        x_full = h.astype(jnp.float32)
        inv_rms = lax.rsqrt(jnp.mean(x_full * x_full, axis=-1, keepdims=True) + EPS)
        n = (x_full * inv_rms).astype(jnp.bfloat16)
        g_bf = grad_out.reshape(tokens, width)
        g = g_bf.astype(jnp.float32)
        last = layers - 1
        ids = iter(range(1, 100))

        order = tuple(reversed(range(layers)))
        w, n_all, g_in, rows, *down = first_gather(
            gate_sh, up_sh, n[last], g_bf, down_sh, order, dp, next(ids)
        )
        pieces = {}
        for k, layer in enumerate(order):
            ahead = (n[layer - 1], rows) if layer else ()
            w = w.reshape(2, dp, *w.shape[3:])
            grad, dn, *following = layer_grads(w, n_all, g_in, down[layer], ahead, k, next(ids))
            if layer:
                pieces[layer] = scatter_dp(grad)
                n_all, w = following
                g, g_in = next_g(dn, g, h[layer], next(ids))
        rows = {}
        (rows[last],) = grad_rows((pieces[last],), (dn,), next(ids))
        gathered = {last: gather_dp(rows[last])}
        grad = grad.reshape(dp // RING, RING, *grad.shape[1:])
        d_h0, pieces[0] = last_sum(dn, g, h[0], grad, (rows[last],), next(ids))
        rows[1], rows[0] = grad_rows((pieces[1], pieces[0]), (), next(ids))
        gathered[0] = gather_dp(rows[0])
        mine = rows[1].reshape(4, -1, rows[1].shape[1])
        all_rows = gather_rows(mine, (), next(ids))
        gathered[1] = all_rows.reshape(gathered[0].shape)

        rows = (layers, dp, gate_sh.shape[1] // dp, gate_sh.shape[2])
        shapes = tuple(jax.ShapeDtypeStruct(shape, jnp.float32) for shape in (rows, rows, down_sh.shape))
        stacks = ()
        for layer in order:
            stacks = place(gathered[layer], layer, stacks, (all_rows,) if layer == last else (), shapes)
        gate, up, down_grad = stacks
        return gate.reshape(gate_sh.shape), up.reshape(up_sh.shape), down_grad, d_h0.reshape(b_loc, seq, width)

    return jax.shard_map(
        local_backward,
        mesh=mesh,
        in_specs=(stack_spec, tok_spec, weight_spec, weight_spec, weight_spec),
        out_specs=(weight_spec, weight_spec, weight_spec, tok_spec),
        check_vma=False,
    )
```

```python
import functools

import jax
import jax.numpy as jnp
from jax import lax
from jax.experimental import pallas as pl
from jax.experimental.pallas import tpu as pltpu
from jax.sharding import PartitionSpec as P


EPS = 1e-5
CHIPS = 4
RING = 4
MESH = pl.DeviceIdType.MESH
VMEM = pltpu.VMEM
ANY = pl.ANY
DMA = pltpu.SemaphoreType.DMA


class Place:
    def __init__(self):
        self.dp = lax.axis_index("dp")
        self.f = lax.axis_index("fsdp")
        self.x, self.c = self.f // 2, self.f % 2
        self.z, self.y = self.dp // RING, self.dp % RING

    def chip(self, step):
        return (self.x + step) % CHIPS

    def ring(self, step):
        return (self.dp, 2 * self.chip(step) + self.c)

    def partner(self):
        return (self.dp, 2 * self.x + (1 - self.c))

    def at_y(self, step):
        return (self.y + step) % RING

    def at_z(self, step):
        return (self.z + step) % RING

    def ring_y(self, step):
        return (self.z * RING + self.at_y(step), self.f)

    def ring_z(self, step):
        return (self.at_z(step) * RING + self.y, self.f)


def meet(peers):
    barrier = pltpu.get_barrier_semaphore()
    for peer in peers:
        pl.semaphore_signal(barrier, inc=1, device_id=peer, device_id_type=MESH)
    pl.semaphore_wait(barrier, len(peers))


def send(src, dst, send_sem, recv_sem, device):
    copy = pltpu.make_async_remote_copy(
        src_ref=src, dst_ref=dst, send_sem=send_sem, recv_sem=recv_sem, device_id=device, device_id_type=MESH
    )
    copy.start()
    return copy


def arrived(ref, recv_sem, device, send_sem):
    pltpu.make_async_remote_copy(
        src_ref=ref, dst_ref=ref, send_sem=send_sem, recv_sem=recv_sem, device_id=device, device_id_type=MESH
    ).wait_recv()


def params(collective_id, vmem=None):
    return pltpu.CompilerParams(collective_id=collective_id, has_side_effects=True, vmem_limit_bytes=vmem)


def cost(us):
    return pl.CostEstimate(flops=int(us * 4.0e6), bytes_accessed=0, transcendentals=0)


class Exchange:
    COPIES = 8

    def __init__(self, here, part, landing, relays, send_sem, recv_sem):
        self.here, self.part, self.landing, self.relays = here, part, landing, relays
        self.send_sem, self.recv_sem = send_sem, recv_sem
        self.copies = []

    def _send(self, k, src, dst, step):
        self.copies.append(send(src, dst, self.send_sem.at[k], self.recv_sem.at[k], self.here.ring(step)))

    def _arrived(self, k, ref, step):
        arrived(ref, self.recv_sem.at[k], self.here.ring(step), self.send_sem.at[k])

    def start(self):
        for m, step in enumerate((1, -1)):
            self._send(4 + m, self.part(2, m), self.relays.at[m], step)
        for k, step in enumerate((1, -1)):
            for m in range(2):
                self._send(2 * k + m, self.part(step, m), self.landing(self.here.x, m), step)

    def relay(self):
        for m, step in enumerate((1, -1)):
            self._arrived(4 + m, self.relays.at[m], -step)
            self._send(6 + m, self.relays.at[m], self.landing(self.here.chip(-step), m), step)

    def finish(self):
        for k, step in enumerate((1, -1)):
            for m in range(2):
                self._arrived(2 * k + m, self.landing(self.here.chip(-step), m), -step)
        for m, step in enumerate((1, -1)):
            self._arrived(6 + m, self.landing(self.here.chip(2), m), -step)
        for copy in self.copies:
            copy.wait_send()


def weight_rows_kernel(layers, rows, cols, gate, up, first, others, buf, relays, load_sem, out_sem, send_sem, recv_sem):
    outs = [first] + [others.at[k] for k in range(len(layers) - 1)]
    here = Place()
    mine = pl.ds(pl.multiple_of(here.dp * rows, rows), rows)
    steps = (2, 1, -1, 0)
    loads = {}
    for i, layer in enumerate(layers):
        for j, step in enumerate(steps):
            at = pl.ds(pl.multiple_of(here.chip(step) * cols, cols), cols)
            for m, w in enumerate((gate, up)):
                load = pltpu.make_async_copy(w.at[layer, mine, at], buf.at[i, m, j], load_sem.at[i, m, j])
                load.start()
                loads[i, m, j] = load
    meet([here.ring(1), here.ring(-1)])
    exchanges, stores = [], []
    for i in range(len(layers)):
        for m in range(2):
            for j in range(CHIPS):
                loads[i, m, j].wait()

        def part(step, m, i=i):
            return buf.at[i, m, steps.index(step)]

        def landing(chip, m, i=i):
            return outs[i].at[chip, :, pl.ds(m * cols, cols)]

        exchanges.append(Exchange(here, part, landing, relays.at[i], send_sem.at[i], recv_sem.at[i]))
        exchanges[i].start()
        for m in range(2):
            stores.append(pltpu.make_async_copy(part(0, m), landing(here.x, m), out_sem.at[i, m]))
            stores[-1].start()
    for exchange in exchanges:
        exchange.relay()
    for exchange in exchanges:
        exchange.finish()
    for store in stores:
        store.wait()


def weight_rows(gate, up, layers, dp, collective_id):
    _, shard, ff = gate.shape
    rows, cols = shard // dp, ff // CHIPS
    n = len(layers)
    block = (CHIPS, rows, 2 * cols)
    return pl.pallas_call(
        functools.partial(weight_rows_kernel, layers, rows, cols),
        out_shape=(jax.ShapeDtypeStruct(block, gate.dtype), jax.ShapeDtypeStruct((n - 1, *block), gate.dtype)),
        in_specs=[pl.BlockSpec(memory_space=ANY)] * 2,
        out_specs=(pl.BlockSpec(memory_space=ANY),) * 2,
        scratch_shapes=[
            VMEM((n, 2, CHIPS, rows, cols), gate.dtype),
            VMEM((n, 2, rows, cols), gate.dtype),
            DMA((n, 2, CHIPS)),
            DMA((n, 2)),
            DMA((n, Exchange.COPIES)),
            DMA((n, Exchange.COPIES)),
        ],
        compiler_params=params(collective_id),
        cost_estimate=cost(12),
        name="weight_rows",
    )(gate, up)


class Ring:
    def __init__(self, device, at, block, own, send_sem, recv_sem):
        self.device, self.at, self.block, self.own = device, at, block, own
        self.send_sem, self.recv_sem = send_sem, recv_sem
        self.copies = []

    def _send(self, k, src, dst, step):
        self.copies.append(send(src, dst, self.send_sem(k), self.recv_sem(k), self.device(step)))

    def _arrived(self, k, ref, step):
        arrived(ref, self.recv_sem(k), self.device(step), self.send_sem(k))

    def start(self):
        here = self.block(self.at(0), None)
        self._send(0, self.own, here, 1)
        self._send(1, self.own, here, -1)

    def relay_right(self):
        self._arrived(0, self.block(self.at(-1), None), -1)
        half = self.block(self.at(-1), 0)
        self._send(2, half, half, 1)

    def relay_left(self):
        self._arrived(1, self.block(self.at(1), None), 1)
        half = self.block(self.at(1), 1)
        self._send(3, half, half, -1)

    def finish(self):
        self._arrived(2, self.block(self.at(2), 0), -1)
        self._arrived(3, self.block(self.at(2), 1), 1)

    def drain(self):
        for copy in self.copies:
            copy.wait_send()


class Tokens:
    COPIES = 8

    def __init__(self, here, own, out, send_sem, recv_sem):
        half = out.shape[2] // 2

        def block(chip, part):
            return out.at[0, chip] if part is None else out.at[0, chip, pl.ds(part * half, half)]

        self.here, self.own, self.out = here, own, out
        self.send_sem, self.recv_sem = send_sem, recv_sem
        self.ring = Ring(here.ring, here.chip, block, own, lambda k: send_sem.at[k], lambda k: recv_sem.at[k])
        self.pairs = []

    def _pair(self, k, src, chip):
        dst = self.out.at[1, chip]
        copy = send(src, dst, self.send_sem.at[4 + k], self.recv_sem.at[4 + k], self.here.partner())
        self.pairs.append((k, chip, copy))

    def start(self):
        self.ring.start()
        self._pair(0, self.own, self.here.x)

    def relay(self):
        left, right = self.here.chip(-1), self.here.chip(1)
        self.ring.relay_right()
        self._pair(1, self.out.at[0, left], left)
        self.ring.relay_left()
        self._pair(2, self.out.at[0, right], right)

    def far(self):
        far = self.here.chip(2)
        self.ring.finish()
        self._pair(3, self.out.at[0, far], far)

    def finish(self):
        for k, chip, copy in self.pairs:
            arrived(self.out.at[1, chip], self.recv_sem.at[4 + k], self.here.partner(), self.send_sem.at[4 + k])
            copy.wait_send()
        self.ring.drain()


class Members:
    def __init__(self, here, slots, send_sem, recv_sem):
        self.here, self.slots, self.send_sem, self.recv_sem = here, slots, send_sem, recv_sem
        a1, b1 = self._ring(0, 0, True, here.z), self._ring(1, 2, False, here.y)
        a2 = {step: self._ring(2 + k, 0, False, here.at_y(step)) for k, step in enumerate((0, -1, 1, 2))}
        b2 = {step: self._ring(6 + k, 2, True, here.at_z(step)) for k, step in enumerate((0, -1, 1, 2))}
        self.pairs = ((a1, a2), (b1, b2))

    def _ring(self, group, first, along_y, fixed):
        def block(at, part):
            k = pl.ds(first, 2) if part is None else pl.ds(first + part, 1)
            return self.slots.at[fixed, at, k] if along_y else self.slots.at[at, fixed, k]

        here = self.here
        device, at = (here.ring_y, here.at_y) if along_y else (here.ring_z, here.at_z)
        sems = (lambda k: self.send_sem.at[group, k]), (lambda k: self.recv_sem.at[group, k])
        return Ring(device, at, block, block(at(0), None), *sems)

    def start(self):
        for first, second in self.pairs:
            first.start()
        for first, second in self.pairs:
            second[0].start()

    def relay_first(self):
        for first, second in self.pairs:
            first.relay_right()
            second[-1].start()
        for first, second in self.pairs:
            first.relay_left()
            second[1].start()
        for _, second in self.pairs:
            second[0].relay_right()
            second[0].relay_left()

    def finish(self):
        for first, second in self.pairs:
            first.finish()
            second[2].start()
        for step in (-1, 1, 2):
            for _, second in self.pairs:
                second[step].relay_right()
                second[step].relay_left()
        for step in (0, -1, 1, 2):
            for _, second in self.pairs:
                second[step].finish()

    def drain(self):
        for first, second in self.pairs:
            for r in (first, *second.values()):
                r.drain()


def first_gather_kernel(rows, n_own, g_own, down, w_out, n_all, g_all, *refs):
    layers = down.shape[0]
    downs = refs[:layers]
    w_v, d_v, w_load, own_sem, d_load, d_send, d_recv, w_send, w_recv, n_send, n_recv, g_send, g_recv = refs[layers:]
    here = Place()
    load_w = pltpu.make_async_copy(rows, w_v.at[here.z, here.y], w_load.at[0])
    load_w.start()
    owns = [
        pltpu.make_async_copy(n_own, n_all.at[0, here.x], own_sem.at[0]),
        pltpu.make_async_copy(g_own, g_all.at[0, here.x], own_sem.at[1]),
    ]
    for copy in owns:
        copy.start()
    loads = [pltpu.make_async_copy(down.at[l], d_v.at[l], d_load.at[l]) for l in range(layers)]
    for load in loads:
        load.start()
    meet(
        [here.ring(1), here.ring(-1), here.partner()]
        + [here.ring_y(1), here.ring_y(-1), here.ring_z(1), here.ring_z(-1)]
    )

    members = Members(here, w_v, w_send, w_recv)
    tok_n = Tokens(here, n_own, n_all, n_send, n_recv)
    tok_g = Tokens(here, g_own, g_all, g_send, g_recv)
    tok_n.start()
    tok_g.start()
    load_w.wait()
    members.start()
    copies = []
    for l in reversed(range(layers)):
        loads[l].wait()
        copies.append(send(d_v.at[l], downs[l].at[here.c], d_send.at[l], d_recv.at[l], here.partner()))
        loads[l] = pltpu.make_async_copy(d_v.at[l], downs[l].at[here.c], d_load.at[l])
        loads[l].start()
    members.relay_first()
    tok_n.relay()
    tok_g.relay()
    members.finish()
    store_w = pltpu.make_async_copy(w_v, w_out, w_load.at[0])
    store_w.start()
    tok_n.far()
    tok_g.far()
    tok_n.finish()
    tok_g.finish()
    members.drain()
    for copy in copies:
        copy.wait_send()
    for l in range(layers):
        loads[l].wait()
        arrived(downs[l].at[1 - here.c], d_recv.at[l], here.partner(), d_send.at[l])
    for copy in owns:
        copy.wait()
    store_w.wait()


def first_gather(rows, n_own, g_own, down, collective_id):
    tokens, width = n_own.shape
    layers, d_rows, _ = down.shape
    vmem, anywhere = pl.BlockSpec(memory_space=VMEM), pl.BlockSpec(memory_space=ANY)
    bf = jnp.bfloat16
    token = jax.ShapeDtypeStruct((2, CHIPS, tokens, width), bf)
    weight = (RING, RING, *rows.shape)
    return pl.pallas_call(
        first_gather_kernel,
        out_shape=(jax.ShapeDtypeStruct(weight, bf), token, token)
        + (jax.ShapeDtypeStruct((2, d_rows, width), bf),) * layers,
        in_specs=[anywhere, vmem, vmem, anywhere],
        out_specs=(anywhere,) * (3 + layers),
        scratch_shapes=[VMEM(weight, bf), VMEM(down.shape, bf), DMA((1,)), DMA((2,))]
        + [DMA((layers,))] * 3
        + [DMA((10, 4))] * 2
        + [DMA((Tokens.COPIES,))] * 4,
        compiler_params=params(collective_id),
        cost_estimate=cost(45),
        name="first_gather",
    )(rows, n_own, g_own, down)


def transpose_into(dst, first, src, rows):
    tokens = src.shape[0]
    for k in range(src.shape[1] // rows):
        dst[k * rows : (k + 1) * rows, first : first + tokens] = src[:, k * rows : (k + 1) * rows].T


def layer_kernel(index, has_g, has_next, n_order, w, n_all, g_in, down, *refs):
    refs = list(refs)
    n_own = refs.pop(0) if has_next else None
    refs = refs[n_order:]
    grad, grad_down, dn = refs[:3]
    n_next = refs[3] if has_next else None
    refs = refs[4:] if has_next else refs[3:]
    w_v, d_v, g_v, n_v, n_t, da_v, uv_v, duv_v, act_v, act_t, dn_v, gu_v, down_v, pack_v = refs[:14]
    w_load, load, w_send, w_recv, x_send, x_recv, out_sem, g_send, g_recv, n_send, n_recv = refs[14:]
    here = Place()
    c = here.c
    f32 = jnp.float32
    _, _, members, rows, width = w_v.shape
    shard, ff, deep = members * rows, width // 2, pack_v.shape[2]
    d_model = g_v.shape[-1]
    tokens = g_v.shape[1] * g_v.shape[2]

    w_loads = [pltpu.make_async_copy(w.at[:, index, k], w_v.at[0, k], w_load.at[k]) for k in range(CHIPS)]
    g_load = pltpu.make_async_copy(g_in, g_v if has_g else g_v.at[0, here.x], load.at[0])
    d_loads = [
        pltpu.make_async_copy(down.at[m], d_v.at[pl.ds(m * ff // 2, ff // 2)], load.at[1 + m]) for m in range(2)
    ]
    n_loads = []
    for m, (group, core) in enumerate(((0, c), (0, 1 - c), (1, c))):
        for k in range(CHIPS):
            at = pl.ds(pl.multiple_of(2 * shard * k + shard * core, shard), shard)
            n_loads.append(
                pltpu.make_async_copy(
                    n_all.at[group, :, :, at], n_v.at[m, :, :, pl.ds(shard * k, shard)], load.at[3 + CHIPS * m + k]
                )
            )
    for copy in (*w_loads, g_load, *d_loads, *n_loads):
        copy.start()
    if has_next:
        own = pltpu.make_async_copy(n_own, n_next.at[0, here.x], out_sem.at[6])
        own.start()
        ahead = Tokens(here, n_own, n_next, n_send, n_recv)
    meet([here.partner(), here.ring(1), here.ring(-1)])
    if not has_g:
        tok_g = Tokens(here, g_in, g_v, g_send, g_recv)
        tok_g.start()
    w_copies = []
    for k in range(CHIPS):
        w_loads[k].wait()
        w_copies.append(send(w_v.at[0, k], w_v.at[1, k], w_send.at[k], w_recv.at[k], here.partner()))

    def da_pass():
        g_load.wait()
        for copy in d_loads:
            copy.wait()
        g_here = g_v[0].reshape(tokens, d_model)
        for first in range(0, ff, 768):
            last = min(first + 768, ff)
            da_v[:, first:last] = lax.dot_general(
                g_here, d_v[first:last, :], (((1,), (1,)), ((), ())), preferred_element_type=f32
            )

    if has_g:
        da_pass()
    for copy in n_loads:
        copy.wait()
    for m, first in ((0, 0), (2, tokens)):
        transpose_into(n_t, first, n_v[m].reshape(tokens, CHIPS * shard), min(128, shard))

    def uv_pass(part):
        lhs = n_v.at[part]
        step = 256 if width % 256 == 0 else width

        @pl.loop(0, width // step)
        def _(k):
            at = pl.ds(pl.multiple_of(k * step, step), step)
            rhs = w_v[part, :, :, :, at].reshape(CHIPS * shard, step)
            block = jnp.dot(lhs[...].reshape(tokens, CHIPS * shard), rhs, preferred_element_type=f32)
            uv_v[:, at] = block if part == 0 else uv_v[:, at] + block

    uv_pass(0)
    if not has_g:
        tok_g.relay()
    if has_next:
        ahead.start()
    for k in range(CHIPS):
        arrived(w_v.at[1, k], w_recv.at[k], here.partner(), w_send.at[k])
    uv_pass(1)
    tile = min(32, tokens)

    def act_rows(at, u, v, sig):
        act_v[0, at] = (u * sig * v).astype(jnp.bfloat16)

    if not has_g:

        @pl.loop(0, tokens // tile)
        def _(k):
            at = pl.ds(pl.multiple_of(k * tile, tile), tile)
            u = uv_v[at, :ff]
            act_rows(at, u, uv_v[at, ff:], jax.nn.sigmoid(u))

        tok_g.far()
        da_pass()
    if has_next:
        ahead.relay()

    @pl.loop(0, tokens // tile)
    def _(k):
        at = pl.ds(pl.multiple_of(k * tile, tile), tile)
        u, v, d_act = uv_v[at, :ff], uv_v[at, ff:], da_v[at, :]
        sig = jax.nn.sigmoid(u)
        if has_g:
            act_rows(at, u, v, sig)
        duv_v[0, at, :ff] = (d_act * v * sig * (1.0 + u * (1.0 - sig))).astype(jnp.bfloat16)
        duv_v[0, at, ff:] = (d_act * (u * sig)).astype(jnp.bfloat16)

    def dn_pass(part):
        core = c if part == 0 else 1 - c

        @pl.loop(0, CHIPS)
        def _(k):
            at = pl.ds(pl.multiple_of(2 * shard * k + shard * core, shard), shard)
            block = lax.dot_general(
                duv_v[0], w_v[part, k].reshape(shard, width), (((1,), (1,)), ((), ())), preferred_element_type=f32
            )
            dn_v[:, :, at] = block.reshape(dn_v.shape[0], dn_v.shape[1], shard)

    dn_pass(0)
    x_copies = [
        send(duv_v.at[0], duv_v.at[1], x_send.at[0], x_recv.at[0], here.partner()),
        send(act_v.at[0], act_v.at[1], x_send.at[1], x_recv.at[1], here.partner()),
    ]
    dn_pass(1)
    dn_out = pltpu.make_async_copy(dn_v, dn, out_sem.at[4])
    dn_out.start()
    if has_next:
        ahead.far()

    def gu_out(m, k):
        return pltpu.make_async_copy(
            gu_v.at[k % 2],
            grad.at[:, pl.ds(pl.multiple_of(rows * k, rows), rows), pl.ds(m * ff, ff)],
            out_sem.at[k % 2],
        )

    arrived(duv_v.at[1], x_recv.at[0], here.partner(), x_send.at[0])
    for m in range(2):

        @pl.loop(0, CHIPS)
        def _(k):
            if m == 0:

                @pl.when(k >= 2)
                def _():
                    gu_out(m, k).wait()
            else:
                gu_out(m, k).wait()

            at = pl.ds(pl.multiple_of(k * shard, shard), shard)
            rhs = duv_v[:, :, m * ff : (m + 1) * ff].reshape(2 * tokens, ff)
            gu_v[k % 2] = jnp.dot(n_t[at, :], rhs, preferred_element_type=f32).reshape(members, rows, ff)
            gu_out(m, k).start()

    arrived(act_v.at[1], x_recv.at[1], here.partner(), x_send.at[1])
    if not has_g:
        tok_g.finish()
    half = ff // 2
    odd = half % 128
    act_at = pl.ds(pl.multiple_of(c * (half - odd), 128), half + odd)
    for m in range(2):
        transpose_into(act_t, m * tokens, act_v[m, :, act_at], 128)
    group = pack_v.shape[1]
    col = d_model // members

    def down_out(k):
        return pltpu.make_async_copy(
            pack_v.at[k % 2], grad_down.at[pl.ds(k * group, group)], out_sem.at[2 + k % 2]
        )

    @pl.loop(0, members // group)
    def _(k):
        at = pl.ds(pl.multiple_of(k * group * col, group * col), group * col)
        rhs = g_v[:, :, :, at].reshape(2 * tokens, group * col)
        down_v[...] = jnp.dot(act_t[...], rhs, preferred_element_type=f32)

        @pl.when(k >= 2)
        def _():
            down_out(k).wait()

        for d in range(group):
            for j in range(half // deep):
                at_rows = pl.ds(pl.multiple_of(c * odd + j * deep, 8), deep)
                pack_v[k % 2, d, :, j * col : (j + 1) * col] = down_v[at_rows, d * col : (d + 1) * col]
        down_out(k).start()

    for copy in (*w_copies, *x_copies):
        copy.wait_send()
    if has_next:
        ahead.finish()
        own.wait()
    dn_out.wait()
    for k in range(2):
        gu_out(1, k).wait()
        down_out(k).wait()


def layer_grads(w, index, n_all, g, down, n_own, order, collective_id):
    members, _, _, rows, width = w.shape
    _, _, seq, d_model = n_all.shape
    tokens, shard, ff = CHIPS * seq, members * rows, width // 2
    deep = d_model // members // CHIPS
    half = ff // 2 + (ff // 2) % 128
    group = max(members // 4, 1)
    bf, f32 = jnp.bfloat16, jnp.float32
    vmem, anywhere = pl.BlockSpec(memory_space=VMEM), pl.BlockSpec(memory_space=ANY)
    has_next, has_g = n_own is not None, len(g.shape) == 4
    out = [
        jax.ShapeDtypeStruct((members, CHIPS * rows, width), f32),
        jax.ShapeDtypeStruct((members, deep, width), f32),
        jax.ShapeDtypeStruct((CHIPS, seq, d_model), f32),
    ]
    if has_next:
        out.append(jax.ShapeDtypeStruct(n_all.shape, bf))
    extra = Tokens.COPIES if has_next else 1
    return pl.pallas_call(
        functools.partial(layer_kernel, index, has_g, has_next, len(order)),
        out_shape=tuple(out),
        in_specs=[anywhere] * 2 + [anywhere if has_g else vmem, anywhere] + [vmem] * has_next + [anywhere] * len(order),
        out_specs=(anywhere,) * len(out),
        scratch_shapes=[
            VMEM((2, CHIPS, members, rows, width), bf),
            VMEM((ff, d_model), bf),
            VMEM((2, CHIPS, seq, d_model), bf),
            VMEM((3, CHIPS, seq, CHIPS * shard), bf),
            VMEM((CHIPS * shard, 2 * tokens), bf),
            VMEM((tokens, ff), f32),
            VMEM((tokens, width), f32),
            VMEM((2, tokens, width), bf),
            VMEM((2, tokens, ff), bf),
            VMEM((half, 2 * tokens), bf),
            VMEM((CHIPS, seq, d_model), f32),
            VMEM((2, members, rows, ff), f32),
            VMEM((half, group * d_model // members), f32),
            VMEM((2, group, deep, width), f32),
            DMA((CHIPS,)),
            DMA((3 + 3 * CHIPS,)),
            DMA((CHIPS,)),
            DMA((CHIPS,)),
            DMA((2,)),
            DMA((2,)),
            DMA((7,)),
            DMA((Tokens.COPIES,)),
            DMA((Tokens.COPIES,)),
            DMA((extra,)),
            DMA((extra,)),
        ],
        compiler_params=params(collective_id, 60 * 1024 * 1024),
        cost_estimate=cost(45),
        name="layer_grads",
    )(w, n_all, g, down, *((n_own,) if has_next else ()), *order)


class RingSum:
    def __init__(self, device, block, buffers, send_sem, recv_sem):
        self.device, self.block = device, block
        self.from_left, self.from_right, self.in_left, self.in_right = buffers
        self.send_sem, self.recv_sem = send_sem, recv_sem
        self.copies = []

    def _half(self, ref, part):
        half = ref.shape[-2] // 2
        return ref.at[*[slice(None)] * (len(ref.shape) - 2), pl.ds(part * half, half)]

    def _send(self, k, src, dst, step):
        self.copies.append(send(src, dst, self.send_sem.at[k], self.recv_sem.at[k], self.device(step)))

    def _arrived(self, k, ref, step):
        arrived(ref, self.recv_sem.at[k], self.device(step), self.send_sem.at[k])

    def start(self):
        self._send(0, self.block(2, 0), self.from_left, 1)
        self._send(1, self.block(2, 1), self.from_right, -1)
        self._send(2, self.block(1, 1), self._half(self.in_left, 1), 1)
        self._send(3, self.block(-1, 0), self._half(self.in_right, 0), -1)

    def pass_right(self):
        self._arrived(0, self.from_left, -1)
        block = self.block(1, 0)
        block[...] = block[...] + self.from_left[...]
        self._send(4, block, self._half(self.in_left, 0), 1)

    def pass_left(self):
        self._arrived(1, self.from_right, 1)
        block = self.block(-1, 1)
        block[...] = block[...] + self.from_right[...]
        self._send(5, block, self._half(self.in_right, 1), -1)

    def total(self):
        self._arrived(2, self._half(self.in_left, 1), -1)
        self._arrived(3, self._half(self.in_right, 0), 1)
        self._arrived(4, self._half(self.in_left, 0), -1)
        self._arrived(5, self._half(self.in_right, 1), 1)
        return self.block(0, None)[...] + self.in_left[...] + self.in_right[...]

    def drain(self):
        for copy in self.copies:
            copy.wait_send()


def sum_scratch(lead, rows, width):
    half, whole = VMEM((*lead, rows // 2, width), jnp.float32), VMEM((*lead, rows, width), jnp.float32)
    return [half, half, whole, whole]


def dn_ring(here, dn_v, buffers, send_sem, recv_sem):
    half = dn_v.shape[1] // 2

    def block(step, part):
        at = here.chip(step)
        return dn_v.at[at] if part is None else dn_v.at[at, pl.ds(part * half, half)]

    return RingSum(here.ring, block, buffers, send_sem, recv_sem)


def dn_loads(here, dn, dn_v, load_sem):
    loads = []
    for k, step in enumerate((2, 1, -1, 0)):
        loads.append(pltpu.make_async_copy(dn.at[here.chip(step)], dn_v.at[here.chip(step)], load_sem.at[k]))
        loads[k].start()
    return loads


def g_step(d_norm, g, h):
    x_full = h[...].astype(jnp.float32)
    inv_rms = lax.rsqrt(jnp.mean(x_full * x_full, axis=-1, keepdims=True) + EPS)
    norm_f = x_full * inv_rms
    return g[...] + inv_rms * (d_norm - norm_f * jnp.mean(d_norm * norm_f, axis=-1, keepdims=True))


class MemberSum:
    def __init__(self, here, grad_v, buffers, send_sem, recv_sem):
        rows = grad_v.shape[2] // 2
        self.rows = rows

        def span(first, part):
            return pl.ds(first, rows) if part is None else pl.ds(first + part * rows // 2, rows // 2)

        def block_a1(step, part):
            return grad_v.at[:, here.at_y(step), span(0, part)]

        def block_b1(step, part):
            return grad_v.at[here.at_z(step), :, span(rows, part)]

        def block_a2(step, part):
            return grad_v.at[here.at_z(step), here.y, span(0, part)]

        def block_b2(step, part):
            return grad_v.at[here.z, here.at_y(step), span(rows, part)]

        devices = (here.ring_y, here.ring_z, here.ring_z, here.ring_y)
        blocks = (block_a1, block_b1, block_a2, block_b2)
        self.a1, self.b1, self.a2, self.b2 = (
            RingSum(*each) for each in zip(devices, blocks, buffers, send_sem, recv_sem)
        )

    def start(self):
        self.a1.start()
        self.b1.start()

    def pass_first(self):
        for ring in (self.a1, self.b1):
            ring.pass_right()
        for ring in (self.a1, self.b1):
            ring.pass_left()

    def second(self):
        for first, second in ((self.a1, self.a2), (self.b1, self.b2)):
            first.block(0, None)[...] = first.total()
            second.start()

    def finish(self, piece):
        for ring in (self.a2, self.b2):
            ring.pass_right()
            ring.pass_left()
        piece[: self.rows] = self.a2.total()
        piece[self.rows :] = self.b2.total()

    def drain(self):
        for ring in (self.a1, self.b1, self.a2, self.b2):
            ring.drain()


def members_sum_kernel(n_grads, n_order, dn, g, h, *refs):
    grads, refs = refs[:n_grads], refs[n_grads + n_order :]
    last = n_grads == 2
    outs, piece, dn_v, grad_v = refs[: 1 if last else 2], *refs[1 if last else 2 :][:3]
    refs = refs[len(outs) + 3 :]
    buffers = [refs[4 * k : 4 * k + 4] for k in range(5)]
    load_sem, grad_sem, send_sem, recv_sem = refs[20:]
    here = Place()
    rows = grad_v.shape[2] // 2
    loads = dn_loads(here, dn, dn_v, load_sem)
    grad_loads = []
    for k, step in enumerate((2, 1, -1, 0)):
        for m in range(2):
            at = (slice(None), here.at_y(step)) if m == 0 else (here.at_z(step), slice(None))
            first = 0
            for i, grad in enumerate(grads):
                low, high = max(first, m * rows), min(first + grad.shape[2], (m + 1) * rows)
                if low < high:
                    src = grad.at[*at, pl.ds(low - first, high - low)]
                    dst = grad_v.at[*at, pl.ds(low, high - low)]
                    load = pltpu.make_async_copy(src, dst, grad_sem.at[i, m, k])
                    load.start()
                    grad_loads.append(load)
                first += grad.shape[2]
    meet(
        [here.ring(1), here.ring(-1), here.ring_y(1), here.ring_y(-1), here.ring_z(1), here.ring_z(-1)]
    )
    x = dn_ring(here, dn_v, buffers[0], send_sem.at[0], recv_sem.at[0])
    sems = [send_sem.at[k] for k in range(1, 5)], [recv_sem.at[k] for k in range(1, 5)]
    members = MemberSum(here, grad_v, buffers[1:], *sems)

    def step_g():
        g_new = g_step(x.total(), g, h)
        if last:
            outs[0][...] = g_new.astype(outs[0].dtype)
        else:
            outs[0][...] = g_new
            outs[1][...] = g_new.astype(jnp.bfloat16)

    if not last:
        for load in loads:
            load.wait()
        x.start()
    for load in grad_loads:
        load.wait()
    members.start()
    if last:
        for load in loads:
            load.wait()
        x.start()
        x.pass_right()
        x.pass_left()
        members.pass_first()
        step_g()
        members.second()
    else:
        x.pass_right()
        x.pass_left()
        members.pass_first()
        members.second()
        step_g()
    members.finish(piece)
    x.drain()
    members.drain()


def members_sum(dn, g, h, grads, order, collective_id):
    vmem, anywhere = pl.BlockSpec(memory_space=VMEM), pl.BlockSpec(memory_space=ANY)
    n = len(grads)
    grads = tuple(grad.reshape(grad.shape[0] // RING, RING, *grad.shape[1:]) for grad in grads)
    rows, width = sum(grad.shape[2] for grad in grads), grads[0].shape[3]
    g_types = (jnp.bfloat16,) if n == 2 else (g.dtype, jnp.bfloat16)
    return pl.pallas_call(
        functools.partial(members_sum_kernel, n, len(order)),
        out_shape=tuple(jax.ShapeDtypeStruct(g.shape, t) for t in g_types)
        + (jax.ShapeDtypeStruct((rows, width), grads[0].dtype),),
        in_specs=[anywhere, vmem, vmem] + [anywhere] * (n + len(order)),
        out_specs=(vmem,) * (len(g_types) + 1),
        scratch_shapes=[VMEM(dn.shape, dn.dtype), VMEM((*grads[0].shape[:2], rows, width), grads[0].dtype)]
        + sum_scratch((), *g.shape)
        + sum_scratch((RING,), rows // 2, width) * 2
        + sum_scratch((), rows // 2, width) * 2
        + [DMA((4,)), DMA((n, 2, 4)), DMA((5, 6)), DMA((5, 6))],
        compiler_params=params(collective_id, 60 * 1024 * 1024),
        cost_estimate=cost(100 if n == 2 else 45),
        name="last_sum" if n == 2 else "next_g",
    )(dn, g, h, *grads, *order)


def gather_rows_kernel(n_order, rows, *refs):
    out, send_sem, recv_sem, own_sem = refs[n_order:]
    here = Place()
    own = pltpu.make_async_copy(rows, out.at[here.z, here.y], own_sem.at[0])
    own.start()
    meet([here.ring_y(1), here.ring_y(-1), here.ring_z(1), here.ring_z(-1)])
    own.wait()
    members = Members(here, out, send_sem, recv_sem)
    members.start()
    members.relay_first()
    members.finish()
    members.drain()


def gather_rows(rows, order, collective_id):
    anywhere = pl.BlockSpec(memory_space=ANY)
    return pl.pallas_call(
        functools.partial(gather_rows_kernel, len(order)),
        out_shape=jax.ShapeDtypeStruct((RING, RING, *rows.shape), rows.dtype),
        in_specs=[pl.BlockSpec(memory_space=VMEM)] + [anywhere] * len(order),
        out_specs=anywhere,
        scratch_shapes=[DMA((10, 4)), DMA((10, 4)), DMA((1,))],
        compiler_params=params(collective_id),
        cost_estimate=cost(100),
        name="gather_rows",
    )(rows, *order)


def grad_rows_kernel(counts, *refs):
    pieces, outs = [], refs[-5 - len(counts) : -5]
    relays, send_sem, recv_sem, local_sem, down_sem = refs[-5:]
    for count in counts:
        pieces.append(refs[:count])
        refs = refs[count:]
    here = Place()
    cols = outs[0].shape[1] // 2
    rows = outs[0].shape[0] // 6
    down = pl.ds(4 * rows, 2 * rows)
    exchanges, local = [], []
    for i, piece in enumerate(pieces):

        def part(step, m, piece=piece):
            return piece[0].at[pl.ds(pl.multiple_of(here.chip(step) * rows, rows), rows), pl.ds(m * cols, cols)]

        def landing(chip, m, i=i):
            at = pl.ds(pl.multiple_of((2 * m + chip // 2) * rows, rows), rows)
            return outs[i].at[at, pl.ds(pl.multiple_of(chip % 2 * cols, cols), cols)]

        exchanges.append(Exchange(here, part, landing, relays.at[i], send_sem.at[i], recv_sem.at[i]))
        src = piece[1] if len(piece) == 2 else piece[0].at[down]
        local.append(pltpu.make_async_copy(src, outs[i].at[down], down_sem.at[i]))
        for m in range(2):
            local.append(pltpu.make_async_copy(part(0, m), landing(here.x, m), local_sem.at[i, m]))
    for copy in local:
        copy.start()
    meet([here.ring(1), here.ring(-1)])
    for exchange in exchanges:
        exchange.start()
    for exchange in exchanges:
        exchange.relay()
    for exchange in exchanges:
        exchange.finish()
    for copy in local:
        copy.wait()


def grad_rows(pieces, order, collective_id):
    vmem = pl.BlockSpec(memory_space=VMEM)
    n = len(pieces)
    flat = [ref for piece in pieces for ref in piece]
    rows, width = sum(ref.shape[0] for ref in pieces[0]), flat[0].shape[1]
    dtype = flat[0].dtype
    return pl.pallas_call(
        functools.partial(grad_rows_kernel, tuple(len(piece) for piece in pieces)),
        out_shape=(jax.ShapeDtypeStruct((rows, width), dtype),) * n,
        in_specs=[vmem] * len(flat) + [pl.BlockSpec(memory_space=ANY)] * len(order),
        out_specs=(vmem,) * n,
        scratch_shapes=[
            VMEM((n, 2, rows // 6, width // 2), dtype),
            DMA((n, Exchange.COPIES)),
            DMA((n, Exchange.COPIES)),
            DMA((n, 2)),
            DMA((n,)),
        ],
        compiler_params=params(collective_id),
        cost_estimate=cost(12),
        name="grad_rows",
    )(*flat, *order)


PARTS = 4


def place_kernel(layer, grad, *refs):
    gate, up, down, buf, d_buf, pack, load_sem, d_sem, store_sem = refs[-9:]
    members, rows, half = grad.shape[0], grad.shape[1] // 6, grad.shape[2]
    part = max(members // PARTS, 1)
    parts = members // part
    d_load = pltpu.make_async_copy(grad.at[:, pl.ds(4 * rows, 2 * rows)], d_buf, d_sem.at[0])
    d_load.start()
    loads = []
    for m in range(2):
        for k in range(parts):
            at = pl.ds(k * part, part)
            for h in range(2):
                src = grad.at[at, pl.ds((2 * m + h) * rows, rows)]
                load = pltpu.make_async_copy(src, buf.at[m, at, :, pl.ds(h * half, half)], load_sem.at[m, k, h])
                load.start()
                loads.append(load)
    d_load.wait()
    stores = []
    for m, out in enumerate((gate, up)):
        for k in range(parts):
            at = pl.ds(k * part, part)
            for h in range(2):
                loads[(m * parts + k) * 2 + h].wait()
            store = pltpu.make_async_copy(buf.at[m, at], out.at[layer, at], store_sem.at[m, k])
            store.start()
            stores.append(store)
    col, deep = down.shape[2] // members, 2 * rows

    @pl.loop(0, half // col)
    def _(j):
        at = pl.ds(pl.multiple_of(j * deep, deep), deep)
        cols = pl.ds(pl.multiple_of(j * col, col), col)
        for d in range(members):
            pack[at, d * col : (d + 1) * col] = d_buf[d, :, cols]

    store = pltpu.make_async_copy(pack, down.at[layer], d_sem.at[1])
    store.start()
    stores.append(store)
    for store in stores:
        store.wait()


def place(grad, layer, stacks, order, shapes):
    members, rows, half = grad.shape
    anywhere = pl.BlockSpec(memory_space=ANY)
    return pl.pallas_call(
        functools.partial(place_kernel, layer),
        out_shape=shapes,
        in_specs=[anywhere] * (1 + len(stacks) + len(order)),
        out_specs=(anywhere,) * 3,
        input_output_aliases={1 + m: m for m in range(len(stacks))},
        scratch_shapes=[
            VMEM((2, members, rows // 6, 2 * half), grad.dtype),
            VMEM((members, rows // 3, half), grad.dtype),
            VMEM(shapes[2].shape[1:], grad.dtype),
            DMA((2, PARTS, 2)),
            DMA((2,)),
            DMA((2, PARTS)),
        ],
        compiler_params=pltpu.CompilerParams(vmem_limit_bytes=58 * 1024 * 1024),
        cost_estimate=cost(13),
        name="place",
    )(grad, *stacks, *order)


def gather_dp(value):
    return lax.all_gather(value[None], "dp", axis=0, tiled=True)


def scatter_dp(value):
    members, *piece = value.shape
    value = value.reshape(members * piece[0], *piece[1:])
    return lax.psum_scatter(value, "dp", scatter_dimension=0, tiled=True)


def solution(mesh):
    dp = mesh.shape["dp"]
    tok_spec = P(("dp", "fsdp"))
    stack_spec = P(None, ("dp", "fsdp"))
    weight_spec = P(None, "fsdp")

    def local_backward(h_saved, grad_out, gate_sh, up_sh, down_sh):
        layers = h_saved.shape[0]
        b_loc, seq, width = grad_out.shape
        tokens = b_loc * seq
        h = h_saved.reshape(layers, tokens, width)
        x_full = h.astype(jnp.float32)
        inv_rms = lax.rsqrt(jnp.mean(x_full * x_full, axis=-1, keepdims=True) + EPS)
        n = (x_full * inv_rms).astype(jnp.bfloat16)
        g_bf = grad_out.reshape(tokens, width)
        g = g_bf.astype(jnp.float32)
        last = layers - 1
        ids = iter(range(1, 100))

        order = tuple(reversed(range(layers)))
        rows, other_rows = weight_rows(gate_sh, up_sh, order, dp, next(ids))
        others = gather_dp(other_rows)
        w, n_all, g_in, *down = first_gather(rows, n[last], g_bf, down_sh, next(ids))
        weights = {layer: (others, k - 1) for k, layer in enumerate(order)}
        weights[last] = w.reshape(dp, 1, *w.shape[2:]), 0
        pieces, sent = {}, ()
        for layer in order:
            n_own = n[layer - 1] if layer else None
            grad, grad_down, dn, *n_next = layer_grads(
                *weights[layer], n_all, g_in, down[layer], n_own, sent, next(ids)
            )
            if layer:
                piece = scatter_dp(grad)
                n_all = n_next[0]
                g, g_in, piece_down = members_sum(dn, g, h[layer], (grad_down,), (), next(ids))
                pieces[layer] = piece, piece_down
            if layer == 1:
                (first_rows,) = grad_rows((pieces[last],), (g_in,), next(ids))
                gathered = {last: gather_dp(first_rows)}
                sent = (first_rows,)
        d_h0, pieces[0] = members_sum(dn, g, h[0], (grad, grad_down), (), next(ids))
        rows = {}
        rows[1], rows[0] = grad_rows((pieces[1], (pieces[0],)), (), next(ids))
        gathered[0] = gather_dp(rows[0])
        mine = rows[1].reshape(4, -1, rows[1].shape[1])
        all_rows = gather_rows(mine, (), next(ids))
        gathered[1] = all_rows.reshape(gathered[0].shape)

        rows = (layers, dp, gate_sh.shape[1] // dp, gate_sh.shape[2])
        shapes = tuple(jax.ShapeDtypeStruct(shape, jnp.float32) for shape in (rows, rows, down_sh.shape))
        stacks = ()
        for layer in order:
            stacks = place(gathered[layer], layer, stacks, (all_rows,) if layer == last else (), shapes)
        gate, up, down_grad = stacks
        return gate.reshape(gate_sh.shape), up.reshape(up_sh.shape), down_grad, d_h0.reshape(b_loc, seq, width)

    return jax.shard_map(
        local_backward,
        mesh=mesh,
        in_specs=(stack_spec, tok_spec, weight_spec, weight_spec, weight_spec),
        out_specs=(weight_spec, weight_spec, weight_spec, tok_spec),
        check_vma=False,
    )
```

```python
import functools
import types

import jax
import jax.numpy as jnp
from jax import lax
from jax.experimental import pallas as pl
from jax.experimental.pallas import tpu as pltpu
from jax.sharding import PartitionSpec as P


EPS = 1e-5
CHIPS = 4
RING = 4
MESH = pl.DeviceIdType.MESH
VMEM = pltpu.VMEM
ANY = pl.ANY
DMA = pltpu.SemaphoreType.DMA


class Place:
    def __init__(self):
        self.dp = lax.axis_index("dp")
        self.f = lax.axis_index("fsdp")
        self.x, self.c = self.f // 2, self.f % 2
        self.z, self.y = self.dp // RING, self.dp % RING

    def chip(self, step):
        return (self.x + step) % CHIPS

    def ring(self, step):
        return (self.dp, 2 * self.chip(step) + self.c)

    def partner(self):
        return (self.dp, 2 * self.x + (1 - self.c))

    def at_y(self, step):
        return (self.y + step) % RING

    def at_z(self, step):
        return (self.z + step) % RING

    def ring_y(self, step):
        return (self.z * RING + self.at_y(step), self.f)

    def ring_z(self, step):
        return (self.at_z(step) * RING + self.y, self.f)


def meet(peers):
    barrier = pltpu.get_barrier_semaphore()
    for peer in peers:
        pl.semaphore_signal(barrier, inc=1, device_id=peer, device_id_type=MESH)
    pl.semaphore_wait(barrier, len(peers))


def send(src, dst, send_sem, recv_sem, device):
    copy = pltpu.make_async_remote_copy(
        src_ref=src, dst_ref=dst, send_sem=send_sem, recv_sem=recv_sem, device_id=device, device_id_type=MESH
    )
    copy.start()
    return copy


def arrived(ref, recv_sem, device, send_sem):
    pltpu.make_async_remote_copy(
        src_ref=ref, dst_ref=ref, send_sem=send_sem, recv_sem=recv_sem, device_id=device, device_id_type=MESH
    ).wait_recv()


def params(collective_id, vmem=None):
    return pltpu.CompilerParams(collective_id=collective_id, has_side_effects=True, vmem_limit_bytes=vmem)


def cost(us):
    return pl.CostEstimate(flops=int(us * 4.0e6), bytes_accessed=0, transcendentals=0)


class Ring:
    def __init__(self, device, at, block, own, send_sem, recv_sem):
        self.device, self.at, self.block, self.own = device, at, block, own
        self.send_sem, self.recv_sem = send_sem, recv_sem
        self.copies = []

    def _send(self, k, src, dst, step):
        self.copies.append(send(src, dst, self.send_sem(k), self.recv_sem(k), self.device(step)))

    def _arrived(self, k, ref, step):
        arrived(ref, self.recv_sem(k), self.device(step), self.send_sem(k))

    def start(self):
        here = self.block(self.at(0), None)
        self._send(0, self.own, here, 1)
        self._send(1, self.own, here, -1)

    def relay_right(self):
        self._arrived(0, self.block(self.at(-1), None), -1)
        half = self.block(self.at(-1), 0)
        self._send(2, half, half, 1)

    def relay_left(self):
        self._arrived(1, self.block(self.at(1), None), 1)
        half = self.block(self.at(1), 1)
        self._send(3, half, half, -1)

    def finish(self):
        self._arrived(2, self.block(self.at(2), 0), -1)
        self._arrived(3, self.block(self.at(2), 1), 1)

    def drain(self):
        for copy in self.copies:
            copy.wait_send()


class Tokens:
    COPIES = 8

    def __init__(self, here, own, out, send_sem, recv_sem):
        half = out.shape[2] // 2

        def block(chip, part):
            return out.at[0, chip] if part is None else out.at[0, chip, pl.ds(part * half, half)]

        self.here, self.own, self.out = here, own, out
        self.send_sem, self.recv_sem = send_sem, recv_sem
        self.ring = Ring(here.ring, here.chip, block, own, lambda k: send_sem.at[k], lambda k: recv_sem.at[k])
        self.pairs = []

    def _pair(self, k, src, chip):
        dst = self.out.at[1, chip]
        copy = send(src, dst, self.send_sem.at[4 + k], self.recv_sem.at[4 + k], self.here.partner())
        self.pairs.append((k, chip, copy))

    def start(self):
        self.ring.start()
        self._pair(0, self.own, self.here.x)

    def relay(self):
        left, right = self.here.chip(-1), self.here.chip(1)
        self.ring.relay_right()
        self._pair(1, self.out.at[0, left], left)
        self.ring.relay_left()
        self._pair(2, self.out.at[0, right], right)

    def far(self):
        far = self.here.chip(2)
        self.ring.finish()
        self._pair(3, self.out.at[0, far], far)

    def finish(self):
        for k, chip, copy in self.pairs:
            arrived(self.out.at[1, chip], self.recv_sem.at[4 + k], self.here.partner(), self.send_sem.at[4 + k])
            copy.wait_send()
        self.ring.drain()


class Members:
    GROUPS = 10
    PAIRS = 8

    def __init__(self, here, slots, send_sem, recv_sem, pair=None, pair_send=None, pair_recv=None):
        self.here, self.slots, self.send_sem, self.recv_sem = here, slots, send_sem, recv_sem
        self.pair, self.pair_send, self.pair_recv = pair, pair_send, pair_recv
        a1, b1 = self._ring(0, 0, True, here.z), self._ring(1, 2, False, here.y)
        a2 = {step: self._ring(2 + k, 0, False, here.at_y(step)) for k, step in enumerate((0, -1, 1, 2))}
        b2 = {step: self._ring(6 + k, 2, True, here.at_z(step)) for k, step in enumerate((0, -1, 1, 2))}
        self.rings = ((a1, a2), (b1, b2))
        self.forwards = []

    def _ring(self, group, first, along_y, fixed):
        def block(at, part):
            k = pl.ds(first, 2) if part is None else pl.ds(first + part, 1)
            return self.slots.at[fixed, at, k] if along_y else self.slots.at[at, fixed, k]

        here = self.here
        device, at = (here.ring_y, here.at_y) if along_y else (here.ring_z, here.at_z)
        sems = (lambda k: self.send_sem.at[group, k]), (lambda k: self.recv_sem.at[group, k])
        return Ring(device, at, block, block(at(0), None), *sems)

    def start(self):
        for first, second in self.rings:
            first.start()
        for first, second in self.rings:
            second[0].start()

    def relay_first(self):
        for first, second in self.rings:
            first.relay_right()
            second[-1].start()
        for first, second in self.rings:
            first.relay_left()
            second[1].start()
        for _, second in self.rings:
            second[0].relay_right()
            second[0].relay_left()

    def far(self):
        for first, second in self.rings:
            first.finish()
            second[2].start()
        self.relay(-1)

    def relay(self, step):
        for _, second in self.rings:
            second[step].relay_right()
            second[step].relay_left()

    def done(self, *steps):
        for step in steps:
            for m, (_, second) in enumerate(self.rings):
                second[step].finish()
                if self.pair is not None:
                    self._forward(m, step)

    def _group(self, ref, m, step):
        here = self.here
        return ref.at[:, here.at_y(step), pl.ds(0, 2)] if m == 0 else ref.at[here.at_z(step), :, pl.ds(2, 2)]

    def _forward(self, m, step):
        k = 4 * m + (step + 1)
        dst = self._group(self.pair, m, step)
        send_sem, recv_sem = self.pair_send.at[k], self.pair_recv.at[k]
        copy = send(self._group(self.slots, m, step), dst, send_sem, recv_sem, self.here.partner())
        self.forwards.append((copy, dst, k))

    def arrived_pair(self):
        for _, dst, k in self.forwards:
            arrived(dst, self.pair_recv.at[k], self.here.partner(), self.pair_send.at[k])

    def drain(self):
        for copy, _, _ in self.forwards:
            copy.wait_send()
        for first, second in self.rings:
            for r in (first, *second.values()):
                r.drain()


class Exchange:
    COPIES = 8

    def __init__(self, here, part, landing, relays, send_sem, recv_sem):
        self.here, self.part, self.landing, self.relays = here, part, landing, relays
        self.send_sem, self.recv_sem = send_sem, recv_sem
        self.copies = []

    def _send(self, k, src, dst, step):
        self.copies.append(send(src, dst, self.send_sem.at[k], self.recv_sem.at[k], self.here.ring(step)))

    def _arrived(self, k, ref, step):
        arrived(ref, self.recv_sem.at[k], self.here.ring(step), self.send_sem.at[k])

    def start(self):
        for m, step in enumerate((1, -1)):
            self._send(4 + m, self.part(2, m), self.relays.at[m], step)
        for k, step in enumerate((1, -1)):
            for m in range(2):
                self._send(2 * k + m, self.part(step, m), self.landing(self.here.x, m), step)

    def relay(self):
        for m, step in enumerate((1, -1)):
            self._arrived(4 + m, self.relays.at[m], -step)
            self._send(6 + m, self.relays.at[m], self.landing(self.here.chip(-step), m), step)

    def finish(self):
        for k, step in enumerate((1, -1)):
            for m in range(2):
                self._arrived(2 * k + m, self.landing(self.here.chip(-step), m), -step)
        for m, step in enumerate((1, -1)):
            self._arrived(6 + m, self.landing(self.here.chip(2), m), -step)
        for copy in self.copies:
            copy.wait_send()


def norm_rows(h):
    x_full = h[...].astype(jnp.float32)
    inv_rms = lax.rsqrt(jnp.mean(x_full * x_full, axis=-1, keepdims=True) + EPS)
    return (x_full * inv_rms).astype(jnp.bfloat16)


class WeightRows:
    def __init__(self, here, layer, weights, rows_v, landing, load_sem, send_sem, recv_sem, own_sem):
        self.here, self.rows_v, self.landing = here, rows_v, landing
        self.send_sem, self.recv_sem = send_sem, recv_sem
        cols = rows_v.shape[2] // 2
        self.loads, self.copies = [], []
        for j in range(CHIPS):
            at = pl.ds(pl.multiple_of(here.chip(j) * cols, cols), cols)
            for m, w in enumerate(weights):
                dst = rows_v.at[j, :, pl.ds(m * cols, cols)]
                self.loads.append(pltpu.make_async_copy(w.at[layer, here.z, here.y, :, at], dst, load_sem.at[j, m]))
        self.own = pltpu.make_async_copy(rows_v.at[0], landing.at[here.x], own_sem)

    def load(self):
        for load in self.loads:
            load.start()

    def start(self):
        for load in self.loads:
            load.wait()
        self.own.start()
        for j in (2, 1, 3):
            dst, device = self.landing.at[self.here.x], self.here.ring(j)
            self.copies.append(send(self.rows_v.at[j], dst, self.send_sem.at[j], self.recv_sem.at[j], device))

    def finish(self):
        self.own.wait()
        for j in (1, 3, 2):
            src = self.landing.at[self.here.chip(-j)]
            arrived(src, self.recv_sem.at[j], self.here.ring(-j), self.send_sem.at[j])

    def drain(self):
        for copy in self.copies:
            copy.wait_send()


def transpose_into(dst, row, first, src):
    dst[row : row + src.shape[1], first : first + src.shape[0]] = src.T


def layer_kernel(layer, names, *refs):
    r = types.SimpleNamespace(**dict(zip(names, refs)))
    first, last = "h" in names, layer == 0
    here = Place()
    c = here.c
    f32, bf = jnp.float32, jnp.bfloat16
    _, zs, ys, _, rows, width = r.w_v.shape
    members = zs * ys
    shard, ff, deep = members * rows, width // 2, r.pack_v.shape[2]
    seq, d_model = r.n_v.shape[2:]
    tokens = CHIPS * seq
    partner = here.partner()

    d_own, d_other = (pl.ds(pl.multiple_of(k * (ff // 2), ff // 2), ff // 2) for k in (c, 1 - c))
    d_load = pltpu.make_async_copy(r.down.at[layer], r.d_v.at[d_own], r.load.at[0])
    g_own = pltpu.make_async_copy(r.g, r.g_v.at[0, here.x], r.load.at[1])
    peers = [partner, here.ring(1), here.ring(-1)]
    w_loads = []
    if first:
        rows_2 = WeightRows(
            here, layer, (r.gate, r.up), r.rows_v.at[0], r.w_v.at[0, here.z, here.y],
            r.r_load.at[0], r.r_send.at[0], r.r_recv.at[0], r.load.at[2],
        )
        rows_1 = WeightRows(
            here, layer - 1, (r.gate, r.up), r.rows_v.at[1], r.w_next.at[here.z, here.y],
            r.r_load.at[1], r.r_send.at[1], r.r_recv.at[1], r.load.at[3],
        )
        rows_2.load()
        rows_1.load()
        peers += [here.ring(2), here.ring_y(1), here.ring_y(-1), here.ring_z(1), here.ring_z(-1)]
    elif not last:
        w_loads = [pltpu.make_async_copy(r.w.at[z], r.w_v.at[0, z], r.w_load.at[z]) for z in range(zs)]
    else:
        own_cols = pl.ds(pl.multiple_of(here.x * ff, ff), ff)
        for m, (w, others) in enumerate(((r.gate, r.wx_gate), (r.up, r.wx_up))):
            for j in range(CHIPS):
                chip = here.chip(j)
                src = others.at[chip] if j else w.at[layer, :, :, :, own_cols]
                dst = r.w_v.at[0, :, :, chip, :, pl.ds(m * ff, ff)]
                w_loads.append(pltpu.make_async_copy(src, dst, r.w_load.at[CHIPS * m + j]))
    for load in w_loads:
        load.start()
    if not first:
        n_load = pltpu.make_async_copy(r.n, r.n_v, r.load.at[4])
        n_load.start()
    d_load.start()
    g_own.start()
    if first:
        r.h_v[0] = norm_rows(r.h)
        r.n_v[0, here.x] = r.h_v[0]
    if not last:
        r.h_v[1] = norm_rows(r.h_next)
        n_own = pltpu.make_async_copy(r.h_v.at[1], r.n_next.at[0, here.x], r.load.at[5])
        n_own.start()
    meet(peers)

    tok_g = Tokens(here, r.g, r.g_v, r.g_send, r.g_recv)
    if first:
        tok_n = Tokens(here, r.h_v.at[0], r.n_v, r.n_send.at[0], r.n_recv.at[0])
        mem = Members(here, r.w_v.at[0], r.m_send.at[0], r.m_recv.at[0], r.w_v.at[1], r.p_send, r.p_recv)
        ahead_w = Members(here, r.w_next, r.m_send.at[1], r.m_recv.at[1])
    if not last:
        ahead_n = Tokens(here, r.h_v.at[1], r.n_next, r.n_send.at[1], r.n_recv.at[1])
        source = r.gate if first else r.up
        half = zs // 2

        def cross_part(step, m):
            at = pl.ds(pl.multiple_of(here.chip(step) * ff, ff), ff)
            return source.at[0, pl.ds(m * half, half), :, :, at]

        def cross_landing(chip, m):
            return r.wx.at[chip, pl.ds(m * half, half)]

        cross = Exchange(here, cross_part, cross_landing, r.relays, r.x_send, r.x_recv)

    def da_pass():
        g_here = r.g_v[0].reshape(tokens, d_model)
        for low in range(0, ff, 768):
            high = min(low + 768, ff)
            r.da_v[:, low:high] = lax.dot_general(
                g_here, r.d_v[low:high, :], (((1,), (1,)), ((), ())), preferred_element_type=f32
            )

    def columns(k, core, offset=0, size=shard):
        return pl.ds(pl.multiple_of(2 * shard * k + shard * core + offset, size), size)

    def transposes():
        chunk = min(128, shard)
        for group in range(2):
            for k in range(CHIPS):
                for q in range(shard // chunk):
                    block = r.n_v[group, :, :, columns(k, c, q * chunk, chunk)].reshape(tokens, chunk)
                    transpose_into(r.n_t, k * shard + q * chunk, group * tokens, block)

    def uv_pass(parts):
        step = 256 if width % 256 == 0 else width

        @pl.loop(0, width // step)
        def _(i):
            at = pl.ds(pl.multiple_of(i * step, step), step)
            total = r.uv_v[:, at] if 0 not in parts else None
            for part in parts:
                core = c if part == 0 else 1 - c
                lhs = jnp.concatenate([r.n_v[0, :, :, columns(k, core)].reshape(tokens, shard) for k in range(CHIPS)], 1)
                rhs = jnp.concatenate([r.w_v[part, :, :, k, :, at].reshape(shard, step) for k in range(CHIPS)], 0)
                block = jnp.dot(lhs, rhs, preferred_element_type=f32)
                total = block if total is None else total + block
            r.uv_v[:, at] = total

    tile = min(32, tokens)

    def act_rows(at, u, v, sig):
        r.act_v[0, at] = (u * sig * v).astype(bf)

    def act_pass():
        @pl.loop(0, tokens // tile)
        def _(k):
            at = pl.ds(pl.multiple_of(k * tile, tile), tile)
            u = r.uv_v[at, :ff]
            act_rows(at, u, r.uv_v[at, ff:], jax.nn.sigmoid(u))

    def duv_pass(with_act):
        @pl.loop(0, tokens // tile)
        def _(k):
            at = pl.ds(pl.multiple_of(k * tile, tile), tile)
            u, v, d_act = r.uv_v[at, :ff], r.uv_v[at, ff:], r.da_v[at, :]
            sig = jax.nn.sigmoid(u)
            if with_act:
                act_rows(at, u, v, sig)
            r.duv_v[0, at, :ff] = (d_act * v * sig * (1.0 + u * (1.0 - sig))).astype(bf)
            r.duv_v[0, at, ff:] = (d_act * (u * sig)).astype(bf)

    if first:
        rows_2.start()
        tok_n.start()
        rows_1.start()
        d_load.wait()
        d_copy = send(r.d_v.at[d_own], r.d_v.at[d_own], r.d_send.at[0], r.d_recv.at[0], partner)
        rows_2.finish()
        mem.start()
        tok_g.start()
        mem.relay_first()
        tok_n.relay()
        mem.far()
        mem.relay(1)
        rows_1.finish()
        tok_g.relay()
        mem.done(0)
        mem.relay(2)
        tok_n.far()
        ahead_w.start()
        ahead_n.start()
        cross.start()
        mem.done(-1, 1, 2)
        ahead_w.relay_first()
        tok_n.finish()
        transposes()
        tok_g.far()
        g_own.wait()
        arrived(r.d_v.at[d_other], r.d_recv.at[0], partner, r.d_send.at[0])
        da_pass()
        ahead_w.far()
        mem.arrived_pair()
        uv_pass((0, 1))
        ahead_w.relay(1)
        ahead_n.relay()
        duv_pass(True)
    else:
        tok_g.start()
        for load in w_loads:
            load.wait()
        w_copies = [
            send(r.w_v.at[0, z], r.w_v.at[1, z], r.w_send.at[z], r.w_recv.at[z], partner) for z in range(zs)
        ]
        d_load.wait()
        d_copy = send(r.d_v.at[d_own], r.d_v.at[d_own], r.d_send.at[0], r.d_recv.at[0], partner)
        n_load.wait()
        transposes()
        uv_pass((0,))
        tok_g.relay()
        if not last:
            ahead_n.start()
            cross.start()
        for z in range(zs):
            arrived(r.w_v.at[1, z], r.w_recv.at[z], partner, r.w_send.at[z])
        uv_pass((1,))
        act_pass()
        tok_g.far()
        g_own.wait()
        arrived(r.d_v.at[d_other], r.d_recv.at[0], partner, r.d_send.at[0])
        da_pass()
        if not last:
            ahead_n.relay()
        duv_pass(False)

    def dn_pass(part):
        core = c if part == 0 else 1 - c

        @pl.loop(0, CHIPS)
        def _(k):
            rhs = r.w_v[part, :, :, k].reshape(shard, width)
            block = lax.dot_general(r.duv_v[0], rhs, (((1,), (1,)), ((), ())), preferred_element_type=f32)
            r.dn_v[:, :, columns(k, core)] = block.reshape(CHIPS, seq, shard)

    dn_pass(0)
    x_copies = [
        send(r.duv_v.at[0], r.duv_v.at[1], r.c_send.at[0], r.c_recv.at[0], partner),
        send(r.act_v.at[0], r.act_v.at[1], r.c_send.at[1], r.c_recv.at[1], partner),
    ]
    if first:
        ahead_w.done(0)
        ahead_w.relay(2)
    if not last:
        ahead_n.far()
        cross.relay()
    dn_pass(1)
    dn_out = pltpu.make_async_copy(r.dn_v, r.dn, r.out_sem.at[4])
    dn_out.start()

    def gu_out(m, k):
        return pltpu.make_async_copy(
            r.gu_v.at[k % 2],
            r.grad.at[:, pl.ds(pl.multiple_of(rows * k, rows), rows), pl.ds(m * ff, ff)],
            r.out_sem.at[k % 2],
        )

    arrived(r.duv_v.at[1], r.c_recv.at[0], partner, r.c_send.at[0])
    for m in range(2):

        @pl.loop(0, CHIPS)
        def _(k):
            if m == 0:

                @pl.when(k >= 2)
                def _():
                    gu_out(m, k).wait()
            else:
                gu_out(m, k).wait()

            at = pl.ds(pl.multiple_of(k * shard, shard), shard)
            rhs = r.duv_v[:, :, m * ff : (m + 1) * ff].reshape(2 * tokens, ff)
            r.gu_v[k % 2] = jnp.dot(r.n_t[at, :], rhs, preferred_element_type=f32).reshape(members, rows, ff)
            gu_out(m, k).start()

    arrived(r.act_v.at[1], r.c_recv.at[1], partner, r.c_send.at[1])
    if first:
        ahead_w.done(-1, 1, 2)
    tok_g.finish()
    half_ff = ff // 2
    odd = half_ff % 128
    for m in range(2):
        for q in range((half_ff + odd) // 128):
            at = pl.ds(pl.multiple_of(c * (half_ff - odd) + q * 128, 128), 128)
            transpose_into(r.act_t, q * 128, m * tokens, r.act_v[m, :, at])
    group = r.pack_v.shape[1]
    col = d_model // members

    def down_out(k):
        return pltpu.make_async_copy(
            r.pack_v.at[k % 2], r.grad.at[pl.ds(k * group, group), pl.ds(CHIPS * rows, deep)], r.out_sem.at[2 + k % 2]
        )

    @pl.loop(0, members // group)
    def _(k):
        at = pl.ds(pl.multiple_of(k * group * col, group * col), group * col)
        rhs = r.g_v[:, :, :, at].reshape(2 * tokens, group * col)
        r.down_v[...] = jnp.dot(r.act_t[...], rhs, preferred_element_type=f32)

        @pl.when(k >= 2)
        def _():
            down_out(k).wait()

        for d in range(group):
            for j in range(half_ff // deep):
                at_rows = pl.ds(pl.multiple_of(c * odd + j * deep, 8), deep)
                r.pack_v[k % 2, d, :, j * col : (j + 1) * col] = r.down_v[at_rows, d * col : (d + 1) * col]
        down_out(k).start()

    for copy in (*x_copies, d_copy):
        copy.wait_send()
    if first:
        for part in (rows_1, rows_2, mem, ahead_w):
            part.drain()
    else:
        for copy in w_copies:
            copy.wait_send()
    if not last:
        cross.finish()
        ahead_n.finish()
        n_own.wait()
    dn_out.wait()
    for k in range(2):
        gu_out(1, k).wait()
        down_out(k).wait()


def layer_grads(layer, dp, inputs, collective_id):
    seq, d_model = inputs["g"].shape
    *_, rows, ff_all = inputs["gate"].shape
    tokens, shard, ff = CHIPS * seq, dp * rows, ff_all // CHIPS
    width, zs = 2 * ff, dp // RING
    deep = d_model // dp // CHIPS
    half = ff // 2 + (ff // 2) % 128
    group = max(dp // 4, 1)
    bf, f32 = jnp.bfloat16, jnp.float32
    vmem, anywhere = pl.BlockSpec(memory_space=VMEM), pl.BlockSpec(memory_space=ANY)
    first, last = "h" in inputs, layer == 0
    outs = {
        "grad": jax.ShapeDtypeStruct((dp, CHIPS * rows + deep, width), f32),
        "dn": jax.ShapeDtypeStruct((CHIPS, seq, d_model), f32),
    }
    if not last:
        outs["n_next"] = jax.ShapeDtypeStruct((2, CHIPS, seq, d_model), bf)
        outs["wx"] = jax.ShapeDtypeStruct((CHIPS, zs, RING, rows, ff), bf)
    if first:
        outs["w_next"] = jax.ShapeDtypeStruct((zs, RING, CHIPS, rows, width), bf)
    scratch = {
        "w_v": VMEM((2, zs, RING, CHIPS, rows, width), bf),
        "d_v": VMEM((ff, d_model), bf),
        "g_v": VMEM((2, CHIPS, seq, d_model), bf),
        "n_v": VMEM((2, CHIPS, seq, d_model), bf),
        "n_t": VMEM((CHIPS * shard, 2 * tokens), bf),
        "da_v": VMEM((tokens, ff), f32),
        "uv_v": VMEM((tokens, width), f32),
        "duv_v": VMEM((2, tokens, width), bf),
        "act_v": VMEM((2, tokens, ff), bf),
        "act_t": VMEM((half, 2 * tokens), bf),
        "dn_v": VMEM((CHIPS, seq, d_model), f32),
        "gu_v": VMEM((2, dp, rows, ff), f32),
        "down_v": VMEM((half, group * d_model // dp), f32),
        "pack_v": VMEM((2, group, deep, width), f32),
        "load": DMA((6,)),
        "out_sem": DMA((5,)),
        "c_send": DMA((2,)),
        "c_recv": DMA((2,)),
        "d_send": DMA((1,)),
        "d_recv": DMA((1,)),
        "g_send": DMA((Tokens.COPIES,)),
        "g_recv": DMA((Tokens.COPIES,)),
    }
    if first:
        scratch["rows_v"] = VMEM((2, CHIPS, rows, width), bf)
        for name in ("m_send", "m_recv"):
            scratch[name] = DMA((2, Members.GROUPS, 4))
        scratch["r_load"] = DMA((2, CHIPS, 2))
        for name in ("r_send", "r_recv"):
            scratch[name] = DMA((2, CHIPS))
        for name in ("p_send", "p_recv"):
            scratch[name] = DMA((Members.PAIRS,))
    else:
        scratch["w_load"] = DMA((2 * CHIPS,))
        scratch["w_send"] = scratch["w_recv"] = DMA((zs,))
    if not last:
        scratch["h_v"] = VMEM((2, seq, d_model), bf)
        scratch["relays"] = VMEM((2, zs // 2, RING, rows, ff), bf)
        scratch["n_send"] = scratch["n_recv"] = DMA((2, Tokens.COPIES))
        scratch["x_send"] = scratch["x_recv"] = DMA((Exchange.COPIES,))
    results = pl.pallas_call(
        functools.partial(layer_kernel, layer, (*inputs, *outs, *scratch)),
        out_shape=tuple(outs.values()),
        in_specs=[vmem if name in ("g", "h", "h_next") else anywhere for name in inputs],
        out_specs=(anywhere,) * len(outs),
        scratch_shapes=list(scratch.values()),
        compiler_params=params(collective_id, 65400 * 1024),
        cost_estimate=cost(50),
        name="layer_grads",
    )(*inputs.values())
    return dict(zip(outs, results))


class RingSum:
    def __init__(self, device, block, buffers, send_sem, recv_sem):
        self.device, self.block = device, block
        self.from_left, self.from_right, self.in_left, self.in_right = buffers
        self.send_sem, self.recv_sem = send_sem, recv_sem
        self.copies = []

    def _half(self, ref, part):
        half = ref.shape[-2] // 2
        return ref.at[*[slice(None)] * (len(ref.shape) - 2), pl.ds(part * half, half)]

    def _send(self, k, src, dst, step):
        self.copies.append(send(src, dst, self.send_sem.at[k], self.recv_sem.at[k], self.device(step)))

    def _arrived(self, k, ref, step):
        arrived(ref, self.recv_sem.at[k], self.device(step), self.send_sem.at[k])

    def start(self):
        self._send(0, self.block(2, 0), self.from_left, 1)
        self._send(1, self.block(2, 1), self.from_right, -1)
        self._send(2, self.block(1, 1), self._half(self.in_left, 1), 1)
        self._send(3, self.block(-1, 0), self._half(self.in_right, 0), -1)

    def pass_right(self):
        self._arrived(0, self.from_left, -1)
        block = self.block(1, 0)
        block[...] = block[...] + self.from_left[...]
        self._send(4, block, self._half(self.in_left, 0), 1)

    def pass_left(self):
        self._arrived(1, self.from_right, 1)
        block = self.block(-1, 1)
        block[...] = block[...] + self.from_right[...]
        self._send(5, block, self._half(self.in_right, 1), -1)

    def total(self):
        self._arrived(2, self._half(self.in_left, 1), -1)
        self._arrived(3, self._half(self.in_right, 0), 1)
        self._arrived(4, self._half(self.in_left, 0), -1)
        self._arrived(5, self._half(self.in_right, 1), 1)
        return self.block(0, None)[...] + self.in_left[...] + self.in_right[...]

    def drain(self):
        for copy in self.copies:
            copy.wait_send()


def sum_scratch(lead, rows, width):
    half, whole = VMEM((*lead, rows // 2, width), jnp.float32), VMEM((*lead, rows, width), jnp.float32)
    return [half, half, whole, whole]


def dn_ring(here, dn_v, buffers, send_sem, recv_sem):
    half = dn_v.shape[1] // 2

    def block(step, part):
        at = here.chip(step)
        return dn_v.at[at] if part is None else dn_v.at[at, pl.ds(part * half, half)]

    return RingSum(here.ring, block, buffers, send_sem, recv_sem)


def dn_loads(here, dn, dn_v, load_sem):
    loads = []
    for k, step in enumerate((2, 1, -1, 0)):
        loads.append(pltpu.make_async_copy(dn.at[here.chip(step)], dn_v.at[here.chip(step)], load_sem.at[k]))
        loads[k].start()
    return loads


def g_step(d_norm, g, h):
    x_full = h[...].astype(jnp.float32)
    inv_rms = lax.rsqrt(jnp.mean(x_full * x_full, axis=-1, keepdims=True) + EPS)
    norm_f = x_full * inv_rms
    return g[...] + inv_rms * (d_norm - norm_f * jnp.mean(d_norm * norm_f, axis=-1, keepdims=True))


def next_g_kernel(dn, g, h, g_out, g_bf, dn_v, *refs):
    load_sem, send_sem, recv_sem = refs[4:]
    here = Place()
    loads = dn_loads(here, dn, dn_v, load_sem)
    meet([here.ring(1), here.ring(-1)])
    ring = dn_ring(here, dn_v, refs[:4], send_sem, recv_sem)
    for load in loads:
        load.wait()
    ring.start()
    ring.pass_right()
    ring.pass_left()
    g_new = g_step(ring.total(), g, h)
    g_out[...] = g_new
    g_bf[...] = g_new.astype(jnp.bfloat16)
    ring.drain()


def next_g(dn, g, h, collective_id):
    vmem = pl.BlockSpec(memory_space=VMEM)
    return pl.pallas_call(
        next_g_kernel,
        out_shape=(jax.ShapeDtypeStruct(g.shape, g.dtype), jax.ShapeDtypeStruct(g.shape, jnp.bfloat16)),
        in_specs=[pl.BlockSpec(memory_space=ANY), vmem, vmem],
        out_specs=(vmem,) * 2,
        scratch_shapes=[VMEM(dn.shape, dn.dtype)] + sum_scratch((), *g.shape) + [DMA((4,)), DMA((6,)), DMA((6,))],
        compiler_params=params(collective_id),
        cost_estimate=cost(42),
        name="next_g",
    )(dn, g, h)


class MemberSum:
    def __init__(self, here, grad_v, buffers, send_sem, recv_sem):
        rows = grad_v.shape[2] // 2
        self.rows = rows

        def span(first, part):
            return pl.ds(first, rows) if part is None else pl.ds(first + part * rows // 2, rows // 2)

        def block_a1(step, part):
            return grad_v.at[:, here.at_y(step), span(0, part)]

        def block_b1(step, part):
            return grad_v.at[here.at_z(step), :, span(rows, part)]

        def block_a2(step, part):
            return grad_v.at[here.at_z(step), here.y, span(0, part)]

        def block_b2(step, part):
            return grad_v.at[here.z, here.at_y(step), span(rows, part)]

        devices = (here.ring_y, here.ring_z, here.ring_z, here.ring_y)
        blocks = (block_a1, block_b1, block_a2, block_b2)
        self.a1, self.b1, self.a2, self.b2 = (
            RingSum(*each) for each in zip(devices, blocks, buffers, send_sem, recv_sem)
        )

    def start(self):
        self.a1.start()
        self.b1.start()

    def pass_first(self):
        for ring in (self.a1, self.b1):
            ring.pass_right()
        for ring in (self.a1, self.b1):
            ring.pass_left()

    def second(self):
        for first, second in ((self.a1, self.a2), (self.b1, self.b2)):
            first.block(0, None)[...] = first.total()
            second.start()

    def finish(self, piece):
        for ring in (self.a2, self.b2):
            ring.pass_right()
            ring.pass_left()
        piece[: self.rows] = self.a2.total()
        piece[self.rows :] = self.b2.total()

    def drain(self):
        for ring in (self.a1, self.b1, self.a2, self.b2):
            ring.drain()


def last_sum_kernel(n_order, dn, g, h, grad, *refs):
    g_out, piece, dn_v, grad_v = refs[n_order : n_order + 4]
    refs = refs[n_order + 4 :]
    buffers = [refs[4 * k : 4 * k + 4] for k in range(5)]
    load_sem, grad_sem, send_sem, recv_sem = refs[20:]
    here = Place()
    rows = grad.shape[2] // 2
    loads = dn_loads(here, dn, dn_v, load_sem)
    grad_loads = []
    for k, step in enumerate((2, 1, -1, 0)):
        for m in range(2):
            at = (slice(None), here.at_y(step)) if m == 0 else (here.at_z(step), slice(None))
            part = pl.ds(m * rows, rows)
            load = pltpu.make_async_copy(grad.at[*at, part], grad_v.at[*at, part], grad_sem.at[m, k])
            load.start()
            grad_loads.append(load)

    meet(
        [here.ring(1), here.ring(-1), here.ring_y(1), here.ring_y(-1), here.ring_z(1), here.ring_z(-1)]
    )
    x = dn_ring(here, dn_v, buffers[0], send_sem.at[0], recv_sem.at[0])
    members = MemberSum(here, grad_v, buffers[1:], [send_sem.at[k] for k in range(1, 5)], [recv_sem.at[k] for k in range(1, 5)])
    for load in grad_loads:
        load.wait()
    members.start()
    for load in loads:
        load.wait()
    x.start()
    x.pass_right()
    x.pass_left()
    members.pass_first()
    g_out[...] = g_step(x.total(), g, h).astype(g_out.dtype)
    members.second()
    members.finish(piece)
    x.drain()
    members.drain()


def last_sum(dn, g, h, grad, order, collective_id):
    vmem, anywhere = pl.BlockSpec(memory_space=VMEM), pl.BlockSpec(memory_space=ANY)
    _, _, rows, width = grad.shape
    return pl.pallas_call(
        functools.partial(last_sum_kernel, len(order)),
        out_shape=(jax.ShapeDtypeStruct(g.shape, jnp.bfloat16), jax.ShapeDtypeStruct((rows, width), grad.dtype)),
        in_specs=[anywhere, vmem, vmem, anywhere] + [anywhere] * len(order),
        out_specs=(vmem,) * 2,
        scratch_shapes=[VMEM(dn.shape, dn.dtype), VMEM(grad.shape, grad.dtype)]
        + sum_scratch((), *g.shape)
        + sum_scratch((RING,), rows // 2, width) * 2
        + sum_scratch((), rows // 2, width) * 2
        + [DMA((4,)), DMA((2, 4)), DMA((5, 6)), DMA((5, 6))],
        compiler_params=params(collective_id, 60 * 1024 * 1024),
        cost_estimate=cost(100),
        name="last_sum",
    )(dn, g, h, grad, *order)


def gather_rows_kernel(n_order, rows, *refs):
    out, send_sem, recv_sem, own_sem = refs[n_order:]
    here = Place()
    own = pltpu.make_async_copy(rows, out.at[here.z, here.y], own_sem.at[0])
    own.start()
    meet([here.ring_y(1), here.ring_y(-1), here.ring_z(1), here.ring_z(-1)])
    own.wait()
    members = Members(here, out, send_sem, recv_sem)
    members.start()
    members.relay_first()
    members.far()
    members.relay(1)
    members.relay(2)
    members.done(0, -1, 1, 2)
    members.drain()


def gather_rows(rows, order, collective_id):
    anywhere = pl.BlockSpec(memory_space=ANY)
    return pl.pallas_call(
        functools.partial(gather_rows_kernel, len(order)),
        out_shape=jax.ShapeDtypeStruct((RING, RING, *rows.shape), rows.dtype),
        in_specs=[pl.BlockSpec(memory_space=VMEM)] + [anywhere] * len(order),
        out_specs=anywhere,
        scratch_shapes=[DMA((Members.GROUPS, 4)), DMA((Members.GROUPS, 4)), DMA((1,))],
        compiler_params=params(collective_id),
        cost_estimate=cost(100),
        name="gather_rows",
    )(rows, *order)


def grad_rows_kernel(count, *refs):
    pieces, outs, (send_sem, recv_sem, local_sem) = refs[:count], refs[-3 - count : -3], refs[-3:]
    here = Place()
    cols = pieces[0].shape[1] // 2
    rows = pieces[0].shape[0] // 6

    def landing(i, m, chip):
        at = pl.ds(pl.multiple_of((2 * m + chip // 2) * rows, rows), rows)
        return outs[i].at[at, pl.ds(pl.multiple_of(chip % 2 * cols, cols), cols)]

    def part(i, m, chip):
        return pieces[i].at[pl.ds(pl.multiple_of(chip * rows, rows), rows), pl.ds(m * cols, cols)]

    down = pl.ds(4 * rows, 2 * rows)
    local = []
    for i in range(count):
        local.append(pltpu.make_async_copy(pieces[i].at[down], outs[i].at[down], local_sem.at[i, 2]))
        for m in range(2):
            local.append(pltpu.make_async_copy(part(i, m, here.x), landing(i, m, here.x), local_sem.at[i, m]))
    for copy in local:
        copy.start()
    meet([here.ring(j) for j in range(1, CHIPS)])
    copies = []
    for i in range(count):
        for j in (2, 1, 3):
            for m in range(2):
                src, dst = part(i, m, here.chip(j)), landing(i, m, here.x)
                copies.append(send(src, dst, send_sem.at[i, j, m], recv_sem.at[i, j, m], here.ring(j)))
    for i in range(count):
        for j in (1, 3, 2):
            for m in range(2):
                sems = recv_sem.at[i, j, m], here.ring(-j), send_sem.at[i, j, m]
                arrived(landing(i, m, here.chip(-j)), *sems)
    for copy in copies:
        copy.wait_send()
    for copy in local:
        copy.wait()


def grad_rows(pieces, order, collective_id):
    vmem = pl.BlockSpec(memory_space=VMEM)
    n = len(pieces)
    return pl.pallas_call(
        functools.partial(grad_rows_kernel, n),
        out_shape=tuple(jax.ShapeDtypeStruct(piece.shape, piece.dtype) for piece in pieces),
        in_specs=[vmem] * n + [pl.BlockSpec(memory_space=ANY)] * len(order),
        out_specs=(vmem,) * n,
        scratch_shapes=[DMA((n, CHIPS, 2)), DMA((n, CHIPS, 2)), DMA((n, 3))],
        compiler_params=params(collective_id),
        cost_estimate=cost(12),
        name="grad_rows",
    )(*pieces, *order)


PARTS = 4


def place_kernel(layer, grad, *refs):
    gate, up, down, buf, d_buf, pack, load_sem, d_sem, store_sem = refs[-9:]
    members, rows, half = grad.shape[0], grad.shape[1] // 6, grad.shape[2]
    part = max(members // PARTS, 1)
    parts = members // part
    d_load = pltpu.make_async_copy(grad.at[:, pl.ds(4 * rows, 2 * rows)], d_buf, d_sem.at[0])
    d_load.start()
    loads = []
    for m in range(2):
        for k in range(parts):
            at = pl.ds(k * part, part)
            for h in range(2):
                src = grad.at[at, pl.ds((2 * m + h) * rows, rows)]
                load = pltpu.make_async_copy(src, buf.at[m, at, :, pl.ds(h * half, half)], load_sem.at[m, k, h])
                load.start()
                loads.append(load)
    d_load.wait()
    stores = []
    for m, out in enumerate((gate, up)):
        for k in range(parts):
            at = pl.ds(k * part, part)
            for h in range(2):
                loads[(m * parts + k) * 2 + h].wait()
            store = pltpu.make_async_copy(buf.at[m, at], out.at[layer, at], store_sem.at[m, k])
            store.start()
            stores.append(store)
    col, deep = down.shape[2] // members, 2 * rows

    @pl.loop(0, half // col)
    def _(j):
        at = pl.ds(pl.multiple_of(j * deep, deep), deep)
        cols = pl.ds(pl.multiple_of(j * col, col), col)
        for d in range(members):
            pack[at, d * col : (d + 1) * col] = d_buf[d, :, cols]

    store = pltpu.make_async_copy(pack, down.at[layer], d_sem.at[1])
    store.start()
    stores.append(store)
    for store in stores:
        store.wait()


def place(grad, layer, stacks, order, shapes):
    members, rows, half = grad.shape
    anywhere = pl.BlockSpec(memory_space=ANY)
    return pl.pallas_call(
        functools.partial(place_kernel, layer),
        out_shape=shapes,
        in_specs=[anywhere] * (1 + len(stacks) + len(order)),
        out_specs=(anywhere,) * 3,
        input_output_aliases={1 + m: m for m in range(len(stacks))},
        scratch_shapes=[
            VMEM((2, members, rows // 6, 2 * half), grad.dtype),
            VMEM((members, rows // 3, half), grad.dtype),
            VMEM(shapes[2].shape[1:], grad.dtype),
            DMA((2, PARTS, 2)),
            DMA((2,)),
            DMA((2, PARTS)),
        ],
        compiler_params=pltpu.CompilerParams(vmem_limit_bytes=58 * 1024 * 1024),
        cost_estimate=cost(13),
        name="place",
    )(grad, *stacks, *order)


def gather_dp(value):
    return lax.all_gather(value[None], "dp", axis=0, tiled=True)


def scatter_dp(value):
    members, *piece = value.shape
    value = value.reshape(members * piece[0], *piece[1:])
    return lax.psum_scatter(value, "dp", scatter_dimension=0, tiled=True)


def solution(mesh):
    dp = mesh.shape["dp"]
    tok_spec = P(("dp", "fsdp"))
    stack_spec = P(None, ("dp", "fsdp"))
    weight_spec = P(None, "fsdp")

    def local_backward(h_saved, grad_out, gate_sh, up_sh, down_sh):
        layers = h_saved.shape[0]
        b_loc, seq, width = grad_out.shape
        tokens = b_loc * seq
        h = h_saved.reshape(layers, tokens, width)
        g_bf = grad_out.reshape(tokens, width)
        g = g_bf.astype(jnp.float32)
        last = layers - 1
        ids = iter(range(1, 100))

        order = tuple(reversed(range(layers)))
        gate5, up5 = (w.reshape(layers, dp // RING, RING, -1, w.shape[2]) for w in (gate_sh, up_sh))
        weights = {"gate": gate5, "up": up5, "down": down_sh}
        inputs = {"g": g_bf, **weights, "h": h[last], "h_next": h[last - 1]}
        pieces = {}
        for layer in order:
            out = layer_grads(layer, dp, inputs, next(ids))
            grad, dn = out["grad"], out["dn"]
            if layer:
                pieces[layer] = scatter_dp(grad)
                g, g_bf = next_g(dn, g, h[layer], next(ids))
                inputs = {"g": g_bf, **weights, "n": out["n_next"]}
                if layer == last:
                    inputs |= {"w": out["w_next"], "h_next": h[layer - 2]}
                    cross_gate = out["wx"]
                else:
                    inputs |= {"wx_gate": cross_gate, "wx_up": out["wx"]}
        rows = {}
        (rows[last],) = grad_rows((pieces[last],), (dn,), next(ids))
        gathered = {last: gather_dp(rows[last])}
        grad = grad.reshape(dp // RING, RING, *grad.shape[1:])
        d_h0, pieces[0] = last_sum(dn, g, h[0], grad, (rows[last],), next(ids))
        rows[1], rows[0] = grad_rows((pieces[1], pieces[0]), (), next(ids))
        gathered[0] = gather_dp(rows[0])
        mine = rows[1].reshape(4, -1, rows[1].shape[1])
        all_rows = gather_rows(mine, (), next(ids))
        gathered[1] = all_rows.reshape(gathered[0].shape)

        rows = (layers, dp, gate_sh.shape[1] // dp, gate_sh.shape[2])
        shapes = tuple(jax.ShapeDtypeStruct(shape, jnp.float32) for shape in (rows, rows, down_sh.shape))
        stacks = ()
        for layer in order:
            stacks = place(gathered[layer], layer, stacks, (all_rows,) if layer == last else (), shapes)
        gate, up, down_grad = stacks
        return gate.reshape(gate_sh.shape), up.reshape(up_sh.shape), down_grad, d_h0.reshape(b_loc, seq, width)

    return jax.shard_map(
        local_backward,
        mesh=mesh,
        in_specs=(stack_spec, tok_spec, weight_spec, weight_spec, weight_spec),
        out_specs=(weight_spec, weight_spec, weight_spec, tok_spec),
        check_vma=False,
    )
```

```python
import functools
import types

import jax
import jax.numpy as jnp
from jax import lax
from jax.experimental import pallas as pl
from jax.experimental.pallas import tpu as pltpu
from jax.sharding import PartitionSpec as P


EPS = 1e-5
CHIPS = 4
RING = 4
MESH = pl.DeviceIdType.MESH
VMEM = pltpu.VMEM
ANY = pl.ANY
DMA = pltpu.SemaphoreType.DMA


class Place:
    def __init__(self):
        self.dp = lax.axis_index("dp")
        self.f = lax.axis_index("fsdp")
        self.x, self.c = self.f // 2, self.f % 2
        self.z, self.y = self.dp // RING, self.dp % RING

    def chip(self, step):
        return (self.x + step) % CHIPS

    def ring(self, step):
        return (self.dp, 2 * self.chip(step) + self.c)

    def partner(self):
        return (self.dp, 2 * self.x + (1 - self.c))

    def at_y(self, step):
        return (self.y + step) % RING

    def at_z(self, step):
        return (self.z + step) % RING

    def ring_y(self, step):
        return (self.z * RING + self.at_y(step), self.f)

    def ring_z(self, step):
        return (self.at_z(step) * RING + self.y, self.f)


def meet(peers):
    barrier = pltpu.get_barrier_semaphore()
    for peer in peers:
        pl.semaphore_signal(barrier, inc=1, device_id=peer, device_id_type=MESH)
    pl.semaphore_wait(barrier, len(peers))


def send(src, dst, send_sem, recv_sem, device):
    copy = pltpu.make_async_remote_copy(
        src_ref=src, dst_ref=dst, send_sem=send_sem, recv_sem=recv_sem, device_id=device, device_id_type=MESH
    )
    copy.start()
    return copy


def arrived(ref, recv_sem, device, send_sem):
    pltpu.make_async_remote_copy(
        src_ref=ref, dst_ref=ref, send_sem=send_sem, recv_sem=recv_sem, device_id=device, device_id_type=MESH
    ).wait_recv()


def params(collective_id, vmem=None):
    return pltpu.CompilerParams(collective_id=collective_id, has_side_effects=True, vmem_limit_bytes=vmem)


def cost(us):
    return pl.CostEstimate(flops=int(us * 4.0e6), bytes_accessed=0, transcendentals=0)


class Ring:
    def __init__(self, device, at, block, own, send_sem, recv_sem):
        self.device, self.at, self.block, self.own = device, at, block, own
        self.send_sem, self.recv_sem = send_sem, recv_sem
        self.copies = []

    def _send(self, k, src, dst, step):
        self.copies.append(send(src, dst, self.send_sem(k), self.recv_sem(k), self.device(step)))

    def _arrived(self, k, ref, step):
        arrived(ref, self.recv_sem(k), self.device(step), self.send_sem(k))

    def start(self):
        here = self.block(self.at(0), None)
        self._send(0, self.own, here, 1)
        self._send(1, self.own, here, -1)

    def relay_right(self):
        self._arrived(0, self.block(self.at(-1), None), -1)
        half = self.block(self.at(-1), 0)
        self._send(2, half, half, 1)

    def relay_left(self):
        self._arrived(1, self.block(self.at(1), None), 1)
        half = self.block(self.at(1), 1)
        self._send(3, half, half, -1)

    def finish(self):
        self._arrived(2, self.block(self.at(2), 0), -1)
        self._arrived(3, self.block(self.at(2), 1), 1)

    def drain(self):
        for copy in self.copies:
            copy.wait_send()


class Tokens:
    COPIES = 8

    def __init__(self, here, own, out, send_sem, recv_sem):
        half = out.shape[2] // 2

        def block(chip, part):
            return out.at[0, chip] if part is None else out.at[0, chip, pl.ds(part * half, half)]

        self.here, self.own, self.out = here, own, out
        self.send_sem, self.recv_sem = send_sem, recv_sem
        self.ring = Ring(here.ring, here.chip, block, own, lambda k: send_sem.at[k], lambda k: recv_sem.at[k])
        self.pairs = []

    def _pair(self, k, src, chip):
        dst = self.out.at[1, chip]
        copy = send(src, dst, self.send_sem.at[4 + k], self.recv_sem.at[4 + k], self.here.partner())
        self.pairs.append((k, chip, copy))

    def start(self):
        self.ring.start()
        self._pair(0, self.own, self.here.x)

    def relay(self):
        left, right = self.here.chip(-1), self.here.chip(1)
        self.ring.relay_right()
        self._pair(1, self.out.at[0, left], left)
        self.ring.relay_left()
        self._pair(2, self.out.at[0, right], right)

    def far(self):
        far = self.here.chip(2)
        self.ring.finish()
        self._pair(3, self.out.at[0, far], far)

    def finish(self):
        for k, chip, copy in self.pairs:
            arrived(self.out.at[1, chip], self.recv_sem.at[4 + k], self.here.partner(), self.send_sem.at[4 + k])
            copy.wait_send()
        self.ring.drain()


class Members:
    GROUPS = 10
    PAIRS = 8

    def __init__(self, here, slots, send_sem, recv_sem, pair=None, pair_send=None, pair_recv=None):
        self.here, self.slots, self.send_sem, self.recv_sem = here, slots, send_sem, recv_sem
        self.pair, self.pair_send, self.pair_recv = pair, pair_send, pair_recv
        a1, b1 = self._ring(0, 0, True, here.z), self._ring(1, 2, False, here.y)
        a2 = {step: self._ring(2 + k, 0, False, here.at_y(step)) for k, step in enumerate((0, -1, 1, 2))}
        b2 = {step: self._ring(6 + k, 2, True, here.at_z(step)) for k, step in enumerate((0, -1, 1, 2))}
        self.rings = ((a1, a2), (b1, b2))
        self.forwards = []

    def _ring(self, group, first, along_y, fixed):
        def block(at, part):
            k = pl.ds(first, 2) if part is None else pl.ds(first + part, 1)
            return self.slots.at[fixed, at, k] if along_y else self.slots.at[at, fixed, k]

        here = self.here
        device, at = (here.ring_y, here.at_y) if along_y else (here.ring_z, here.at_z)
        sems = (lambda k: self.send_sem.at[group, k]), (lambda k: self.recv_sem.at[group, k])
        return Ring(device, at, block, block(at(0), None), *sems)

    def start(self):
        for first, second in self.rings:
            first.start()
        for first, second in self.rings:
            second[0].start()

    def relay_first(self):
        for first, second in self.rings:
            first.relay_right()
            second[-1].start()
        for first, second in self.rings:
            first.relay_left()
            second[1].start()
        for _, second in self.rings:
            second[0].relay_right()
            second[0].relay_left()

    def far(self):
        for first, second in self.rings:
            first.finish()
            second[2].start()
        self.relay(-1)

    def relay(self, step):
        for _, second in self.rings:
            second[step].relay_right()
            second[step].relay_left()

    def done(self, *steps):
        for step in steps:
            for m, (_, second) in enumerate(self.rings):
                second[step].finish()
                if self.pair is not None:
                    self._forward(m, step)

    def _group(self, ref, m, step):
        here = self.here
        return ref.at[:, here.at_y(step), pl.ds(0, 2)] if m == 0 else ref.at[here.at_z(step), :, pl.ds(2, 2)]

    def _forward(self, m, step):
        k = 4 * m + (step + 1)
        dst = self._group(self.pair, m, step)
        send_sem, recv_sem = self.pair_send.at[k], self.pair_recv.at[k]
        copy = send(self._group(self.slots, m, step), dst, send_sem, recv_sem, self.here.partner())
        self.forwards.append((copy, dst, k))

    def arrived_pair(self):
        for _, dst, k in self.forwards:
            arrived(dst, self.pair_recv.at[k], self.here.partner(), self.pair_send.at[k])

    def drain(self):
        for copy, _, _ in self.forwards:
            copy.wait_send()
        for first, second in self.rings:
            for r in (first, *second.values()):
                r.drain()


def norm_rows(h):
    x_full = h.astype(jnp.float32)
    inv_rms = lax.rsqrt(jnp.mean(x_full * x_full, axis=-1, keepdims=True) + EPS)
    return (x_full * inv_rms).astype(jnp.bfloat16)


class WeightRows:
    def __init__(self, here, layer, weights, rows_v, landing, load_sem, send_sem, recv_sem, own_sem):
        self.here, self.rows_v, self.landing = here, rows_v, landing
        self.send_sem, self.recv_sem = send_sem, recv_sem
        cols = rows_v.shape[2] // 2
        self.loads, self.copies = [], []
        for j in range(CHIPS):
            at = pl.ds(pl.multiple_of(here.chip(j) * cols, cols), cols)
            for m, w in enumerate(weights):
                dst = rows_v.at[j, :, pl.ds(m * cols, cols)]
                self.loads.append(pltpu.make_async_copy(w.at[layer, here.z, here.y, :, at], dst, load_sem.at[j, m]))
        self.own = pltpu.make_async_copy(rows_v.at[0], landing.at[here.x], own_sem)

    def load(self):
        for load in self.loads:
            load.start()

    def start(self):
        for load in self.loads:
            load.wait()
        self.own.start()
        for j in (2, 1, 3):
            dst, device = self.landing.at[self.here.x], self.here.ring(j)
            self.copies.append(send(self.rows_v.at[j], dst, self.send_sem.at[j], self.recv_sem.at[j], device))

    def finish(self):
        self.own.wait()
        for j in (1, 3, 2):
            src = self.landing.at[self.here.chip(-j)]
            arrived(src, self.recv_sem.at[j], self.here.ring(-j), self.send_sem.at[j])

    def drain(self):
        for copy in self.copies:
            copy.wait_send()


def transpose_into(dst, row, first, src):
    dst[row : row + src.shape[1], first : first + src.shape[0]] = src.T


def layer_kernel(layer, names, *refs):
    r = types.SimpleNamespace(**dict(zip(names, refs)))
    first, last = "n" not in names, layer == 0
    here = Place()
    c = here.c
    f32, bf = jnp.float32, jnp.bfloat16
    _, zs, ys, _, rows, width = r.w_v.shape
    members = zs * ys
    shard, ff, deep = members * rows, width // 2, r.pack_v.shape[2]
    seq, d_model = r.n_v.shape[2:]
    tokens = CHIPS * seq
    partner = here.partner()

    d_own, d_other = (pl.ds(pl.multiple_of(k * (ff // 2), ff // 2), ff // 2) for k in (c, 1 - c))
    d_load = pltpu.make_async_copy(r.down.at[layer], r.d_v.at[d_own], r.load.at[0])
    g_own = pltpu.make_async_copy(r.g, r.g_v.at[0, here.x], r.load.at[1])
    peers = [partner, here.ring(1), here.ring(-1)]
    w_loads = []
    if first:
        slots = (r.w_v.at[0], *(r.w_next.at[i] for i in range(layer)))
        weight_rows = [
            WeightRows(
                here, layer - i, (r.gate, r.up), r.rows_v.at[i], slot.at[here.z, here.y],
                r.r_load.at[i], r.r_send.at[i], r.r_recv.at[i], r.own_sem.at[i],
            )
            for i, slot in enumerate(slots)
        ]
        for part in weight_rows:
            part.load()
        peers += [here.ring(2), here.ring_y(1), here.ring_y(-1), here.ring_z(1), here.ring_z(-1)]
    else:
        w_loads = [pltpu.make_async_copy(r.w.at[r.w.shape[0] - 1 - layer, z], r.w_v.at[0, z], r.w_load.at[z]) for z in range(zs)]
    h_loads = [
        pltpu.make_async_copy(r.h.at[layer - i], r.h_v.at[i], r.load.at[2 + i])
        for i in (((0, 1) if first else (1,)) if not last else ())
    ]
    for load in (*h_loads, *w_loads):
        load.start()
    if not first:
        n_load = pltpu.make_async_copy(r.n, r.n_v, r.load.at[4])
        n_load.start()
    d_load.start()
    g_own.start()
    if first:
        h_loads[0].wait()
        r.h_v[0] = norm_rows(r.h_v[0])
        r.n_v[0, here.x] = r.h_v[0]
    if not last:
        h_loads[-1].wait()
        r.h_v[1] = norm_rows(r.h_v[1])
        n_own = pltpu.make_async_copy(r.h_v.at[1], r.n_next.at[0, here.x], r.load.at[5])
        n_own.start()
    meet(peers)

    tok_g = Tokens(here, r.g, r.g_v, r.g_send, r.g_recv)
    if first:
        tok_n = Tokens(here, r.h_v.at[0], r.n_v, r.n_send.at[0], r.n_recv.at[0])
        mem = Members(here, r.w_v.at[0], r.m_send.at[0], r.m_recv.at[0], r.w_v.at[1], r.p_send, r.p_recv)
        ahead_1, ahead_2 = (Members(here, r.w_next.at[i], r.m_send.at[1 + i], r.m_recv.at[1 + i]) for i in range(2))
    if not last:
        ahead_n = Tokens(here, r.h_v.at[1], r.n_next, r.n_send.at[1], r.n_recv.at[1])

    def da_pass():
        g_here = r.g_v[0].reshape(tokens, d_model)
        for low in range(0, ff, 768):
            high = min(low + 768, ff)
            r.da_v[:, low:high] = lax.dot_general(
                g_here, r.d_v[low:high, :], (((1,), (1,)), ((), ())), preferred_element_type=f32
            )

    def columns(k, core, offset=0, size=shard):
        return pl.ds(pl.multiple_of(2 * shard * k + shard * core + offset, size), size)

    def transposes():
        chunk = min(128, shard)
        for group in range(2):
            for k in range(CHIPS):
                for q in range(shard // chunk):
                    block = r.n_v[group, :, :, columns(k, c, q * chunk, chunk)].reshape(tokens, chunk)
                    transpose_into(r.n_t, k * shard + q * chunk, group * tokens, block)

    def uv_pass(parts):
        step = 256 if width % 256 == 0 else width

        @pl.loop(0, width // step)
        def _(i):
            at = pl.ds(pl.multiple_of(i * step, step), step)
            total = r.uv_v[:, at] if 0 not in parts else None
            for part in parts:
                core = c if part == 0 else 1 - c
                lhs = jnp.concatenate([r.n_v[0, :, :, columns(k, core)].reshape(tokens, shard) for k in range(CHIPS)], 1)
                rhs = jnp.concatenate([r.w_v[part, :, :, k, :, at].reshape(shard, step) for k in range(CHIPS)], 0)
                block = jnp.dot(lhs, rhs, preferred_element_type=f32)
                total = block if total is None else total + block
            r.uv_v[:, at] = total

    tile = min(32, tokens)

    def act_rows(at, u, v, sig):
        r.act_v[0, at] = (u * sig * v).astype(bf)

    def act_pass():
        @pl.loop(0, tokens // tile)
        def _(k):
            at = pl.ds(pl.multiple_of(k * tile, tile), tile)
            u = r.uv_v[at, :ff]
            act_rows(at, u, r.uv_v[at, ff:], jax.nn.sigmoid(u))

    def duv_pass(with_act):
        @pl.loop(0, tokens // tile)
        def _(k):
            at = pl.ds(pl.multiple_of(k * tile, tile), tile)
            u, v, d_act = r.uv_v[at, :ff], r.uv_v[at, ff:], r.da_v[at, :]
            sig = jax.nn.sigmoid(u)
            if with_act:
                act_rows(at, u, v, sig)
            r.duv_v[0, at, :ff] = (d_act * v * sig * (1.0 + u * (1.0 - sig))).astype(bf)
            r.duv_v[0, at, ff:] = (d_act * (u * sig)).astype(bf)

    if first:
        weight_rows[0].start()
        tok_n.start()
        d_load.wait()
        d_copy = send(r.d_v.at[d_own], r.d_v.at[d_own], r.d_send.at[0], r.d_recv.at[0], partner)
        weight_rows[0].finish()
        mem.start()
        mem.relay_first()
        tok_n.relay()
        weight_rows[1].start()
        g_own.wait()
        tok_g.start()
        mem.far()
        mem.relay(1)
        tok_n.far()
        mem.done(0)
        mem.relay(2)
        weight_rows[1].finish()
        ahead_1.start()
        mem.done(-1, 1)
        tok_n.finish()
        transposes()
        mem.done(2)
        ahead_1.relay_first()
        tok_g.relay()
        weight_rows[2].start()
        ahead_n.start()
        mem.arrived_pair()
        ahead_1.far()
        uv_pass((0, 1))
        ahead_1.relay(1)
        ahead_1.done(0)
        ahead_1.relay(2)
        tok_g.far()
        arrived(r.d_v.at[d_other], r.d_recv.at[0], partner, r.d_send.at[0])
        weight_rows[2].finish()
        ahead_2.start()
        da_pass()
        ahead_1.done(-1, 1, 2)
        ahead_2.relay_first()
        duv_pass(True)
    else:
        tok_g.start()
        for load in w_loads:
            load.wait()
        w_copies = [
            send(r.w_v.at[0, z], r.w_v.at[1, z], r.w_send.at[z], r.w_recv.at[z], partner) for z in range(zs)
        ]
        d_load.wait()
        d_copy = send(r.d_v.at[d_own], r.d_v.at[d_own], r.d_send.at[0], r.d_recv.at[0], partner)
        n_load.wait()
        transposes()
        uv_pass((0,))
        tok_g.relay()
        if not last:
            ahead_n.start()
        for z in range(zs):
            arrived(r.w_v.at[1, z], r.w_recv.at[z], partner, r.w_send.at[z])
        uv_pass((1,))
        act_pass()
        tok_g.far()
        g_own.wait()
        arrived(r.d_v.at[d_other], r.d_recv.at[0], partner, r.d_send.at[0])
        da_pass()
        duv_pass(False)
        if not last:
            ahead_n.relay()

    def dn_pass(part):
        core = c if part == 0 else 1 - c

        @pl.loop(0, CHIPS)
        def _(k):
            rhs = r.w_v[part, :, :, k].reshape(shard, width)
            block = lax.dot_general(r.duv_v[0], rhs, (((1,), (1,)), ((), ())), preferred_element_type=f32)
            r.dn_v[:, :, columns(k, core)] = block.reshape(CHIPS, seq, shard)

    dn_pass(0)
    x_copies = [
        send(r.duv_v.at[0], r.duv_v.at[1], r.c_send.at[0], r.c_recv.at[0], partner),
        send(r.act_v.at[0], r.act_v.at[1], r.c_send.at[1], r.c_recv.at[1], partner),
    ]
    if first:
        ahead_2.far()
    dn_pass(1)
    if first:
        ahead_2.relay(1)
        ahead_n.relay()
    dn_out = pltpu.make_async_copy(r.dn_v, r.dn, r.out_sem.at[4])
    dn_out.start()

    def gu_out(m, k):
        return pltpu.make_async_copy(
            r.gu_v.at[k % 2],
            r.grad.at[:, pl.ds(pl.multiple_of(rows * k, rows), rows), pl.ds(m * ff, ff)],
            r.out_sem.at[k % 2],
        )

    arrived(r.duv_v.at[1], r.c_recv.at[0], partner, r.c_send.at[0])
    for m in range(2):

        @pl.loop(0, CHIPS)
        def _(k):
            if m == 0:

                @pl.when(k >= 2)
                def _():
                    gu_out(m, k).wait()
            else:
                gu_out(m, k).wait()

            at = pl.ds(pl.multiple_of(k * shard, shard), shard)
            rhs = r.duv_v[:, :, m * ff : (m + 1) * ff].reshape(2 * tokens, ff)
            r.gu_v[k % 2] = jnp.dot(r.n_t[at, :], rhs, preferred_element_type=f32).reshape(members, rows, ff)
            gu_out(m, k).start()

    if first:
        ahead_2.done(0)
        ahead_2.relay(2)
    if not last:
        ahead_n.far()
    arrived(r.act_v.at[1], r.c_recv.at[1], partner, r.c_send.at[1])
    tok_g.finish()
    half_ff = ff // 2
    odd = half_ff % 128
    for m in range(2):
        for q in range((half_ff + odd) // 128):
            at = pl.ds(pl.multiple_of(c * (half_ff - odd) + q * 128, 128), 128)
            transpose_into(r.act_t, q * 128, m * tokens, r.act_v[m, :, at])
    group = r.pack_v.shape[1]
    col = d_model // members

    def down_out(k):
        return pltpu.make_async_copy(
            r.pack_v.at[k % 2], r.grad.at[pl.ds(k * group, group), pl.ds(CHIPS * rows, deep)], r.out_sem.at[2 + k % 2]
        )

    @pl.loop(0, members // group)
    def _(k):
        at = pl.ds(pl.multiple_of(k * group * col, group * col), group * col)
        rhs = r.g_v[:, :, :, at].reshape(2 * tokens, group * col)
        r.down_v[...] = jnp.dot(r.act_t[...], rhs, preferred_element_type=f32)

        @pl.when(k >= 2)
        def _():
            down_out(k).wait()

        for d in range(group):
            for j in range(half_ff // deep):
                at_rows = pl.ds(pl.multiple_of(c * odd + j * deep, 8), deep)
                r.pack_v[k % 2, d, :, j * col : (j + 1) * col] = r.down_v[at_rows, d * col : (d + 1) * col]
        down_out(k).start()

    for copy in (*x_copies, d_copy):
        copy.wait_send()
    if first:
        ahead_2.done(-1, 1, 2)
        for part in (*weight_rows, mem, ahead_1, ahead_2):
            part.drain()
    else:
        for copy in w_copies:
            copy.wait_send()
    if not last:
        ahead_n.finish()
        n_own.wait()
    dn_out.wait()
    for k in range(2):
        gu_out(1, k).wait()
        down_out(k).wait()


def layer_grads(layer, dp, shard_shape, inputs, collective_id):
    seq, d_model = inputs["g"].shape
    rows, ff_all = shard_shape
    tokens, shard, ff = CHIPS * seq, dp * rows, ff_all // CHIPS
    width, zs = 2 * ff, dp // RING
    deep = d_model // dp // CHIPS
    half = ff // 2 + (ff // 2) % 128
    group = max(dp // 4, 1)
    bf, f32 = jnp.bfloat16, jnp.float32
    vmem, anywhere = pl.BlockSpec(memory_space=VMEM), pl.BlockSpec(memory_space=ANY)
    first, last = "n" not in inputs, layer == 0
    outs = {
        "grad": jax.ShapeDtypeStruct((dp, CHIPS * rows + deep, width), f32),
        "dn": jax.ShapeDtypeStruct((CHIPS, seq, d_model), f32),
    }
    if not last:
        outs["n_next"] = jax.ShapeDtypeStruct((2, CHIPS, seq, d_model), bf)
    if first:
        outs["w_next"] = jax.ShapeDtypeStruct((layer, zs, RING, CHIPS, rows, width), bf)
    scratch = {
        "w_v": VMEM((2, zs, RING, CHIPS, rows, width), bf),
        "d_v": VMEM((ff, d_model), bf),
        "g_v": VMEM((2, CHIPS, seq, d_model), bf),
        "n_v": VMEM((2, CHIPS, seq, d_model), bf),
        "n_t": VMEM((CHIPS * shard, 2 * tokens), bf),
        "da_v": VMEM((tokens, ff), f32),
        "uv_v": VMEM((tokens, width), f32),
        "duv_v": VMEM((2, tokens, width), bf),
        "act_v": VMEM((2, tokens, ff), bf),
        "act_t": VMEM((half, 2 * tokens), bf),
        "dn_v": VMEM((CHIPS, seq, d_model), f32),
        "gu_v": VMEM((2, dp, rows, ff), f32),
        "down_v": VMEM((half, group * d_model // dp), f32),
        "pack_v": VMEM((2, group, deep, width), f32),
        "load": DMA((6,)),
        "out_sem": DMA((5,)),
        "c_send": DMA((2,)),
        "c_recv": DMA((2,)),
        "d_send": DMA((1,)),
        "d_recv": DMA((1,)),
        "g_send": DMA((Tokens.COPIES,)),
        "g_recv": DMA((Tokens.COPIES,)),
    }
    if first:
        scratch["rows_v"] = VMEM((1 + layer, CHIPS, rows, width), bf)
        scratch["own_sem"] = DMA((1 + layer,))
        for name in ("m_send", "m_recv"):
            scratch[name] = DMA((1 + layer, Members.GROUPS, 4))
        scratch["r_load"] = DMA((1 + layer, CHIPS, 2))
        for name in ("r_send", "r_recv"):
            scratch[name] = DMA((1 + layer, CHIPS))
        for name in ("p_send", "p_recv"):
            scratch[name] = DMA((Members.PAIRS,))
    else:
        scratch["w_load"] = DMA((zs,))
        scratch["w_send"] = scratch["w_recv"] = DMA((zs,))
    if not last:
        scratch["h_v"] = VMEM((2, seq, d_model), bf)
        scratch["n_send"] = scratch["n_recv"] = DMA((2, Tokens.COPIES))
    results = pl.pallas_call(
        functools.partial(layer_kernel, layer, (*inputs, *outs, *scratch)),
        out_shape=tuple(outs.values()),
        in_specs=[vmem if name == "g" else anywhere for name in inputs],
        out_specs=(anywhere,) * len(outs),
        scratch_shapes=list(scratch.values()),
        compiler_params=params(collective_id, 65400 * 1024),
        cost_estimate=cost(50),
        name="layer_grads",
    )(*inputs.values())
    return dict(zip(outs, results))


class RingSum:
    def __init__(self, device, block, buffers, send_sem, recv_sem):
        self.device, self.block = device, block
        self.from_left, self.from_right, self.in_left, self.in_right = buffers
        self.send_sem, self.recv_sem = send_sem, recv_sem
        self.copies = []

    def _half(self, ref, part):
        half = ref.shape[-2] // 2
        return ref.at[*[slice(None)] * (len(ref.shape) - 2), pl.ds(part * half, half)]

    def _send(self, k, src, dst, step):
        self.copies.append(send(src, dst, self.send_sem.at[k], self.recv_sem.at[k], self.device(step)))

    def _arrived(self, k, ref, step):
        arrived(ref, self.recv_sem.at[k], self.device(step), self.send_sem.at[k])

    def start(self):
        self._send(0, self.block(2, 0), self.from_left, 1)
        self._send(1, self.block(2, 1), self.from_right, -1)
        self._send(2, self.block(1, 1), self._half(self.in_left, 1), 1)
        self._send(3, self.block(-1, 0), self._half(self.in_right, 0), -1)

    def pass_right(self):
        self._arrived(0, self.from_left, -1)
        block = self.block(1, 0)
        block[...] = block[...] + self.from_left[...]
        self._send(4, block, self._half(self.in_left, 0), 1)

    def pass_left(self):
        self._arrived(1, self.from_right, 1)
        block = self.block(-1, 1)
        block[...] = block[...] + self.from_right[...]
        self._send(5, block, self._half(self.in_right, 1), -1)

    def total(self):
        self._arrived(2, self._half(self.in_left, 1), -1)
        self._arrived(3, self._half(self.in_right, 0), 1)
        self._arrived(4, self._half(self.in_left, 0), -1)
        self._arrived(5, self._half(self.in_right, 1), 1)
        return self.block(0, None)[...] + self.in_left[...] + self.in_right[...]

    def drain(self):
        for copy in self.copies:
            copy.wait_send()


def sum_scratch(lead, rows, width):
    half, whole = VMEM((*lead, rows // 2, width), jnp.float32), VMEM((*lead, rows, width), jnp.float32)
    return [half, half, whole, whole]


def dn_ring(here, dn_v, buffers, send_sem, recv_sem):
    half = dn_v.shape[1] // 2

    def block(step, part):
        at = here.chip(step)
        return dn_v.at[at] if part is None else dn_v.at[at, pl.ds(part * half, half)]

    return RingSum(here.ring, block, buffers, send_sem, recv_sem)


def dn_loads(here, dn, dn_v, load_sem):
    loads = []
    for k, step in enumerate((2, 1, -1, 0)):
        loads.append(pltpu.make_async_copy(dn.at[here.chip(step)], dn_v.at[here.chip(step)], load_sem.at[k]))
        loads[k].start()
    return loads


def g_step(d_norm, g, h):
    x_full = h[...].astype(jnp.float32)
    inv_rms = lax.rsqrt(jnp.mean(x_full * x_full, axis=-1, keepdims=True) + EPS)
    norm_f = x_full * inv_rms
    return g[...] + inv_rms * (d_norm - norm_f * jnp.mean(d_norm * norm_f, axis=-1, keepdims=True))


def next_g_kernel(layer, dn, g, h, g_out, g_bf, dn_v, h_v, *refs):
    load_sem, h_sem, send_sem, recv_sem = refs[4:]
    here = Place()
    h_load = pltpu.make_async_copy(h.at[layer], h_v, h_sem.at[0])
    h_load.start()
    loads = dn_loads(here, dn, dn_v, load_sem)
    meet([here.ring(1), here.ring(-1)])
    ring = dn_ring(here, dn_v, refs[:4], send_sem, recv_sem)
    for load in loads:
        load.wait()
    ring.start()
    ring.pass_right()
    ring.pass_left()
    h_load.wait()
    g_new = g_step(ring.total(), g, h_v)
    g_out[...] = g_new
    g_bf[...] = g_new.astype(jnp.bfloat16)
    ring.drain()


def next_g(dn, g, h, layer, collective_id):
    vmem = pl.BlockSpec(memory_space=VMEM)
    return pl.pallas_call(
        functools.partial(next_g_kernel, layer),
        out_shape=(jax.ShapeDtypeStruct(g.shape, g.dtype), jax.ShapeDtypeStruct(g.shape, jnp.bfloat16)),
        in_specs=[pl.BlockSpec(memory_space=ANY), vmem, pl.BlockSpec(memory_space=ANY)],
        out_specs=(vmem,) * 2,
        scratch_shapes=[VMEM(dn.shape, dn.dtype), VMEM(g.shape, h.dtype)]
        + sum_scratch((), *g.shape)
        + [DMA((4,)), DMA((1,)), DMA((6,)), DMA((6,))],
        compiler_params=params(collective_id),
        cost_estimate=cost(42),
        name="next_g",
    )(dn, g, h)


class MemberSum:
    def __init__(self, here, grad_v, buffers, send_sem, recv_sem):
        rows = grad_v.shape[2] // 2
        self.rows = rows

        def span(first, part):
            return pl.ds(first, rows) if part is None else pl.ds(first + part * rows // 2, rows // 2)

        def block_a1(step, part):
            return grad_v.at[:, here.at_y(step), span(0, part)]

        def block_b1(step, part):
            return grad_v.at[here.at_z(step), :, span(rows, part)]

        def block_a2(step, part):
            return grad_v.at[here.at_z(step), here.y, span(0, part)]

        def block_b2(step, part):
            return grad_v.at[here.z, here.at_y(step), span(rows, part)]

        devices = (here.ring_y, here.ring_z, here.ring_z, here.ring_y)
        blocks = (block_a1, block_b1, block_a2, block_b2)
        self.a1, self.b1, self.a2, self.b2 = (
            RingSum(*each) for each in zip(devices, blocks, buffers, send_sem, recv_sem)
        )

    def start(self):
        self.a1.start()
        self.b1.start()

    def pass_first(self):
        for ring in (self.a1, self.b1):
            ring.pass_right()
        for ring in (self.a1, self.b1):
            ring.pass_left()

    def second(self):
        for first, second in ((self.a1, self.a2), (self.b1, self.b2)):
            first.block(0, None)[...] = first.total()
            second.start()

    def finish(self, piece):
        for ring in (self.a2, self.b2):
            ring.pass_right()
            ring.pass_left()
        piece[: self.rows] = self.a2.total()
        piece[self.rows :] = self.b2.total()

    def drain(self):
        for ring in (self.a1, self.b1, self.a2, self.b2):
            ring.drain()


def last_sum_kernel(n_order, dn, g, h, grad, *refs):
    g_out, piece, dn_v, grad_v, h_v = refs[n_order : n_order + 5]
    refs = refs[n_order + 5 :]
    buffers = [refs[4 * k : 4 * k + 4] for k in range(5)]
    load_sem, grad_sem, h_sem, send_sem, recv_sem = refs[20:]
    here = Place()
    rows = grad.shape[2] // 2
    h_load = pltpu.make_async_copy(h.at[0], h_v, h_sem.at[0])
    h_load.start()
    loads = dn_loads(here, dn, dn_v, load_sem)
    grad_loads = []
    for k, step in enumerate((2, 1, -1, 0)):
        for m in range(2):
            at = (slice(None), here.at_y(step)) if m == 0 else (here.at_z(step), slice(None))
            part = pl.ds(m * rows, rows)
            load = pltpu.make_async_copy(grad.at[*at, part], grad_v.at[*at, part], grad_sem.at[m, k])
            load.start()
            grad_loads.append(load)

    meet(
        [here.ring(1), here.ring(-1), here.ring_y(1), here.ring_y(-1), here.ring_z(1), here.ring_z(-1)]
    )
    x = dn_ring(here, dn_v, buffers[0], send_sem.at[0], recv_sem.at[0])
    members = MemberSum(here, grad_v, buffers[1:], [send_sem.at[k] for k in range(1, 5)], [recv_sem.at[k] for k in range(1, 5)])
    for load in grad_loads:
        load.wait()
    members.start()
    for load in loads:
        load.wait()
    x.start()
    x.pass_right()
    x.pass_left()
    members.pass_first()
    h_load.wait()
    g_out[...] = g_step(x.total(), g, h_v).astype(g_out.dtype)
    members.second()
    members.finish(piece)
    x.drain()
    members.drain()


def last_sum(dn, g, h, grad, order, collective_id):
    vmem, anywhere = pl.BlockSpec(memory_space=VMEM), pl.BlockSpec(memory_space=ANY)
    _, _, rows, width = grad.shape
    return pl.pallas_call(
        functools.partial(last_sum_kernel, len(order)),
        out_shape=(jax.ShapeDtypeStruct(g.shape, jnp.bfloat16), jax.ShapeDtypeStruct((rows, width), grad.dtype)),
        in_specs=[anywhere, vmem, anywhere, anywhere] + [anywhere] * len(order),
        out_specs=(vmem,) * 2,
        scratch_shapes=[VMEM(dn.shape, dn.dtype), VMEM(grad.shape, grad.dtype), VMEM(g.shape, h.dtype)]
        + sum_scratch((), *g.shape)
        + sum_scratch((RING,), rows // 2, width) * 2
        + sum_scratch((), rows // 2, width) * 2
        + [DMA((4,)), DMA((2, 4)), DMA((1,)), DMA((5, 6)), DMA((5, 6))],
        compiler_params=params(collective_id, 60 * 1024 * 1024),
        cost_estimate=cost(100),
        name="last_sum",
    )(dn, g, h, grad, *order)


def gather_rows_kernel(n_order, rows, *refs):
    out, send_sem, recv_sem, own_sem = refs[n_order:]
    here = Place()
    own = pltpu.make_async_copy(rows, out.at[here.z, here.y], own_sem.at[0])
    own.start()
    meet([here.ring_y(1), here.ring_y(-1), here.ring_z(1), here.ring_z(-1)])
    own.wait()
    members = Members(here, out, send_sem, recv_sem)
    members.start()
    members.relay_first()
    members.far()
    members.relay(1)
    members.relay(2)
    members.done(0, -1, 1, 2)
    members.drain()


def gather_rows(rows, order, collective_id):
    anywhere = pl.BlockSpec(memory_space=ANY)
    return pl.pallas_call(
        functools.partial(gather_rows_kernel, len(order)),
        out_shape=jax.ShapeDtypeStruct((RING, RING, *rows.shape), rows.dtype),
        in_specs=[pl.BlockSpec(memory_space=VMEM)] + [anywhere] * len(order),
        out_specs=anywhere,
        scratch_shapes=[DMA((Members.GROUPS, 4)), DMA((Members.GROUPS, 4)), DMA((1,))],
        compiler_params=params(collective_id),
        cost_estimate=cost(100),
        name="gather_rows",
    )(rows, *order)


def grad_rows_kernel(count, *refs):
    pieces, outs, (send_sem, recv_sem, local_sem) = refs[:count], refs[-3 - count : -3], refs[-3:]
    here = Place()
    cols = pieces[0].shape[1] // 2
    rows = pieces[0].shape[0] // 6

    def landing(i, m, chip):
        at = pl.ds(pl.multiple_of((2 * m + chip // 2) * rows, rows), rows)
        return outs[i].at[at, pl.ds(pl.multiple_of(chip % 2 * cols, cols), cols)]

    def part(i, m, chip):
        return pieces[i].at[pl.ds(pl.multiple_of(chip * rows, rows), rows), pl.ds(m * cols, cols)]

    down = pl.ds(4 * rows, 2 * rows)
    local = []
    for i in range(count):
        local.append(pltpu.make_async_copy(pieces[i].at[down], outs[i].at[down], local_sem.at[i, 2]))
        for m in range(2):
            local.append(pltpu.make_async_copy(part(i, m, here.x), landing(i, m, here.x), local_sem.at[i, m]))
    for copy in local:
        copy.start()
    meet([here.ring(j) for j in range(1, CHIPS)])
    copies = []
    for i in range(count):
        for j in (2, 1, 3):
            for m in range(2):
                src, dst = part(i, m, here.chip(j)), landing(i, m, here.x)
                copies.append(send(src, dst, send_sem.at[i, j, m], recv_sem.at[i, j, m], here.ring(j)))
    for i in range(count):
        for j in (1, 3, 2):
            for m in range(2):
                sems = recv_sem.at[i, j, m], here.ring(-j), send_sem.at[i, j, m]
                arrived(landing(i, m, here.chip(-j)), *sems)
    for copy in copies:
        copy.wait_send()
    for copy in local:
        copy.wait()


def grad_rows(pieces, order, collective_id):
    vmem = pl.BlockSpec(memory_space=VMEM)
    n = len(pieces)
    return pl.pallas_call(
        functools.partial(grad_rows_kernel, n),
        out_shape=tuple(jax.ShapeDtypeStruct(piece.shape, piece.dtype) for piece in pieces),
        in_specs=[vmem] * n + [pl.BlockSpec(memory_space=ANY)] * len(order),
        out_specs=(vmem,) * n,
        scratch_shapes=[DMA((n, CHIPS, 2)), DMA((n, CHIPS, 2)), DMA((n, 3))],
        compiler_params=params(collective_id),
        cost_estimate=cost(12),
        name="grad_rows",
    )(*pieces, *order)


PARTS = 4


def place_kernel(layer, grad, *refs):
    gate, up, down, buf, d_buf, pack, load_sem, d_sem, store_sem = refs[-9:]
    members, rows, half = grad.shape[0], grad.shape[1] // 6, grad.shape[2]
    part = max(members // PARTS, 1)
    parts = members // part
    d_load = pltpu.make_async_copy(grad.at[:, pl.ds(4 * rows, 2 * rows)], d_buf, d_sem.at[0])
    d_load.start()
    loads = []
    for m in range(2):
        for k in range(parts):
            at = pl.ds(k * part, part)
            for h in range(2):
                src = grad.at[at, pl.ds((2 * m + h) * rows, rows)]
                load = pltpu.make_async_copy(src, buf.at[m, at, :, pl.ds(h * half, half)], load_sem.at[m, k, h])
                load.start()
                loads.append(load)
    d_load.wait()
    stores = []
    for m, out in enumerate((gate, up)):
        for k in range(parts):
            at = pl.ds(k * part, part)
            for h in range(2):
                loads[(m * parts + k) * 2 + h].wait()
            store = pltpu.make_async_copy(buf.at[m, at], out.at[layer, at], store_sem.at[m, k])
            store.start()
            stores.append(store)
    col, deep = down.shape[2] // members, 2 * rows

    @pl.loop(0, half // col)
    def _(j):
        at = pl.ds(pl.multiple_of(j * deep, deep), deep)
        cols = pl.ds(pl.multiple_of(j * col, col), col)
        for d in range(members):
            pack[at, d * col : (d + 1) * col] = d_buf[d, :, cols]

    store = pltpu.make_async_copy(pack, down.at[layer], d_sem.at[1])
    store.start()
    stores.append(store)
    for store in stores:
        store.wait()


def place(grad, layer, stacks, order, shapes):
    members, rows, half = grad.shape
    anywhere = pl.BlockSpec(memory_space=ANY)
    return pl.pallas_call(
        functools.partial(place_kernel, layer),
        out_shape=shapes,
        in_specs=[anywhere] * (1 + len(stacks) + len(order)),
        out_specs=(anywhere,) * 3,
        input_output_aliases={1 + m: m for m in range(len(stacks))},
        scratch_shapes=[
            VMEM((2, members, rows // 6, 2 * half), grad.dtype),
            VMEM((members, rows // 3, half), grad.dtype),
            VMEM(shapes[2].shape[1:], grad.dtype),
            DMA((2, PARTS, 2)),
            DMA((2,)),
            DMA((2, PARTS)),
        ],
        compiler_params=pltpu.CompilerParams(vmem_limit_bytes=58 * 1024 * 1024),
        cost_estimate=cost(13),
        name="place",
    )(grad, *stacks, *order)


def gather_dp(value):
    return lax.all_gather(value[None], "dp", axis=0, tiled=True)


def scatter_dp(value):
    members, *piece = value.shape
    value = value.reshape(members * piece[0], *piece[1:])
    return lax.psum_scatter(value, "dp", scatter_dimension=0, tiled=True)


def solution(mesh):
    dp = mesh.shape["dp"]
    tok_spec = P(("dp", "fsdp"))
    stack_spec = P(None, ("dp", "fsdp"))
    weight_spec = P(None, "fsdp")

    def local_backward(h_saved, grad_out, gate_sh, up_sh, down_sh):
        layers = h_saved.shape[0]
        b_loc, seq, width = grad_out.shape
        tokens = b_loc * seq
        h = h_saved.reshape(layers, tokens, width)
        g_bf = grad_out.reshape(tokens, width)
        g = g_bf.astype(jnp.float32)
        last = layers - 1
        ids = iter(range(1, 100))

        order = tuple(reversed(range(layers)))
        gate5, up5 = (w.reshape(layers, dp // RING, RING, -1, w.shape[2]) for w in (gate_sh, up_sh))
        inputs = {"g": g_bf, "down": down_sh, "h": h, "gate": gate5, "up": up5}
        shard_shape = gate5.shape[3:]
        pieces = {}
        for layer in order:
            out = layer_grads(layer, dp, shard_shape, inputs, next(ids))
            grad, dn = out["grad"], out["dn"]
            if layer:
                pieces[layer] = scatter_dp(grad)
                g, g_bf = next_g(dn, g, h, layer, next(ids))
                w_next = out["w_next"] if layer == last else w_next
                inputs = {"g": g_bf, "down": down_sh, "h": h, "n": out["n_next"], "w": w_next}
        rows = {}
        (rows[last],) = grad_rows((pieces[last],), (dn,), next(ids))
        gathered = {last: gather_dp(rows[last])}
        grad = grad.reshape(dp // RING, RING, *grad.shape[1:])
        d_h0, pieces[0] = last_sum(dn, g, h, grad, (rows[last],), next(ids))
        rows[1], rows[0] = grad_rows((pieces[1], pieces[0]), (), next(ids))
        gathered[0] = gather_dp(rows[0])
        mine = rows[1].reshape(4, -1, rows[1].shape[1])
        all_rows = gather_rows(mine, (), next(ids))
        gathered[1] = all_rows.reshape(gathered[0].shape)

        rows = (layers, dp, gate_sh.shape[1] // dp, gate_sh.shape[2])
        shapes = tuple(jax.ShapeDtypeStruct(shape, jnp.float32) for shape in (rows, rows, down_sh.shape))
        stacks = ()
        for layer in order:
            stacks = place(gathered[layer], layer, stacks, (all_rows,) if layer == last else (), shapes)
        gate, up, down_grad = stacks
        return gate.reshape(gate_sh.shape), up.reshape(up_sh.shape), down_grad, d_h0.reshape(b_loc, seq, width)

    return jax.shard_map(
        local_backward,
        mesh=mesh,
        in_specs=(stack_spec, tok_spec, weight_spec, weight_spec, weight_spec),
        out_specs=(weight_spec, weight_spec, weight_spec, tok_spec),
        check_vma=False,
    )
```

```python
import functools
import types

import jax
import jax.numpy as jnp
from jax import lax
from jax.experimental import pallas as pl
from jax.experimental.pallas import tpu as pltpu
from jax.sharding import PartitionSpec as P


EPS = 1e-5
CHIPS = 4
RING = 4
MESH = pl.DeviceIdType.MESH
VMEM = pltpu.VMEM
ANY = pl.ANY
DMA = pltpu.SemaphoreType.DMA


class Place:
    def __init__(self):
        self.dp = lax.axis_index("dp")
        self.f = lax.axis_index("fsdp")
        self.x, self.c = self.f // 2, self.f % 2
        self.z, self.y = self.dp // RING, self.dp % RING

    def chip(self, step):
        return (self.x + step) % CHIPS

    def ring(self, step):
        return (self.dp, 2 * self.chip(step) + self.c)

    def partner(self):
        return (self.dp, 2 * self.x + (1 - self.c))

    def at_y(self, step):
        return (self.y + step) % RING

    def at_z(self, step):
        return (self.z + step) % RING

    def ring_y(self, step):
        return (self.z * RING + self.at_y(step), self.f)

    def ring_z(self, step):
        return (self.at_z(step) * RING + self.y, self.f)


def meet(peers):
    barrier = pltpu.get_barrier_semaphore()
    for peer in peers:
        pl.semaphore_signal(barrier, inc=1, device_id=peer, device_id_type=MESH)
    pl.semaphore_wait(barrier, len(peers))


def send(src, dst, send_sem, recv_sem, device):
    copy = pltpu.make_async_remote_copy(
        src_ref=src, dst_ref=dst, send_sem=send_sem, recv_sem=recv_sem, device_id=device, device_id_type=MESH
    )
    copy.start()
    return copy


def arrived(ref, recv_sem, device, send_sem):
    pltpu.make_async_remote_copy(
        src_ref=ref, dst_ref=ref, send_sem=send_sem, recv_sem=recv_sem, device_id=device, device_id_type=MESH
    ).wait_recv()


def params(collective_id, vmem=None):
    return pltpu.CompilerParams(collective_id=collective_id, has_side_effects=True, vmem_limit_bytes=vmem)


def cost(us):
    return pl.CostEstimate(flops=int(us * 4.0e6), bytes_accessed=0, transcendentals=0)


class Ring:
    def __init__(self, device, at, block, own, send_sem, recv_sem):
        self.device, self.at, self.block, self.own = device, at, block, own
        self.send_sem, self.recv_sem = send_sem, recv_sem
        self.copies = []

    def _send(self, k, src, dst, step):
        self.copies.append(send(src, dst, self.send_sem(k), self.recv_sem(k), self.device(step)))

    def _arrived(self, k, ref, step):
        arrived(ref, self.recv_sem(k), self.device(step), self.send_sem(k))

    def start(self):
        here = self.block(self.at(0), None)
        self._send(0, self.own, here, 1)
        self._send(1, self.own, here, -1)

    def relay_right(self):
        self._arrived(0, self.block(self.at(-1), None), -1)
        half = self.block(self.at(-1), 0)
        self._send(2, half, half, 1)

    def relay_left(self):
        self._arrived(1, self.block(self.at(1), None), 1)
        half = self.block(self.at(1), 1)
        self._send(3, half, half, -1)

    def finish(self):
        self._arrived(2, self.block(self.at(2), 0), -1)
        self._arrived(3, self.block(self.at(2), 1), 1)

    def drain(self):
        for copy in self.copies:
            copy.wait_send()


class Tokens:
    COPIES = 8

    def __init__(self, here, own, out, send_sem, recv_sem):
        half = out.shape[2] // 2

        def block(chip, part):
            return out.at[0, chip] if part is None else out.at[0, chip, pl.ds(part * half, half)]

        self.here, self.own, self.out = here, own, out
        self.send_sem, self.recv_sem = send_sem, recv_sem
        self.ring = Ring(here.ring, here.chip, block, own, lambda k: send_sem.at[k], lambda k: recv_sem.at[k])
        self.pairs = []

    def _pair(self, k, src, chip):
        dst = self.out.at[1, chip]
        copy = send(src, dst, self.send_sem.at[4 + k], self.recv_sem.at[4 + k], self.here.partner())
        self.pairs.append((k, chip, copy))

    def start(self):
        self.ring.start()
        self._pair(0, self.own, self.here.x)

    def relay(self):
        left, right = self.here.chip(-1), self.here.chip(1)
        self.ring.relay_right()
        self._pair(1, self.out.at[0, left], left)
        self.ring.relay_left()
        self._pair(2, self.out.at[0, right], right)

    def far(self):
        far = self.here.chip(2)
        self.ring.finish()
        self._pair(3, self.out.at[0, far], far)

    def finish(self):
        for k, chip, copy in self.pairs:
            arrived(self.out.at[1, chip], self.recv_sem.at[4 + k], self.here.partner(), self.send_sem.at[4 + k])
            copy.wait_send()
        self.ring.drain()


class Members:
    GROUPS = 10
    PAIRS = 8

    def __init__(self, here, slots, send_sem, recv_sem, pair=None, pair_send=None, pair_recv=None):
        self.here, self.slots, self.send_sem, self.recv_sem = here, slots, send_sem, recv_sem
        self.pair, self.pair_send, self.pair_recv = pair, pair_send, pair_recv
        a1, b1 = self._ring(0, 0, True, here.z), self._ring(1, 2, False, here.y)
        a2 = {step: self._ring(2 + k, 0, False, here.at_y(step)) for k, step in enumerate((0, -1, 1, 2))}
        b2 = {step: self._ring(6 + k, 2, True, here.at_z(step)) for k, step in enumerate((0, -1, 1, 2))}
        self.rings = ((a1, a2), (b1, b2))
        self.forwards = []

    def _ring(self, group, first, along_y, fixed):
        def block(at, part):
            k = pl.ds(first, 2) if part is None else pl.ds(first + part, 1)
            return self.slots.at[fixed, at, k] if along_y else self.slots.at[at, fixed, k]

        here = self.here
        device, at = (here.ring_y, here.at_y) if along_y else (here.ring_z, here.at_z)
        sems = (lambda k: self.send_sem.at[group, k]), (lambda k: self.recv_sem.at[group, k])
        return Ring(device, at, block, block(at(0), None), *sems)

    def start(self):
        for first, second in self.rings:
            first.start()
        for first, second in self.rings:
            second[0].start()

    def relay_first(self):
        for first, second in self.rings:
            first.relay_right()
            second[-1].start()
        for first, second in self.rings:
            first.relay_left()
            second[1].start()
        for _, second in self.rings:
            second[0].relay_right()
            second[0].relay_left()

    def far(self):
        for first, second in self.rings:
            first.finish()
            second[2].start()
        self.relay(-1)

    def relay(self, step):
        for _, second in self.rings:
            second[step].relay_right()
            second[step].relay_left()

    def done(self, *steps):
        for step in steps:
            for m, (_, second) in enumerate(self.rings):
                second[step].finish()
                if self.pair is not None:
                    self._forward(m, step)

    def _group(self, ref, m, step):
        here = self.here
        return ref.at[:, here.at_y(step), pl.ds(0, 2)] if m == 0 else ref.at[here.at_z(step), :, pl.ds(2, 2)]

    def _forward(self, m, step):
        k = 4 * m + (step + 1)
        dst = self._group(self.pair, m, step)
        send_sem, recv_sem = self.pair_send.at[k], self.pair_recv.at[k]
        copy = send(self._group(self.slots, m, step), dst, send_sem, recv_sem, self.here.partner())
        self.forwards.append((copy, dst, k))

    def arrived_pair(self):
        for _, dst, k in self.forwards:
            arrived(dst, self.pair_recv.at[k], self.here.partner(), self.pair_send.at[k])

    def drain(self):
        for copy, _, _ in self.forwards:
            copy.wait_send()
        for first, second in self.rings:
            for r in (first, *second.values()):
                r.drain()


def norm_rows(h):
    x_full = h.astype(jnp.float32)
    inv_rms = lax.rsqrt(jnp.mean(x_full * x_full, axis=-1, keepdims=True) + EPS)
    return (x_full * inv_rms).astype(jnp.bfloat16)


class WeightRows:
    def __init__(self, here, layer, weights, rows_v, landing, load_sem, send_sem, recv_sem, own_sem):
        self.here, self.rows_v, self.landing = here, rows_v, landing
        self.send_sem, self.recv_sem = send_sem, recv_sem
        cols = rows_v.shape[2] // 2
        self.loads, self.copies = [], []
        for j in range(CHIPS):
            at = pl.ds(pl.multiple_of(here.chip(j) * cols, cols), cols)
            for m, w in enumerate(weights):
                dst = rows_v.at[j, :, pl.ds(m * cols, cols)]
                self.loads.append(pltpu.make_async_copy(w.at[layer, here.z, here.y, :, at], dst, load_sem.at[j, m]))
        self.own = pltpu.make_async_copy(rows_v.at[0], landing.at[here.x], own_sem)

    def load(self):
        for load in self.loads:
            load.start()

    def start(self):
        for load in self.loads:
            load.wait()
        self.own.start()
        for j in (2, 1, 3):
            dst, device = self.landing.at[self.here.x], self.here.ring(j)
            self.copies.append(send(self.rows_v.at[j], dst, self.send_sem.at[j], self.recv_sem.at[j], device))

    def finish(self):
        self.own.wait()
        for j in (1, 3, 2):
            src = self.landing.at[self.here.chip(-j)]
            arrived(src, self.recv_sem.at[j], self.here.ring(-j), self.send_sem.at[j])

    def drain(self):
        for copy in self.copies:
            copy.wait_send()


def transpose_into(dst, row, first, src):
    dst[row : row + src.shape[1], first : first + src.shape[0]] = src.T


def layer_kernel(layer, names, *refs):
    r = types.SimpleNamespace(**dict(zip(names, refs)))
    first, last = "n" not in names, layer == 0
    here = Place()
    c = here.c
    f32, bf = jnp.float32, jnp.bfloat16
    _, zs, ys, _, rows, width = r.w_v.shape
    members = zs * ys
    shard, ff, deep = members * rows, width // 2, r.pack_v.shape[2]
    seq, d_model = r.n_v.shape[2:]
    tokens = CHIPS * seq
    partner = here.partner()

    d_own, d_other = (pl.ds(pl.multiple_of(k * (ff // 2), ff // 2), ff // 2) for k in (c, 1 - c))
    d_load = pltpu.make_async_copy(r.down.at[layer], r.d_v.at[d_own], r.load.at[0])
    g_own = pltpu.make_async_copy(r.g, r.g_v.at[0, here.x], r.load.at[1])
    peers = [partner, here.ring(1), here.ring(-1)]
    w_loads = []
    if first:
        slots = (r.w_v.at[0], *(r.w_next.at[i] for i in range(layer)))
        weight_rows = [
            WeightRows(
                here, layer - i, (r.gate, r.up), r.rows_v.at[i], slot.at[here.z, here.y],
                r.r_load.at[i], r.r_send.at[i], r.r_recv.at[i], r.own_sem.at[i],
            )
            for i, slot in enumerate(slots)
        ]
        for part in weight_rows:
            part.load()
        peers += [here.ring(2), here.ring_y(1), here.ring_y(-1), here.ring_z(1), here.ring_z(-1)]
    else:
        w_loads = [pltpu.make_async_copy(r.w.at[r.w.shape[0] - 1 - layer, z], r.w_v.at[0, z], r.w_load.at[z]) for z in range(zs)]
    h_loads = [
        pltpu.make_async_copy(r.h.at[layer - i], r.h_v.at[i], r.load.at[2 + i])
        for i in (((0, 1) if first else (1,)) if not last else ())
    ]
    for load in (*h_loads, *w_loads):
        load.start()
    if not first:
        n_load = pltpu.make_async_copy(r.n, r.n_v, r.load.at[4])
        n_load.start()
    d_load.start()
    g_own.start()
    if first:
        h_loads[0].wait()
        r.h_v[0] = norm_rows(r.h_v[0])
        r.n_v[0, here.x] = r.h_v[0]
    if not last:
        h_loads[-1].wait()
        r.h_v[1] = norm_rows(r.h_v[1])
        n_own = pltpu.make_async_copy(r.h_v.at[1], r.n_next.at[0, here.x], r.load.at[5])
        n_own.start()
    meet(peers)

    tok_g = Tokens(here, r.g, r.g_v, r.g_send, r.g_recv)
    if first:
        tok_n = Tokens(here, r.h_v.at[0], r.n_v, r.n_send.at[0], r.n_recv.at[0])
        mem = Members(here, r.w_v.at[0], r.m_send.at[0], r.m_recv.at[0], r.w_v.at[1], r.p_send, r.p_recv)
        ahead_1, ahead_2 = (Members(here, r.w_next.at[i], r.m_send.at[1 + i], r.m_recv.at[1 + i]) for i in range(2))
    if not last:
        ahead_n = Tokens(here, r.h_v.at[1], r.n_next, r.n_send.at[1], r.n_recv.at[1])

    def da_pass():
        g_here = r.g_v[0].reshape(tokens, d_model)
        for low in range(0, ff, 768):
            high = min(low + 768, ff)
            r.da_v[:, low:high] = lax.dot_general(
                g_here, r.d_v[low:high, :], (((1,), (1,)), ((), ())), preferred_element_type=f32
            )

    def columns(k, core, offset=0, size=shard):
        return pl.ds(pl.multiple_of(2 * shard * k + shard * core + offset, size), size)

    def transposes():
        chunk = min(128, shard)
        for group in range(2):
            for k in range(CHIPS):
                for q in range(shard // chunk):
                    block = r.n_v[group, :, :, columns(k, c, q * chunk, chunk)].reshape(tokens, chunk)
                    transpose_into(r.n_t, k * shard + q * chunk, group * tokens, block)

    def uv_pass(parts):
        step = 256 if width % 256 == 0 else width

        @pl.loop(0, width // step)
        def _(i):
            at = pl.ds(pl.multiple_of(i * step, step), step)
            total = r.uv_v[:, at] if 0 not in parts else None
            for part in parts:
                core = c if part == 0 else 1 - c
                lhs = jnp.concatenate([r.n_v[0, :, :, columns(k, core)].reshape(tokens, shard) for k in range(CHIPS)], 1)
                rhs = jnp.concatenate([r.w_v[part, :, :, k, :, at].reshape(shard, step) for k in range(CHIPS)], 0)
                block = jnp.dot(lhs, rhs, preferred_element_type=f32)
                total = block if total is None else total + block
            r.uv_v[:, at] = total

    tile = min(32, tokens)

    def act_rows(at, u, v, sig):
        r.act_v[0, at] = (u * sig * v).astype(bf)

    def act_pass():
        @pl.loop(0, tokens // tile)
        def _(k):
            at = pl.ds(pl.multiple_of(k * tile, tile), tile)
            u = r.uv_v[at, :ff]
            act_rows(at, u, r.uv_v[at, ff:], jax.nn.sigmoid(u))

    def duv_pass(with_act):
        @pl.loop(0, tokens // tile)
        def _(k):
            at = pl.ds(pl.multiple_of(k * tile, tile), tile)
            u, v, d_act = r.uv_v[at, :ff], r.uv_v[at, ff:], r.da_v[at, :]
            sig = jax.nn.sigmoid(u)
            if with_act:
                act_rows(at, u, v, sig)
            r.duv_v[0, at, :ff] = (d_act * v * sig * (1.0 + u * (1.0 - sig))).astype(bf)
            r.duv_v[0, at, ff:] = (d_act * (u * sig)).astype(bf)

    if first:
        weight_rows[0].start()
        tok_n.start()
        d_load.wait()
        d_copy = send(r.d_v.at[d_own], r.d_v.at[d_own], r.d_send.at[0], r.d_recv.at[0], partner)
        weight_rows[0].finish()
        mem.start()
        mem.relay_first()
        tok_n.relay()
        weight_rows[1].start()
        g_own.wait()
        tok_g.start()
        mem.far()
        mem.relay(1)
        tok_n.far()
        mem.done(0)
        mem.relay(2)
        weight_rows[1].finish()
        ahead_1.start()
        mem.done(-1, 1)
        tok_n.finish()
        transposes()
        tok_g.relay()
        weight_rows[2].start()
        ahead_n.start()
        mem.done(2)
        mem.arrived_pair()
        uv_pass((0, 1))
        ahead_1.relay_first()
        tok_g.far()
        arrived(r.d_v.at[d_other], r.d_recv.at[0], partner, r.d_send.at[0])
        da_pass()
        duv_pass(True)
        ahead_1.far()
    else:
        tok_g.start()
        for load in w_loads:
            load.wait()
        w_copies = [
            send(r.w_v.at[0, z], r.w_v.at[1, z], r.w_send.at[z], r.w_recv.at[z], partner) for z in range(zs)
        ]
        d_load.wait()
        d_copy = send(r.d_v.at[d_own], r.d_v.at[d_own], r.d_send.at[0], r.d_recv.at[0], partner)
        n_load.wait()
        transposes()
        uv_pass((0,))
        tok_g.relay()
        if not last:
            ahead_n.start()
        for z in range(zs):
            arrived(r.w_v.at[1, z], r.w_recv.at[z], partner, r.w_send.at[z])
        uv_pass((1,))
        act_pass()
        tok_g.far()
        g_own.wait()
        arrived(r.d_v.at[d_other], r.d_recv.at[0], partner, r.d_send.at[0])
        da_pass()
        duv_pass(False)

    def dn_pass(part):
        core = c if part == 0 else 1 - c

        @pl.loop(0, CHIPS)
        def _(k):
            rhs = r.w_v[part, :, :, k].reshape(shard, width)
            block = lax.dot_general(r.duv_v[0], rhs, (((1,), (1,)), ((), ())), preferred_element_type=f32)
            r.dn_v[:, :, columns(k, core)] = block.reshape(CHIPS, seq, shard)

    def exchange():
        return [
            send(r.duv_v.at[0], r.duv_v.at[1], r.c_send.at[0], r.c_recv.at[0], partner),
            send(r.act_v.at[0], r.act_v.at[1], r.c_send.at[1], r.c_recv.at[1], partner),
        ]

    if first:
        x_copies = exchange()
    dn_pass(0)
    if first:
        ahead_1.relay(1)
        ahead_1.done(0)
        ahead_1.relay(2)
        weight_rows[2].finish()
        ahead_2.start()
    else:
        x_copies = exchange()
    dn_pass(1)
    if not last:
        ahead_n.relay()
    dn_out = pltpu.make_async_copy(r.dn_v, r.dn, r.out_sem.at[4])
    dn_out.start()

    def gu_out(m, k):
        return pltpu.make_async_copy(
            r.gu_v.at[k % 2],
            r.grad.at[:, pl.ds(pl.multiple_of(rows * k, rows), rows), pl.ds(m * ff, ff)],
            r.out_sem.at[k % 2],
        )

    arrived(r.duv_v.at[1], r.c_recv.at[0], partner, r.c_send.at[0])
    for m in range(2):

        @pl.loop(0, CHIPS)
        def _(k):
            if m == 0:

                @pl.when(k >= 2)
                def _():
                    gu_out(m, k).wait()
            else:
                gu_out(m, k).wait()

            at = pl.ds(pl.multiple_of(k * shard, shard), shard)
            rhs = r.duv_v[:, :, m * ff : (m + 1) * ff].reshape(2 * tokens, ff)
            r.gu_v[k % 2] = jnp.dot(r.n_t[at, :], rhs, preferred_element_type=f32).reshape(members, rows, ff)
            gu_out(m, k).start()

        if first and m == 0:
            ahead_1.done(-1, 1, 2)
            ahead_2.relay_first()
    if not last:
        ahead_n.far()
    if first:
        ahead_2.far()
    arrived(r.act_v.at[1], r.c_recv.at[1], partner, r.c_send.at[1])
    tok_g.finish()
    half_ff = ff // 2
    odd = half_ff % 128
    for m in range(2):
        for q in range((half_ff + odd) // 128):
            at = pl.ds(pl.multiple_of(c * (half_ff - odd) + q * 128, 128), 128)
            transpose_into(r.act_t, q * 128, m * tokens, r.act_v[m, :, at])
    group = r.pack_v.shape[1]
    col = d_model // members

    def down_out(k):
        return pltpu.make_async_copy(
            r.pack_v.at[k % 2], r.grad.at[pl.ds(k * group, group), pl.ds(CHIPS * rows, deep)], r.out_sem.at[2 + k % 2]
        )

    @pl.loop(0, members // group)
    def _(k):
        at = pl.ds(pl.multiple_of(k * group * col, group * col), group * col)
        rhs = r.g_v[:, :, :, at].reshape(2 * tokens, group * col)
        r.down_v[...] = jnp.dot(r.act_t[...], rhs, preferred_element_type=f32)

        @pl.when(k >= 2)
        def _():
            down_out(k).wait()

        for d in range(group):
            for j in range(half_ff // deep):
                at_rows = pl.ds(pl.multiple_of(c * odd + j * deep, 8), deep)
                r.pack_v[k % 2, d, :, j * col : (j + 1) * col] = r.down_v[at_rows, d * col : (d + 1) * col]
        down_out(k).start()

    for copy in (*x_copies, d_copy):
        copy.wait_send()
    if first:
        ahead_2.relay(1)
        ahead_2.done(0)
        ahead_2.relay(2)
        ahead_2.done(-1, 1, 2)
        for part in (*weight_rows, mem, ahead_1, ahead_2):
            part.drain()
    else:
        for copy in w_copies:
            copy.wait_send()
    if not last:
        ahead_n.finish()
        n_own.wait()
    dn_out.wait()
    for k in range(2):
        gu_out(1, k).wait()
        down_out(k).wait()


def layer_grads(layer, dp, shard_shape, inputs, collective_id):
    seq, d_model = inputs["g"].shape
    rows, ff_all = shard_shape
    tokens, shard, ff = CHIPS * seq, dp * rows, ff_all // CHIPS
    width, zs = 2 * ff, dp // RING
    deep = d_model // dp // CHIPS
    half = ff // 2 + (ff // 2) % 128
    group = max(dp // 4, 1)
    bf, f32 = jnp.bfloat16, jnp.float32
    vmem, anywhere = pl.BlockSpec(memory_space=VMEM), pl.BlockSpec(memory_space=ANY)
    first, last = "n" not in inputs, layer == 0
    outs = {
        "grad": jax.ShapeDtypeStruct((dp, CHIPS * rows + deep, width), f32),
        "dn": jax.ShapeDtypeStruct((CHIPS, seq, d_model), f32),
    }
    if not last:
        outs["n_next"] = jax.ShapeDtypeStruct((2, CHIPS, seq, d_model), bf)
    if first:
        outs["w_next"] = jax.ShapeDtypeStruct((layer, zs, RING, CHIPS, rows, width), bf)
    scratch = {
        "w_v": VMEM((2, zs, RING, CHIPS, rows, width), bf),
        "d_v": VMEM((ff, d_model), bf),
        "g_v": VMEM((2, CHIPS, seq, d_model), bf),
        "n_v": VMEM((2, CHIPS, seq, d_model), bf),
        "n_t": VMEM((CHIPS * shard, 2 * tokens), bf),
        "da_v": VMEM((tokens, ff), f32),
        "uv_v": VMEM((tokens, width), f32),
        "duv_v": VMEM((2, tokens, width), bf),
        "act_v": VMEM((2, tokens, ff), bf),
        "act_t": VMEM((half, 2 * tokens), bf),
        "dn_v": VMEM((CHIPS, seq, d_model), f32),
        "gu_v": VMEM((2, dp, rows, ff), f32),
        "down_v": VMEM((half, group * d_model // dp), f32),
        "pack_v": VMEM((2, group, deep, width), f32),
        "load": DMA((6,)),
        "out_sem": DMA((5,)),
        "c_send": DMA((2,)),
        "c_recv": DMA((2,)),
        "d_send": DMA((1,)),
        "d_recv": DMA((1,)),
        "g_send": DMA((Tokens.COPIES,)),
        "g_recv": DMA((Tokens.COPIES,)),
    }
    if first:
        scratch["rows_v"] = VMEM((1 + layer, CHIPS, rows, width), bf)
        scratch["own_sem"] = DMA((1 + layer,))
        for name in ("m_send", "m_recv"):
            scratch[name] = DMA((1 + layer, Members.GROUPS, 4))
        scratch["r_load"] = DMA((1 + layer, CHIPS, 2))
        for name in ("r_send", "r_recv"):
            scratch[name] = DMA((1 + layer, CHIPS))
        for name in ("p_send", "p_recv"):
            scratch[name] = DMA((Members.PAIRS,))
    else:
        scratch["w_load"] = DMA((zs,))
        scratch["w_send"] = scratch["w_recv"] = DMA((zs,))
    if not last:
        scratch["h_v"] = VMEM((2, seq, d_model), bf)
        scratch["n_send"] = scratch["n_recv"] = DMA((2, Tokens.COPIES))
    results = pl.pallas_call(
        functools.partial(layer_kernel, layer, (*inputs, *outs, *scratch)),
        out_shape=tuple(outs.values()),
        in_specs=[vmem if name == "g" else anywhere for name in inputs],
        out_specs=(anywhere,) * len(outs),
        scratch_shapes=list(scratch.values()),
        compiler_params=params(collective_id, 65400 * 1024),
        cost_estimate=cost(50),
        name="layer_grads",
    )(*inputs.values())
    return dict(zip(outs, results))


class RingSum:
    def __init__(self, device, block, buffers, send_sem, recv_sem):
        self.device, self.block = device, block
        self.from_left, self.from_right, self.in_left, self.in_right = buffers
        self.send_sem, self.recv_sem = send_sem, recv_sem
        self.copies = []

    def _half(self, ref, part):
        half = ref.shape[-2] // 2
        return ref.at[*[slice(None)] * (len(ref.shape) - 2), pl.ds(part * half, half)]

    def _send(self, k, src, dst, step):
        self.copies.append(send(src, dst, self.send_sem.at[k], self.recv_sem.at[k], self.device(step)))

    def _arrived(self, k, ref, step):
        arrived(ref, self.recv_sem.at[k], self.device(step), self.send_sem.at[k])

    def start(self, loads=()):
        for load in loads[:1]:
            load.wait()
        self._send(0, self.block(2, 0), self.from_left, 1)
        self._send(1, self.block(2, 1), self.from_right, -1)
        for load in loads[1:]:
            load.wait()
        self._send(2, self.block(1, 1), self._half(self.in_left, 1), 1)
        self._send(3, self.block(-1, 0), self._half(self.in_right, 0), -1)

    def pass_right(self):
        self._arrived(0, self.from_left, -1)
        block = self.block(1, 0)
        block[...] = block[...] + self.from_left[...]
        self._send(4, block, self._half(self.in_left, 0), 1)

    def pass_left(self):
        self._arrived(1, self.from_right, 1)
        block = self.block(-1, 1)
        block[...] = block[...] + self.from_right[...]
        self._send(5, block, self._half(self.in_right, 1), -1)

    def total(self):
        self._arrived(2, self._half(self.in_left, 1), -1)
        self._arrived(3, self._half(self.in_right, 0), 1)
        self._arrived(4, self._half(self.in_left, 0), -1)
        self._arrived(5, self._half(self.in_right, 1), 1)
        return self.block(0, None)[...] + self.in_left[...] + self.in_right[...]

    def drain(self):
        for copy in self.copies:
            copy.wait_send()


def sum_scratch(lead, rows, width):
    half, whole = VMEM((*lead, rows // 2, width), jnp.float32), VMEM((*lead, rows, width), jnp.float32)
    return [half, half, whole, whole]


def dn_ring(here, dn_v, buffers, send_sem, recv_sem):
    half = dn_v.shape[1] // 2

    def block(step, part):
        at = here.chip(step)
        return dn_v.at[at] if part is None else dn_v.at[at, pl.ds(part * half, half)]

    return RingSum(here.ring, block, buffers, send_sem, recv_sem)


def dn_loads(here, dn, dn_v, load_sem):
    loads = []
    for k, step in enumerate((2, 1, -1, 0)):
        loads.append(pltpu.make_async_copy(dn.at[here.chip(step)], dn_v.at[here.chip(step)], load_sem.at[k]))
        loads[k].start()
    return loads


def g_step(d_norm, g, h):
    x_full = h[...].astype(jnp.float32)
    inv_rms = lax.rsqrt(jnp.mean(x_full * x_full, axis=-1, keepdims=True) + EPS)
    norm_f = x_full * inv_rms
    return g[...].astype(jnp.float32) + inv_rms * (d_norm - norm_f * jnp.mean(d_norm * norm_f, axis=-1, keepdims=True))


def next_g_kernel(layer, dn, g, h, g_out, g_bf, dn_v, h_v, *refs):
    load_sem, h_sem, send_sem, recv_sem = refs[4:]
    here = Place()
    h_load = pltpu.make_async_copy(h.at[layer], h_v, h_sem.at[0])
    h_load.start()
    loads = dn_loads(here, dn, dn_v, load_sem)
    meet([here.ring(1), here.ring(-1)])
    ring = dn_ring(here, dn_v, refs[:4], send_sem, recv_sem)
    ring.start(loads)
    ring.pass_right()
    ring.pass_left()
    h_load.wait()
    g_new = g_step(ring.total(), g, h_v)
    g_out[...] = g_new
    g_bf[...] = g_new.astype(jnp.bfloat16)
    ring.drain()


def next_g(dn, g, h, layer, collective_id):
    vmem = pl.BlockSpec(memory_space=VMEM)
    return pl.pallas_call(
        functools.partial(next_g_kernel, layer),
        out_shape=(jax.ShapeDtypeStruct(g.shape, jnp.float32), jax.ShapeDtypeStruct(g.shape, jnp.bfloat16)),
        in_specs=[pl.BlockSpec(memory_space=ANY), vmem, pl.BlockSpec(memory_space=ANY)],
        out_specs=(vmem,) * 2,
        scratch_shapes=[VMEM(dn.shape, dn.dtype), VMEM(g.shape, h.dtype)]
        + sum_scratch((), *g.shape)
        + [DMA((4,)), DMA((1,)), DMA((6,)), DMA((6,))],
        compiler_params=params(collective_id),
        cost_estimate=cost(42),
        name="next_g",
    )(dn, g, h)


class MemberSum:
    def __init__(self, here, grad_v, buffers, send_sem, recv_sem):
        rows = grad_v.shape[2] // 2
        self.rows = rows

        def span(first, part):
            return pl.ds(first, rows) if part is None else pl.ds(first + part * rows // 2, rows // 2)

        def block_a1(step, part):
            return grad_v.at[:, here.at_y(step), span(0, part)]

        def block_b1(step, part):
            return grad_v.at[here.at_z(step), :, span(rows, part)]

        def block_a2(step, part):
            return grad_v.at[here.at_z(step), here.y, span(0, part)]

        def block_b2(step, part):
            return grad_v.at[here.z, here.at_y(step), span(rows, part)]

        devices = (here.ring_y, here.ring_z, here.ring_z, here.ring_y)
        blocks = (block_a1, block_b1, block_a2, block_b2)
        self.a1, self.b1, self.a2, self.b2 = (
            RingSum(*each) for each in zip(devices, blocks, buffers, send_sem, recv_sem)
        )

    def start(self):
        self.a1.start()
        self.b1.start()

    def pass_first(self):
        for ring in (self.a1, self.b1):
            ring.pass_right()
        for ring in (self.a1, self.b1):
            ring.pass_left()

    def second(self):
        for first, second in ((self.a1, self.a2), (self.b1, self.b2)):
            first.block(0, None)[...] = first.total()
            second.start()

    def finish(self, piece):
        for ring in (self.a2, self.b2):
            ring.pass_right()
            ring.pass_left()
        piece[: self.rows] = self.a2.total()
        piece[self.rows :] = self.b2.total()

    def drain(self):
        for ring in (self.a1, self.b1, self.a2, self.b2):
            ring.drain()


def last_sum_kernel(n_order, dn, g, h, grad, *refs):
    g_out, piece, dn_v, grad_v, h_v = refs[n_order : n_order + 5]
    refs = refs[n_order + 5 :]
    buffers = [refs[4 * k : 4 * k + 4] for k in range(5)]
    load_sem, grad_sem, h_sem, send_sem, recv_sem = refs[20:]
    here = Place()
    rows = grad.shape[2] // 2
    h_load = pltpu.make_async_copy(h.at[0], h_v, h_sem.at[0])
    h_load.start()
    loads = dn_loads(here, dn, dn_v, load_sem)
    grad_loads = []
    for k, step in enumerate((2, 1, -1, 0)):
        for m in range(2):
            at = (slice(None), here.at_y(step)) if m == 0 else (here.at_z(step), slice(None))
            part = pl.ds(m * rows, rows)
            load = pltpu.make_async_copy(grad.at[*at, part], grad_v.at[*at, part], grad_sem.at[m, k])
            load.start()
            grad_loads.append(load)

    meet(
        [here.ring(1), here.ring(-1), here.ring_y(1), here.ring_y(-1), here.ring_z(1), here.ring_z(-1)]
    )
    x = dn_ring(here, dn_v, buffers[0], send_sem.at[0], recv_sem.at[0])
    members = MemberSum(here, grad_v, buffers[1:], [send_sem.at[k] for k in range(1, 5)], [recv_sem.at[k] for k in range(1, 5)])
    for load in grad_loads:
        load.wait()
    members.start()
    x.start(loads)
    x.pass_right()
    x.pass_left()
    members.pass_first()
    h_load.wait()
    g_out[...] = g_step(x.total(), g, h_v).astype(g_out.dtype)
    members.second()
    members.finish(piece)
    x.drain()
    members.drain()


def last_sum(dn, g, h, grad, order, collective_id):
    vmem, anywhere = pl.BlockSpec(memory_space=VMEM), pl.BlockSpec(memory_space=ANY)
    _, _, rows, width = grad.shape
    return pl.pallas_call(
        functools.partial(last_sum_kernel, len(order)),
        out_shape=(jax.ShapeDtypeStruct(g.shape, jnp.bfloat16), jax.ShapeDtypeStruct((rows, width), grad.dtype)),
        in_specs=[anywhere, vmem, anywhere, anywhere] + [anywhere] * len(order),
        out_specs=(vmem,) * 2,
        scratch_shapes=[VMEM(dn.shape, dn.dtype), VMEM(grad.shape, grad.dtype), VMEM(g.shape, h.dtype)]
        + sum_scratch((), *g.shape)
        + sum_scratch((RING,), rows // 2, width) * 2
        + sum_scratch((), rows // 2, width) * 2
        + [DMA((4,)), DMA((2, 4)), DMA((1,)), DMA((5, 6)), DMA((5, 6))],
        compiler_params=params(collective_id, 60 * 1024 * 1024),
        cost_estimate=cost(100),
        name="last_sum",
    )(dn, g, h, grad, *order)


def gather_rows_kernel(n_order, rows, *refs):
    out, send_sem, recv_sem, own_sem = refs[n_order:]
    here = Place()
    own = pltpu.make_async_copy(rows, out.at[here.z, here.y], own_sem.at[0])
    own.start()
    meet([here.ring_y(1), here.ring_y(-1), here.ring_z(1), here.ring_z(-1)])
    own.wait()
    members = Members(here, out, send_sem, recv_sem)
    members.start()
    members.relay_first()
    members.far()
    members.relay(1)
    members.relay(2)
    members.done(0, -1, 1, 2)
    members.drain()


def gather_rows(rows, order, collective_id):
    anywhere = pl.BlockSpec(memory_space=ANY)
    return pl.pallas_call(
        functools.partial(gather_rows_kernel, len(order)),
        out_shape=jax.ShapeDtypeStruct((RING, RING, *rows.shape), rows.dtype),
        in_specs=[pl.BlockSpec(memory_space=VMEM)] + [anywhere] * len(order),
        out_specs=anywhere,
        scratch_shapes=[DMA((Members.GROUPS, 4)), DMA((Members.GROUPS, 4)), DMA((1,))],
        compiler_params=params(collective_id),
        cost_estimate=cost(100),
        name="gather_rows",
    )(rows, *order)


def grad_rows_kernel(count, *refs):
    pieces, outs, (send_sem, recv_sem, local_sem) = refs[:count], refs[-3 - count : -3], refs[-3:]
    here = Place()
    cols = pieces[0].shape[1] // 2
    rows = pieces[0].shape[0] // 6

    def landing(i, m, chip):
        at = pl.ds(pl.multiple_of((2 * m + chip // 2) * rows, rows), rows)
        return outs[i].at[at, pl.ds(pl.multiple_of(chip % 2 * cols, cols), cols)]

    def part(i, m, chip):
        return pieces[i].at[pl.ds(pl.multiple_of(chip * rows, rows), rows), pl.ds(m * cols, cols)]

    down = pl.ds(4 * rows, 2 * rows)
    local = []
    for i in range(count):
        local.append(pltpu.make_async_copy(pieces[i].at[down], outs[i].at[down], local_sem.at[i, 2]))
        for m in range(2):
            local.append(pltpu.make_async_copy(part(i, m, here.x), landing(i, m, here.x), local_sem.at[i, m]))
    for copy in local:
        copy.start()
    meet([here.ring(j) for j in range(1, CHIPS)])
    copies = []
    for i in range(count):
        for j in (2, 1, 3):
            for m in range(2):
                src, dst = part(i, m, here.chip(j)), landing(i, m, here.x)
                copies.append(send(src, dst, send_sem.at[i, j, m], recv_sem.at[i, j, m], here.ring(j)))
    for i in range(count):
        for j in (1, 3, 2):
            for m in range(2):
                sems = recv_sem.at[i, j, m], here.ring(-j), send_sem.at[i, j, m]
                arrived(landing(i, m, here.chip(-j)), *sems)
    for copy in copies:
        copy.wait_send()
    for copy in local:
        copy.wait()


def grad_rows(pieces, order, collective_id):
    vmem = pl.BlockSpec(memory_space=VMEM)
    n = len(pieces)
    return pl.pallas_call(
        functools.partial(grad_rows_kernel, n),
        out_shape=tuple(jax.ShapeDtypeStruct(piece.shape, piece.dtype) for piece in pieces),
        in_specs=[vmem] * n + [pl.BlockSpec(memory_space=ANY)] * len(order),
        out_specs=(vmem,) * n,
        scratch_shapes=[DMA((n, CHIPS, 2)), DMA((n, CHIPS, 2)), DMA((n, 3))],
        compiler_params=params(collective_id),
        cost_estimate=cost(12),
        name="grad_rows",
    )(*pieces, *order)


PARTS = 4


def place_kernel(layer, grad, *refs):
    gate, up, down, buf, d_buf, pack, load_sem, d_sem, store_sem = refs[-9:]
    members, rows, half = grad.shape[0], grad.shape[1] // 6, grad.shape[2]
    part = max(members // PARTS, 1)
    parts = members // part
    d_load = pltpu.make_async_copy(grad.at[:, pl.ds(4 * rows, 2 * rows)], d_buf, d_sem.at[0])
    d_load.start()
    loads = []
    for m in range(2):
        for k in range(parts):
            at = pl.ds(k * part, part)
            for h in range(2):
                src = grad.at[at, pl.ds((2 * m + h) * rows, rows)]
                load = pltpu.make_async_copy(src, buf.at[m, at, :, pl.ds(h * half, half)], load_sem.at[m, k, h])
                load.start()
                loads.append(load)
    d_load.wait()
    col, deep = down.shape[2] // members, 2 * rows

    @pl.loop(0, half // col)
    def _(j):
        at = pl.ds(pl.multiple_of(j * deep, deep), deep)
        cols = pl.ds(pl.multiple_of(j * col, col), col)
        for d in range(members):
            pack[at, d * col : (d + 1) * col] = d_buf[d, :, cols]

    stores = [pltpu.make_async_copy(pack, down.at[layer], d_sem.at[1])]
    stores[0].start()
    for m, out in enumerate((gate, up)):
        for k in range(parts):
            at = pl.ds(k * part, part)
            for h in range(2):
                loads[(m * parts + k) * 2 + h].wait()
            store = pltpu.make_async_copy(buf.at[m, at], out.at[layer, at], store_sem.at[m, k])
            store.start()
            stores.append(store)
    for store in stores:
        store.wait()


def place(grad, layer, stacks, order, shapes):
    members, rows, half = grad.shape
    anywhere = pl.BlockSpec(memory_space=ANY)
    return pl.pallas_call(
        functools.partial(place_kernel, layer),
        out_shape=shapes,
        in_specs=[anywhere] * (1 + len(stacks) + len(order)),
        out_specs=(anywhere,) * 3,
        input_output_aliases={1 + m: m for m in range(len(stacks))},
        scratch_shapes=[
            VMEM((2, members, rows // 6, 2 * half), grad.dtype),
            VMEM((members, rows // 3, half), grad.dtype),
            VMEM(shapes[2].shape[1:], grad.dtype),
            DMA((2, PARTS, 2)),
            DMA((2,)),
            DMA((2, PARTS)),
        ],
        compiler_params=pltpu.CompilerParams(vmem_limit_bytes=58 * 1024 * 1024),
        cost_estimate=cost(13),
        name="place",
    )(grad, *stacks, *order)


def gather_dp(value):
    return lax.all_gather(value[None], "dp", axis=0, tiled=True)


def scatter_dp(value):
    members, *piece = value.shape
    value = value.reshape(members * piece[0], *piece[1:])
    return lax.psum_scatter(value, "dp", scatter_dimension=0, tiled=True)


def solution(mesh):
    dp = mesh.shape["dp"]
    tok_spec = P(("dp", "fsdp"))
    stack_spec = P(None, ("dp", "fsdp"))
    weight_spec = P(None, "fsdp")

    def local_backward(h_saved, grad_out, gate_sh, up_sh, down_sh):
        layers = h_saved.shape[0]
        b_loc, seq, width = grad_out.shape
        tokens = b_loc * seq
        h = h_saved.reshape(layers, tokens, width)
        g_bf = grad_out.reshape(tokens, width)
        g = g_bf
        last = layers - 1
        ids = iter(range(1, 100))

        order = tuple(reversed(range(layers)))
        gate5, up5 = (w.reshape(layers, dp // RING, RING, -1, w.shape[2]) for w in (gate_sh, up_sh))
        inputs = {"g": g_bf, "down": down_sh, "h": h, "gate": gate5, "up": up5}
        shard_shape = gate5.shape[3:]
        pieces = {}
        for layer in order:
            out = layer_grads(layer, dp, shard_shape, inputs, next(ids))
            grad, dn = out["grad"], out["dn"]
            if layer:
                pieces[layer] = scatter_dp(grad)
                g, g_bf = next_g(dn, g, h, layer, next(ids))
                w_next = out["w_next"] if layer == last else w_next
                inputs = {"g": g_bf, "down": down_sh, "h": h, "n": out["n_next"], "w": w_next}
        rows = {}
        (rows[last],) = grad_rows((pieces[last],), (dn,), next(ids))
        gathered = {last: gather_dp(rows[last])}
        grad = grad.reshape(dp // RING, RING, *grad.shape[1:])
        d_h0, pieces[0] = last_sum(dn, g, h, grad, (rows[last],), next(ids))
        rows[1], rows[0] = grad_rows((pieces[1], pieces[0]), (), next(ids))
        gathered[0] = gather_dp(rows[0])
        mine = rows[1].reshape(4, -1, rows[1].shape[1])
        all_rows = gather_rows(mine, (), next(ids))
        gathered[1] = all_rows.reshape(gathered[0].shape)

        rows = (layers, dp, gate_sh.shape[1] // dp, gate_sh.shape[2])
        shapes = tuple(jax.ShapeDtypeStruct(shape, jnp.float32) for shape in (rows, rows, down_sh.shape))
        stacks = ()
        for layer in order:
            stacks = place(gathered[layer], layer, stacks, (all_rows,) if layer == last else (), shapes)
        gate, up, down_grad = stacks
        return gate.reshape(gate_sh.shape), up.reshape(up_sh.shape), down_grad, d_h0.reshape(b_loc, seq, width)

    return jax.shard_map(
        local_backward,
        mesh=mesh,
        in_specs=(stack_spec, tok_spec, weight_spec, weight_spec, weight_spec),
        out_specs=(weight_spec, weight_spec, weight_spec, tok_spec),
        check_vma=False,
    )
```
